8 devices in a mesh: ep: 8 (over z, y, x, core).
Axes of the slice: x: 2, y: 2, z: 1, core: 2. Of those that a mesh axis runs over, the one named last changes fastest.
Arguments:
- tokens: bfloat16 [1024, 4096], P('ep')
- k_cache: bfloat16 [1024, 64, 32, 128], P('ep')
- v_cache: bfloat16 [1024, 64, 32, 128], P('ep')
- positions: int32 [1024], P('ep')
- expert_one: int32 [1024], P('ep')
- expert_two: int32 [1024], P('ep')
- eligible: int32 [1024, 16], P('ep')
- ln1_gain: bfloat16 [4096], replicated
- ln1_bias: bfloat16 [4096], replicated
- w_query: bfloat16 [4096, 4096], replicated
- b_query: bfloat16 [4096], replicated
- w_key: bfloat16 [4096, 4096], replicated
- b_key: bfloat16 [4096], replicated
- w_value: bfloat16 [4096, 4096], replicated
- b_value: bfloat16 [4096], replicated
- w_out: bfloat16 [4096, 4096], replicated
- b_out: bfloat16 [4096], replicated
- ln2_gain: bfloat16 [4096], replicated
- ln2_bias: bfloat16 [4096], replicated
- w_router: bfloat16 [4096, 16], replicated
- w_gate: bfloat16 [16, 4096, 688], P('ep')
- w_up: bfloat16 [16, 4096, 688], P('ep')
- w_down: bfloat16 [16, 688, 4096], P('ep')
Outputs:
- output 1: bfloat16 [1024, 4096], P('ep')
- output 2: bfloat16 [1024, 32, 128], P('ep')
- output 3: bfloat16 [1024, 32, 128], P('ep')
All inputs are finite; a program needn't handle non-finite values.
Results may differ from the reference program's by a relative error of at most 0.00972537.
Values are sent between devices in bfloat16 or wider.
A program may use at most 1.25 GiB of HBM per device.

```python
import jax
import jax.numpy as jnp
from jax import lax

D_MODEL = 4096
NUM_HEADS = 32
NUM_KV_HEADS = 32
HEAD_DIM = 128
FF_DIM = 688
NUM_EXPERTS = 16
TOK_DEV = 128
SEQ_LEN = 64
NUM_GROUPS = 8
BATCH = TOK_DEV * NUM_GROUPS
GROUP_SIZE = NUM_HEADS // NUM_KV_HEADS
Q_DIM = NUM_HEADS * HEAD_DIM
KV_DIM = NUM_KV_HEADS * HEAD_DIM
ROPE_BASE = 10000.0
LN_EPS = 1e-5


def draw_normal(key, arr_shape, std_dev):
    return (jax.random.normal(key, arr_shape, jnp.float32) * std_dev).astype(jnp.bfloat16)


def draw_positions(key):
    k_pos, k_top, k_low = jax.random.split(key, 3)
    row_ids = jnp.arange(BATCH)
    pos_vals = jax.random.randint(k_pos, (BATCH,), 0, SEQ_LEN)
    top_row = jax.random.randint(k_top, (), 0, BATCH)
    low_row = (top_row + 1 + jax.random.randint(k_low, (), 0, BATCH - 1)) % BATCH
    pos_vals = jnp.where(row_ids == top_row, SEQ_LEN - 1, pos_vals)
    return jnp.where(row_ids == low_row, 0, pos_vals).astype(jnp.int32)


def draw_routes(key):
    k_mix, k_hot, k_src, k_rot, k_sec, k_elig = jax.random.split(key, 6)
    row_ids = jnp.arange(BATCH)
    mix_draw = jax.random.randint(k_mix, (BATCH,), 0, 4 * NUM_EXPERTS)
    hot_expert = jax.random.randint(k_hot, (), 0, NUM_EXPERTS)
    first_choice = jnp.where(mix_draw < 2 * NUM_EXPERTS, mix_draw % NUM_EXPERTS, (hot_expert + mix_draw % 2) % NUM_EXPERTS)
    src_group = jax.random.randint(k_src, (), 0, NUM_GROUPS)
    first_choice = jnp.where(row_ids // TOK_DEV == src_group, hot_expert, first_choice)
    rotation = jax.random.randint(k_rot, (), 0, NUM_EXPERTS)
    offset_rows = (row_ids - (src_group + 1) * TOK_DEV) % BATCH
    first_choice = jnp.where(offset_rows < NUM_EXPERTS, (offset_rows + rotation) % NUM_EXPERTS, first_choice)
    second_choice = (first_choice + 1 + jax.random.randint(k_sec, (BATCH,), 0, NUM_EXPERTS - 1)) % NUM_EXPERTS
    expert_ids = jnp.arange(NUM_EXPERTS)[None, :]
    extra_elig = jax.random.randint(k_elig, (BATCH, NUM_EXPERTS), 0, 8) == 0
    eligible = extra_elig | (expert_ids == first_choice[:, None]) | (expert_ids == second_choice[:, None])
    return first_choice.astype(jnp.int32), second_choice.astype(jnp.int32), eligible.astype(jnp.int32)


def setup_inputs(seed: int = 0) -> dict:
    keys = jax.random.split(jax.random.key(seed), 22)
    expert_one, expert_two, eligible = draw_routes(keys[0])
    value_mean = jax.random.normal(keys[3], (BATCH, 1, NUM_KV_HEADS, HEAD_DIM), jnp.float32)
    value_draw = jax.random.normal(keys[4], (BATCH, SEQ_LEN, NUM_KV_HEADS, HEAD_DIM), jnp.float32)
    ln1_gain = (1.0 + 0.3 * jax.random.normal(keys[6], (D_MODEL,), jnp.float32)).astype(jnp.bfloat16)
    ln2_gain = (1.0 + 0.3 * jax.random.normal(keys[16], (D_MODEL,), jnp.float32)).astype(jnp.bfloat16)
    return {
        'tokens': draw_normal(keys[1], (BATCH, D_MODEL), 1.0),
        'k_cache': draw_normal(keys[2], (BATCH, SEQ_LEN, NUM_KV_HEADS, HEAD_DIM), 2.0),
        'v_cache': (value_draw + value_mean).astype(jnp.bfloat16),
        'positions': draw_positions(keys[5]),
        'expert_one': expert_one,
        'expert_two': expert_two,
        'eligible': eligible,
        'ln1_gain': ln1_gain,
        'ln1_bias': draw_normal(keys[7], (D_MODEL,), 0.3),
        'w_query': draw_normal(keys[8], (D_MODEL, Q_DIM), D_MODEL ** -0.5),
        'b_query': draw_normal(keys[9], (Q_DIM,), 0.5),
        'w_key': draw_normal(keys[10], (D_MODEL, KV_DIM), D_MODEL ** -0.5),
        'b_key': draw_normal(keys[11], (KV_DIM,), 0.5),
        'w_value': draw_normal(keys[12], (D_MODEL, KV_DIM), D_MODEL ** -0.5),
        'b_value': draw_normal(keys[13], (KV_DIM,), 0.5),
        'w_out': draw_normal(keys[14], (Q_DIM, D_MODEL), Q_DIM ** -0.5),
        'b_out': draw_normal(keys[15], (D_MODEL,), 0.3),
        'ln2_gain': ln2_gain,
        'ln2_bias': draw_normal(keys[17], (D_MODEL,), 0.3),
        'w_router': draw_normal(keys[18], (D_MODEL, NUM_EXPERTS), D_MODEL ** -0.5),
        'w_gate': draw_normal(keys[19], (NUM_EXPERTS, D_MODEL, FF_DIM), D_MODEL ** -0.5),
        'w_up': draw_normal(keys[20], (NUM_EXPERTS, D_MODEL, FF_DIM), D_MODEL ** -0.5),
        'w_down': draw_normal(keys[21], (NUM_EXPERTS, FF_DIM, D_MODEL), FF_DIM ** -0.5),
    }


def layer_norm(values_in, gain, bias):
    mean_val = jnp.mean(values_in, axis=-1, keepdims=True)
    centered = values_in - mean_val
    var_val = jnp.mean(centered * centered, axis=-1, keepdims=True)
    return centered * lax.rsqrt(var_val + LN_EPS) * gain.astype(jnp.float32) + bias.astype(jnp.float32)


def rope_tables(positions):
    half_dim = HEAD_DIM // 2
    inv_freq = ROPE_BASE ** (jnp.arange(half_dim, dtype=jnp.float32) * (-2.0 / HEAD_DIM))
    angles = positions.astype(jnp.float32)[:, None] * inv_freq[None, :]
    angles = jnp.concatenate([angles, angles], axis=-1)
    return jnp.cos(angles), jnp.sin(angles)


def apply_rope(values_in, cos_tab, sin_tab):
    half_dim = values_in.shape[-1] // 2
    rotated = jnp.concatenate([-values_in[..., half_dim:], values_in[..., :half_dim]], axis=-1)
    return values_in * cos_tab[:, None, :] + rotated * sin_tab[:, None, :]


def attend_one(seq_parts):
    q_seq, k_seq, v_seq, k_one, v_one, pos_one = seq_parts
    score_scale = HEAD_DIM ** -0.5
    q_f = q_seq.astype(jnp.float32)
    s_cache = jnp.einsum('kgd,skd->kgs', q_f, k_seq.astype(jnp.float32)) * score_scale
    valid_mask = jnp.arange(SEQ_LEN)[None, None, :] < pos_one
    s_cache = jnp.where(valid_mask, s_cache, -jnp.inf)
    s_new = jnp.einsum('kgd,kd->kg', q_f, k_one.astype(jnp.float32)) * score_scale
    top_val = jnp.maximum(jnp.max(s_cache, axis=-1), s_new)
    e_cache = jnp.exp(s_cache - top_val[..., None])
    e_new = jnp.exp(s_new - top_val)
    denom_sum = jnp.sum(e_cache, axis=-1) + e_new
    p_cache = (e_cache / denom_sum[..., None]).astype(jnp.bfloat16).astype(jnp.float32)
    p_new = (e_new / denom_sum).astype(jnp.bfloat16).astype(jnp.float32)
    attn_vals = jnp.einsum('kgs,skd->kgd', p_cache, v_seq.astype(jnp.float32))
    return attn_vals + p_new[..., None] * v_one.astype(jnp.float32)[:, None, :]


def router_gates(h_two, w_router, expert_one, expert_two, eligible):
    logits = jnp.dot(h_two, w_router, preferred_element_type=jnp.float32)
    expert_ids = jnp.arange(NUM_EXPERTS)[None, :]
    hit_one = expert_ids == expert_one[:, None]
    hit_two = expert_ids == expert_two[:, None]
    keep_one = eligible == 1
    keep_two = keep_one & jnp.logical_not(hit_one)
    prob_one = jax.nn.softmax(jnp.where(keep_one, logits, -jnp.inf), axis=-1)
    prob_two = jax.nn.softmax(jnp.where(keep_two, logits, -jnp.inf), axis=-1)
    gate_one = jnp.sum(jnp.where(hit_one, prob_one, 0.0), axis=-1)
    gate_two = jnp.sum(jnp.where(hit_two, prob_two, 0.0), axis=-1)
    return gate_one, gate_two


def reference(tokens, k_cache, v_cache, positions, expert_one, expert_two, eligible, ln1_gain, ln1_bias, w_query, b_query, w_key, b_key, w_value, b_value, w_out, b_out, ln2_gain, ln2_bias, w_router, w_gate, w_up, w_down):
    x_f = tokens.astype(jnp.float32)
    h_one = layer_norm(x_f, ln1_gain, ln1_bias).astype(jnp.bfloat16)
    cos_tab, sin_tab = rope_tables(positions)
    q_lin = jnp.dot(h_one, w_query, preferred_element_type=jnp.float32) + b_query.astype(jnp.float32)
    q_rot = apply_rope(q_lin.reshape(BATCH, NUM_HEADS, HEAD_DIM), cos_tab, sin_tab).astype(jnp.bfloat16)
    k_lin = jnp.dot(h_one, w_key, preferred_element_type=jnp.float32) + b_key.astype(jnp.float32)
    key_new = apply_rope(k_lin.reshape(BATCH, NUM_KV_HEADS, HEAD_DIM), cos_tab, sin_tab).astype(jnp.bfloat16)
    v_lin = jnp.dot(h_one, w_value, preferred_element_type=jnp.float32) + b_value.astype(jnp.float32)
    value_new = v_lin.astype(jnp.bfloat16).reshape(BATCH, NUM_KV_HEADS, HEAD_DIM)
    q_grp = q_rot.reshape(BATCH, NUM_KV_HEADS, GROUP_SIZE, HEAD_DIM)
    attn_vals = lax.map(attend_one, (q_grp, k_cache, v_cache, key_new, value_new, positions))
    attn_flat = attn_vals.astype(jnp.bfloat16).reshape(BATCH, Q_DIM)
    x_mid = (x_f + jnp.dot(attn_flat, w_out, preferred_element_type=jnp.float32) + b_out.astype(jnp.float32)).astype(jnp.bfloat16)
    h_two = layer_norm(x_mid.astype(jnp.float32), ln2_gain, ln2_bias).astype(jnp.bfloat16)
    gate_one, gate_two = router_gates(h_two, w_router, expert_one, expert_two, eligible)

    def expert_step(acc_sum, expert_parts):
        gate_w, up_w, down_w, expert_idx = expert_parts
        u_val = jnp.dot(h_two, gate_w, preferred_element_type=jnp.float32)
        v_val = jnp.dot(h_two, up_w, preferred_element_type=jnp.float32)
        z_val = (jax.nn.silu(u_val) * v_val).astype(jnp.bfloat16)
        out_val = jnp.dot(z_val, down_w, preferred_element_type=jnp.float32).astype(jnp.bfloat16)
        weight_col = jnp.where(expert_one == expert_idx, gate_one, 0.0) + jnp.where(expert_two == expert_idx, gate_two, 0.0)
        return acc_sum + weight_col[:, None] * out_val.astype(jnp.float32), None

    y_sum, _ = lax.scan(expert_step, jnp.zeros((BATCH, D_MODEL), jnp.float32), (w_gate, w_up, w_down, jnp.arange(NUM_EXPERTS)))
    tokens_out = (x_mid.astype(jnp.float32) + y_sum).astype(jnp.bfloat16)
    return tokens_out, key_new, value_new
```

```python
import jax
import jax.numpy as jnp
from jax import lax
from jax.sharding import PartitionSpec as P

ROPE_BASE = 10000.0
LN_EPS = 1e-5


def layer_norm(values_in, gain, bias):
    mean_val = jnp.mean(values_in, axis=-1, keepdims=True)
    centered = values_in - mean_val
    var_val = jnp.mean(centered * centered, axis=-1, keepdims=True)
    return centered * lax.rsqrt(var_val + LN_EPS) * gain.astype(jnp.float32) + bias.astype(jnp.float32)


def rope_tables(positions, head_dim):
    half_dim = head_dim // 2
    inv_freq = ROPE_BASE ** (jnp.arange(half_dim, dtype=jnp.float32) * (-2.0 / head_dim))
    angles = positions.astype(jnp.float32)[:, None] * inv_freq[None, :]
    angles = jnp.concatenate([angles, angles], axis=-1)
    return jnp.cos(angles), jnp.sin(angles)


def apply_rope(values_in, cos_tab, sin_tab):
    half_dim = values_in.shape[-1] // 2
    rotated = jnp.concatenate([-values_in[..., half_dim:], values_in[..., :half_dim]], axis=-1)
    return values_in * cos_tab[:, None, :] + rotated * sin_tab[:, None, :]


def attention_block(tokens, k_cache, v_cache, positions, ln1_gain, ln1_bias, w_query, b_query, w_key, b_key, w_value, b_value, w_out, b_out):
    tok_count, seq_len, kv_heads, head_dim = k_cache.shape
    num_heads = w_query.shape[1] // head_dim
    group_size = num_heads // kv_heads
    x_f = tokens.astype(jnp.float32)
    h_one = layer_norm(x_f, ln1_gain, ln1_bias).astype(jnp.bfloat16)
    cos_tab, sin_tab = rope_tables(positions, head_dim)
    q_lin = jnp.dot(h_one, w_query, preferred_element_type=jnp.float32) + b_query.astype(jnp.float32)
    q_rot = apply_rope(q_lin.reshape(tok_count, num_heads, head_dim), cos_tab, sin_tab).astype(jnp.bfloat16)
    q_grp = q_rot.reshape(tok_count, kv_heads, group_size, head_dim)
    k_lin = jnp.dot(h_one, w_key, preferred_element_type=jnp.float32) + b_key.astype(jnp.float32)
    key_new = apply_rope(k_lin.reshape(tok_count, kv_heads, head_dim), cos_tab, sin_tab).astype(jnp.bfloat16)
    v_lin = jnp.dot(h_one, w_value, preferred_element_type=jnp.float32) + b_value.astype(jnp.float32)
    value_new = v_lin.astype(jnp.bfloat16).reshape(tok_count, kv_heads, head_dim)
    score_scale = head_dim ** -0.5
    s_cache = jnp.einsum('tkgd,tskd->tkgs', q_grp, k_cache, preferred_element_type=jnp.float32) * score_scale
    valid_mask = jnp.arange(seq_len)[None, None, None, :] < positions[:, None, None, None]
    s_cache = jnp.where(valid_mask, s_cache, -jnp.inf)
    s_new = jnp.einsum('tkgd,tkd->tkg', q_grp, key_new, preferred_element_type=jnp.float32) * score_scale
    top_val = jnp.maximum(jnp.max(s_cache, axis=-1), s_new)
    e_cache = jnp.exp(s_cache - top_val[..., None])
    e_new = jnp.exp(s_new - top_val)
    denom_sum = jnp.sum(e_cache, axis=-1) + e_new
    p_cache = (e_cache / denom_sum[..., None]).astype(jnp.bfloat16)
    p_new = (e_new / denom_sum).astype(jnp.bfloat16)
    attn_vals = jnp.einsum('tkgs,tskd->tkgd', p_cache, v_cache, preferred_element_type=jnp.float32)
    attn_vals = attn_vals + p_new.astype(jnp.float32)[..., None] * value_new.astype(jnp.float32)[:, :, None, :]
    attn_flat = attn_vals.astype(jnp.bfloat16).reshape(tok_count, num_heads * head_dim)
    x_mid = (x_f + jnp.dot(attn_flat, w_out, preferred_element_type=jnp.float32) + b_out.astype(jnp.float32)).astype(jnp.bfloat16)
    return x_mid, key_new, value_new


def router_gates(h_two, w_router, expert_one, expert_two, eligible):
    logits = jnp.dot(h_two, w_router, preferred_element_type=jnp.float32)
    expert_ids = jnp.arange(logits.shape[1])[None, :]
    hit_one = expert_ids == expert_one[:, None]
    hit_two = expert_ids == expert_two[:, None]
    keep_one = eligible == 1
    keep_two = keep_one & jnp.logical_not(hit_one)
    prob_one = jax.nn.softmax(jnp.where(keep_one, logits, -jnp.inf), axis=-1)
    prob_two = jax.nn.softmax(jnp.where(keep_two, logits, -jnp.inf), axis=-1)
    gate_one = jnp.sum(jnp.where(hit_one, prob_one, 0.0), axis=-1)
    gate_two = jnp.sum(jnp.where(hit_two, prob_two, 0.0), axis=-1)
    return gate_one, gate_two


def expert_mlp(expert_in, w_gate, w_up, w_down):
    u_val = jnp.einsum('md,edf->emf', expert_in, w_gate, preferred_element_type=jnp.float32)
    v_val = jnp.einsum('md,edf->emf', expert_in, w_up, preferred_element_type=jnp.float32)
    z_val = (jax.nn.silu(u_val) * v_val).astype(jnp.bfloat16)
    return jnp.einsum('emf,efd->emd', z_val, w_down, preferred_element_type=jnp.float32).astype(jnp.bfloat16)


def solution(mesh):
    groups = mesh.shape['ep']

    def local_step(tokens, k_cache, v_cache, positions, expert_one, expert_two, eligible, ln1_gain, ln1_bias, w_query, b_query, w_key, b_key, w_value, b_value, w_out, b_out, ln2_gain, ln2_bias, w_router, w_gate, w_up, w_down):
        x_mid, key_new, value_new = attention_block(tokens, k_cache, v_cache, positions, ln1_gain, ln1_bias, w_query, b_query, w_key, b_key, w_value, b_value, w_out, b_out)
        h_two = layer_norm(x_mid.astype(jnp.float32), ln2_gain, ln2_bias).astype(jnp.bfloat16)
        gate_one, gate_two = router_gates(h_two, w_router, expert_one, expert_two, eligible)
        tok_count, d_model = h_two.shape
        local_experts = w_gate.shape[0]
        all_rows = lax.all_gather(h_two, 'ep', axis=0, tiled=True)
        choices = lax.all_gather(jnp.stack([expert_one, expert_two], axis=1), 'ep', axis=0, tiled=True)
        expert_out = expert_mlp(all_rows, w_gate, w_up, w_down)
        local_ids = lax.axis_index('ep') * local_experts + jnp.arange(local_experts, dtype=jnp.int32)
        slots = []
        for slot in range(2):
            hit = choices[:, slot][None, :] == local_ids[:, None]
            slots.append(jnp.sum(jnp.where(hit[:, :, None], expert_out, 0), axis=0, dtype=jnp.bfloat16))
        by_owner = jnp.stack([x.reshape(groups, tok_count, d_model) for x in slots], axis=1).reshape(groups * 2 * tok_count, d_model)
        mine = lax.psum_scatter(by_owner, 'ep', scatter_dimension=0, tiled=True)
        out_one = mine[:tok_count]
        out_two = mine[tok_count:]
        y_sum = gate_one[:, None] * out_one.astype(jnp.float32) + gate_two[:, None] * out_two.astype(jnp.float32)
        tokens_out = (x_mid.astype(jnp.float32) + y_sum).astype(jnp.bfloat16)
        return tokens_out, key_new, value_new

    row_spec = P('ep', None)
    cache_spec = P('ep', None, None, None)
    vec_spec = P('ep')
    rep_one = P(None)
    rep_two = P(None, None)
    expert_spec = P('ep', None, None)
    in_specs = (row_spec, cache_spec, cache_spec, vec_spec, vec_spec, vec_spec, row_spec, rep_one, rep_one, rep_two, rep_one, rep_two, rep_one, rep_two, rep_one, rep_two, rep_one, rep_one, rep_one, rep_two, expert_spec, expert_spec, expert_spec)
    out_specs = (row_spec, expert_spec, expert_spec)
    return jax.shard_map(local_step, mesh=mesh, in_specs=in_specs, out_specs=out_specs, check_vma=False)
```

```python
import jax
import jax.numpy as jnp
from jax import lax
from jax.experimental import pallas as pl
from jax.experimental.pallas import tpu as pltpu
from jax.sharding import PartitionSpec as P

ROPE_BASE = 10000.0
LN_EPS = 1e-5


def rope_tables(positions, head_dim):
    half_dim = head_dim // 2
    inv_freq = ROPE_BASE ** (jnp.arange(half_dim, dtype=jnp.float32) * (-2.0 / head_dim))
    angles = positions.astype(jnp.float32)[:, None] * inv_freq[None, :]
    angles = jnp.concatenate([angles, angles], axis=-1)
    return jnp.cos(angles), jnp.sin(angles)


def norm_rows(x_val, gain, bias):
    mean_val = jnp.mean(x_val, axis=-1, keepdims=True)
    centered = x_val - mean_val
    var_val = jnp.mean(centered * centered, axis=-1, keepdims=True)
    return centered * lax.rsqrt(var_val + LN_EPS) * gain.astype(jnp.float32) + bias.astype(jnp.float32)


def qkv_kernel(x_ref, gain_ref, bias_ref, cos_ref, sin_ref, wq_ref, wk_ref, wv_ref, bq_ref, bk_ref, bv_ref, q_ref, k_ref, v_ref, h_ref):
    @pl.when(pl.program_id(0) == 0)
    def _():
        h_ref[...] = norm_rows(x_ref[...].astype(jnp.float32), gain_ref[...], bias_ref[...]).astype(jnp.bfloat16)

    h_val = h_ref[...]
    head_dim = cos_ref.shape[1]
    cos_tab, sin_tab = cos_ref[...], sin_ref[...]
    for w_ref, b_ref, o_ref in ((wq_ref, bq_ref, q_ref), (wk_ref, bk_ref, k_ref)):
        lin = jnp.dot(h_val, w_ref[...], preferred_element_type=jnp.float32) + b_ref[...].astype(jnp.float32)
        for c in range(lin.shape[1] // head_dim):
            part = lin[:, c * head_dim:(c + 1) * head_dim]
            rot = part * cos_tab + pltpu.roll(part, head_dim // 2, 1) * sin_tab
            o_ref[:, c * head_dim:(c + 1) * head_dim] = rot.astype(jnp.bfloat16)
    lin = jnp.dot(h_val, wv_ref[...], preferred_element_type=jnp.float32) + bv_ref[...].astype(jnp.float32)
    v_ref[...] = lin.astype(jnp.bfloat16)


def qkv_call(tokens, gain, bias, cos_tab, sin_signed, w_query, b_query, w_key, b_key, w_value, b_value):
    rows, d_model = tokens.shape
    cols = w_query.shape[1]
    tile = 256
    whole = lambda shape: pl.BlockSpec(shape, lambda i: (0,) * len(shape))
    wide = pl.BlockSpec((d_model, tile), lambda i: (0, i))
    slim = pl.BlockSpec((1, tile), lambda i: (0, i))
    out = pl.BlockSpec((rows, tile), lambda i: (0, i))
    shape = jax.ShapeDtypeStruct((rows, cols), jnp.bfloat16)
    row = lambda t: t.reshape(1, -1)
    return pl.pallas_call(
        qkv_kernel,
        grid=(cols // tile,),
        in_specs=[whole((rows, d_model)), whole((1, d_model)), whole((1, d_model)), whole(cos_tab.shape), whole(cos_tab.shape), wide, wide, wide, slim, slim, slim],
        out_specs=[out, out, out],
        out_shape=[shape, shape, shape],
        scratch_shapes=[pltpu.VMEM((rows, d_model), jnp.bfloat16)],
        compiler_params=pltpu.CompilerParams(vmem_limit_bytes=40 * 2 ** 20),
        cost_estimate=pl.CostEstimate(flops=6 * rows * d_model * cols, bytes_accessed=6 * d_model * cols, transcendentals=0),
        name='qkv',
    )(tokens, row(gain), row(bias), cos_tab, sin_signed, w_query, w_key, w_value, row(b_query), row(b_key), row(b_value))


GROUP = 4
SLOTS = 3
STEP = 16


def attend_kernel(order_ref, pos_ref, q_ref, kn_ref, vn_ref, k_hbm, v_hbm, out_ref, k_buf, v_buf, sid_ref, sems):
    rows, heads, head_dim = q_ref.shape
    seq = k_hbm.shape[1]
    groups = rows // GROUP
    scale = head_dim ** -0.5
    key_id = lax.broadcasted_iota(jnp.int32, sid_ref.shape, 1)
    row_id = lax.broadcasted_iota(jnp.int32, sid_ref.shape, 0)
    sid_ref[...] = jnp.where(lax.rem(key_id, heads) == row_id, lax.div(key_id, heads), seq)
    v_buf[...] = jnp.zeros_like(v_buf)

    def copies(grp, act):
        slot = lax.rem(grp, SLOTS)
        for i in range(GROUP):
            tok = order_ref[grp * GROUP + i]
            need = (pos_ref[tok] + 3) // 4 * 4
            size = seq
            while size >= 4:
                first = need // (2 * size) * (2 * size)

                @pl.when((need // size) % 2 == 1)
                def _(size=size, first=first):
                    src = pl.ds(first, size)
                    for hbm, buf, n in ((k_hbm, k_buf, 0), (v_hbm, v_buf, 1)):
                        copy = pltpu.make_async_copy(hbm.at[tok, src], buf.at[slot, i, src], sems.at[n, slot])
                        if act == 'start':
                            copy.start()
                        else:
                            copy.wait()
                size //= 2

    def compute(grp, steps):
        slot = lax.rem(grp, SLOTS)
        keys = steps * STEP * heads
        toks = [order_ref[grp * GROUP + i] for i in range(GROUP)]
        q_val = [q_ref[t] for t in toks]
        scores = []
        for i in range(GROUP):
            k_val = k_buf[slot, i, pl.ds(0, steps * STEP)].reshape(keys, head_dim)
            raw = lax.dot_general(q_val[i], k_val, (((1,), (1,)), ((), ())), preferred_element_type=jnp.float32)
            scores.append(jnp.where(sid_ref[:, :keys] < pos_ref[toks[i]], raw * scale, -jnp.inf))
        for i in range(GROUP):
            t = toks[i]
            s_new = jnp.sum(q_val[i].astype(jnp.float32) * kn_ref[t].astype(jnp.float32), axis=-1, keepdims=True) * scale
            top = jnp.maximum(jnp.max(scores[i], axis=-1, keepdims=True), s_new)
            e_val = jnp.exp(scores[i] - top)
            e_new = jnp.exp(s_new - top)
            inv = 1.0 / (jnp.sum(e_val, axis=-1, keepdims=True) + e_new)
            p_val = (e_val * inv).astype(jnp.bfloat16)
            p_new = (e_new * inv).astype(jnp.bfloat16).astype(jnp.float32)
            v_val = v_buf[slot, i, pl.ds(0, steps * STEP)].reshape(keys, head_dim)
            res = jnp.dot(p_val, v_val, preferred_element_type=jnp.float32) + p_new * vn_ref[t].astype(jnp.float32)
            out_ref[t] = res.astype(jnp.bfloat16)

    for g in range(SLOTS - 1):
        copies(g, 'start')

    @pl.loop(0, groups)
    def _(grp):
        @pl.when(grp + SLOTS - 1 < groups)
        def _():
            copies(grp + SLOTS - 1, 'start')

        copies(grp, 'wait')
        most = pos_ref[order_ref[grp * GROUP]]
        for i in range(1, GROUP):
            most = jnp.maximum(most, pos_ref[order_ref[grp * GROUP + i]])
        steps = jnp.maximum((most + STEP - 1) // STEP, 1)
        for n in range(1, seq // STEP + 1):
            @pl.when(steps == n)
            def _(n=n):
                compute(grp, n)


def attend_call(order, positions, q_rot, key_new, value_new, k_cache, v_cache):
    rows, seq, heads, head_dim = k_cache.shape
    vmem = pl.BlockSpec(memory_space=pltpu.VMEM)
    smem = pl.BlockSpec(memory_space=pltpu.SMEM)
    hbm = pl.BlockSpec(memory_space=pl.ANY)
    return pl.pallas_call(
        attend_kernel,
        in_specs=[smem, smem, vmem, vmem, vmem, hbm, hbm],
        out_specs=vmem,
        out_shape=jax.ShapeDtypeStruct((rows, heads, head_dim), jnp.bfloat16),
        scratch_shapes=[
            pltpu.VMEM((SLOTS, GROUP, seq, heads, head_dim), jnp.bfloat16),
            pltpu.VMEM((SLOTS, GROUP, seq, heads, head_dim), jnp.bfloat16),
            pltpu.VMEM((heads, seq * heads), jnp.int32),
            pltpu.SemaphoreType.DMA((2, SLOTS)),
        ],
        compiler_params=pltpu.CompilerParams(vmem_limit_bytes=40 * 2 ** 20),
        cost_estimate=pl.CostEstimate(flops=4 * rows * seq * heads * heads * head_dim, bytes_accessed=2 * rows * seq * heads * head_dim, transcendentals=0),
        name='attend',
    )(order, positions, q_rot, key_new, value_new, k_cache, v_cache)


def out_kernel(tile, a_ref, x_ref, b_ref, gain_ref, bias_ref, wr_ref, one_ref, two_ref, elig_ref, w_ref, mid_ref, h_ref, gate_ref, mid_all):
    i = pl.program_id(0)
    cols = pl.ds(pl.multiple_of(i * tile, tile), tile)
    mid = x_ref[:, cols].astype(jnp.float32) + jnp.dot(a_ref[...], w_ref[...], preferred_element_type=jnp.float32) + b_ref[:, cols].astype(jnp.float32)
    mid = mid.astype(jnp.bfloat16)
    mid_ref[...] = mid
    mid_all[:, cols] = mid

    @pl.when(i == pl.num_programs(0) - 1)
    def _():
        h_two = norm_rows(mid_all[...].astype(jnp.float32), gain_ref[...], bias_ref[...]).astype(jnp.bfloat16)
        h_ref[...] = h_two
        logits = jnp.dot(h_two, wr_ref[...], preferred_element_type=jnp.float32)
        ids = lax.broadcasted_iota(jnp.int32, logits.shape, 1)
        hit_one = ids == one_ref[...]
        hit_two = ids == two_ref[...]
        keep_one = elig_ref[...] == 1
        gates = []
        for keep, hit in ((keep_one, hit_one), (keep_one & jnp.logical_not(hit_one), hit_two)):
            masked = jnp.where(keep, logits, -jnp.inf)
            e_val = jnp.exp(masked - jnp.max(masked, axis=-1, keepdims=True))
            top = jnp.sum(jnp.where(hit, e_val, 0.0), axis=-1, keepdims=True)
            gates.append(top / jnp.sum(e_val, axis=-1, keepdims=True))
        lane = lax.broadcasted_iota(jnp.int32, gate_ref.shape, 1)
        gate_ref[...] = jnp.where(lane == 0, gates[0], jnp.where(lane == 1, gates[1], 0.0))


def out_call(attn_flat, tokens, b_out, gain, bias, w_router, expert_one, expert_two, eligible, w_out):
    rows, d_model = tokens.shape
    tile = 512
    whole = lambda shape: pl.BlockSpec(shape, lambda i: (0,) * len(shape))
    row = lambda t: t.reshape(1, -1)
    col = lambda t: t.reshape(-1, 1)
    return pl.pallas_call(
        lambda *refs: out_kernel(tile, *refs),
        grid=(d_model // tile,),
        in_specs=[whole(attn_flat.shape), whole(tokens.shape), whole((1, d_model)), whole((1, d_model)), whole((1, d_model)), whole(w_router.shape), whole((rows, 1)), whole((rows, 1)), whole(eligible.shape), pl.BlockSpec((w_out.shape[0], tile), lambda i: (0, i))],
        out_specs=[pl.BlockSpec((rows, tile), lambda i: (0, i)), whole((rows, d_model)), whole((rows, 128))],
        out_shape=[jax.ShapeDtypeStruct((rows, d_model), jnp.bfloat16), jax.ShapeDtypeStruct((rows, d_model), jnp.bfloat16), jax.ShapeDtypeStruct((rows, 128), jnp.float32)],
        scratch_shapes=[pltpu.VMEM((rows, d_model), jnp.bfloat16)],
        compiler_params=pltpu.CompilerParams(vmem_limit_bytes=40 * 2 ** 20),
        cost_estimate=pl.CostEstimate(flops=2 * rows * d_model * d_model, bytes_accessed=2 * d_model * d_model, transcendentals=0),
        name='project',
    )(attn_flat, tokens, row(b_out), row(gain), row(bias), w_router, col(expert_one), col(expert_two), eligible, w_out)


def attention_order(positions):
    ids = jnp.arange(positions.shape[0], dtype=jnp.int32)
    ahead = (positions[None, :] > positions[:, None]) | ((positions[None, :] == positions[:, None]) & (ids[None, :] < ids[:, None]))
    rank = jnp.sum(ahead.astype(jnp.int32), axis=1)
    return jnp.sum(jnp.where(rank[:, None] == ids[None, :], ids[:, None], 0), axis=0)


def expert_mlp(expert_in, w_gate, w_up, w_down):
    u_val = jnp.einsum('md,edf->emf', expert_in, w_gate, preferred_element_type=jnp.float32)
    v_val = jnp.einsum('md,edf->emf', expert_in, w_up, preferred_element_type=jnp.float32)
    z_val = (jax.nn.silu(u_val) * v_val).astype(jnp.bfloat16)
    return jnp.einsum('emf,efd->emd', z_val, w_down, preferred_element_type=jnp.float32).astype(jnp.bfloat16)


def solution(mesh):
    groups = mesh.shape['ep']

    def local_step(tokens, k_cache, v_cache, positions, expert_one, expert_two, eligible, ln1_gain, ln1_bias, w_query, b_query, w_key, b_key, w_value, b_value, w_out, b_out, ln2_gain, ln2_bias, w_router, w_gate, w_up, w_down):
        tok_count, seq_len, heads, head_dim = k_cache.shape
        d_model = tokens.shape[1]
        cos_tab, sin_tab = rope_tables(positions, head_dim)
        sign = jnp.where(jnp.arange(head_dim) < head_dim // 2, -1.0, 1.0)
        q_flat, k_flat, v_flat = qkv_call(tokens, ln1_gain, ln1_bias, cos_tab, sin_tab * sign[None, :], w_query, b_query, w_key, b_key, w_value, b_value)
        split = lambda t: t.reshape(tok_count, heads, head_dim)
        key_new, value_new = split(k_flat), split(v_flat)
        attn = attend_call(attention_order(positions), positions, split(q_flat), key_new, value_new, k_cache, v_cache)
        x_mid, h_two, gates = out_call(attn.reshape(tok_count, heads * head_dim), tokens, b_out, ln2_gain, ln2_bias, w_router, expert_one, expert_two, eligible, w_out)
        gate_one, gate_two = gates[:, 0], gates[:, 1]
        local_experts = w_gate.shape[0]
        all_rows = lax.all_gather(h_two, 'ep', axis=0, tiled=True)
        choices = lax.all_gather(jnp.stack([expert_one, expert_two], axis=1), 'ep', axis=0, tiled=True)
        expert_out = expert_mlp(all_rows, w_gate, w_up, w_down)
        local_ids = lax.axis_index('ep') * local_experts + jnp.arange(local_experts, dtype=jnp.int32)
        slots = []
        for slot in range(2):
            hit = choices[:, slot][None, :] == local_ids[:, None]
            slots.append(jnp.sum(jnp.where(hit[:, :, None], expert_out, 0), axis=0, dtype=jnp.bfloat16))
        by_owner = jnp.stack([x.reshape(groups, tok_count, d_model) for x in slots], axis=1).reshape(groups * 2 * tok_count, d_model)
        mine = lax.psum_scatter(by_owner, 'ep', scatter_dimension=0, tiled=True)
        out_one = mine[:tok_count]
        out_two = mine[tok_count:]
        y_sum = gate_one[:, None] * out_one.astype(jnp.float32) + gate_two[:, None] * out_two.astype(jnp.float32)
        tokens_out = (x_mid.astype(jnp.float32) + y_sum).astype(jnp.bfloat16)
        return tokens_out, key_new, value_new

    row_spec = P('ep', None)
    cache_spec = P('ep', None, None, None)
    vec_spec = P('ep')
    rep_one = P(None)
    rep_two = P(None, None)
    expert_spec = P('ep', None, None)
    in_specs = (row_spec, cache_spec, cache_spec, vec_spec, vec_spec, vec_spec, row_spec, rep_one, rep_one, rep_two, rep_one, rep_two, rep_one, rep_two, rep_one, rep_two, rep_one, rep_one, rep_one, rep_two, expert_spec, expert_spec, expert_spec)
    out_specs = (row_spec, expert_spec, expert_spec)
    return jax.shard_map(local_step, mesh=mesh, in_specs=in_specs, out_specs=out_specs, check_vma=False)
```

```python
import jax
import jax.numpy as jnp
from jax import lax
from jax.experimental import pallas as pl
from jax.experimental.pallas import tpu as pltpu
from jax.sharding import PartitionSpec as P

ROPE_BASE = 10000.0
LN_EPS = 1e-5


def rope_tables(positions, head_dim):
    half_dim = head_dim // 2
    inv_freq = ROPE_BASE ** (jnp.arange(half_dim, dtype=jnp.float32) * (-2.0 / head_dim))
    angles = positions.astype(jnp.float32)[:, None] * inv_freq[None, :]
    angles = jnp.concatenate([angles, angles], axis=-1)
    return jnp.cos(angles), jnp.sin(angles)


def norm_rows(x_val, gain, bias):
    mean_val = jnp.mean(x_val, axis=-1, keepdims=True)
    centered = x_val - mean_val
    var_val = jnp.mean(centered * centered, axis=-1, keepdims=True)
    return centered * lax.rsqrt(var_val + LN_EPS) * gain.astype(jnp.float32) + bias.astype(jnp.float32)


def row_stack(vectors):
    which = lax.broadcasted_iota(jnp.int32, (len(vectors), vectors[0].shape[0]), 0)
    out = jnp.zeros((len(vectors), vectors[0].shape[0]), vectors[0].dtype)
    for n, vec in enumerate(vectors):
        out = jnp.where(which == n, vec[None, :], out)
    return out


def qkv_kernel(x_ref, norm_ref, cos_ref, sin_ref, wq_ref, wk_ref, wv_ref, b_ref, q_ref, k_ref, v_ref, h_ref):
    @pl.when(pl.program_id(0) == 0)
    def _():
        h_ref[...] = norm_rows(x_ref[...].astype(jnp.float32), norm_ref[0:1], norm_ref[1:2]).astype(jnp.bfloat16)

    h_val = h_ref[...]
    head_dim = cos_ref.shape[1]
    cos_tab, sin_tab = cos_ref[...], sin_ref[...]
    for w_ref, n, o_ref in ((wq_ref, 2, q_ref), (wk_ref, 3, k_ref)):
        lin = jnp.dot(h_val, w_ref[...], preferred_element_type=jnp.float32) + b_ref[n:n + 1].astype(jnp.float32)
        for c in range(lin.shape[1] // head_dim):
            part = lin[:, c * head_dim:(c + 1) * head_dim]
            rot = part * cos_tab + pltpu.roll(part, head_dim // 2, 1) * sin_tab
            o_ref[:, c * head_dim:(c + 1) * head_dim] = rot.astype(jnp.bfloat16)
    lin = jnp.dot(h_val, wv_ref[...], preferred_element_type=jnp.float32) + b_ref[4:5].astype(jnp.float32)
    v_ref[...] = lin.astype(jnp.bfloat16)


def qkv_call(tokens, vectors, cos_tab, sin_signed, w_query, w_key, w_value):
    rows, d_model = tokens.shape
    cols = w_query.shape[1]
    tile = 256
    whole = lambda shape: pl.BlockSpec(shape, lambda i: (0,) * len(shape))
    wide = pl.BlockSpec((d_model, tile), lambda i: (0, i))
    slim = pl.BlockSpec((8, tile), lambda i: (0, i))
    out = pl.BlockSpec((rows, tile), lambda i: (0, i))
    shape = jax.ShapeDtypeStruct((rows, cols), jnp.bfloat16)
    return pl.pallas_call(
        qkv_kernel,
        grid=(cols // tile,),
        in_specs=[whole((rows, d_model)), whole((8, d_model)), whole(cos_tab.shape), whole(cos_tab.shape), wide, wide, wide, slim],
        out_specs=[out, out, out],
        out_shape=[shape, shape, shape],
        scratch_shapes=[pltpu.VMEM((rows, d_model), jnp.bfloat16)],
        compiler_params=pltpu.CompilerParams(vmem_limit_bytes=40 * 2 ** 20),
        cost_estimate=pl.CostEstimate(flops=6 * rows * d_model * cols, bytes_accessed=6 * d_model * cols, transcendentals=0),
        name='qkv',
    )(tokens, vectors, cos_tab, sin_signed, w_query, w_key, w_value, vectors)


GROUP = 4
SLOTS = 3
STEP = 16


def attend_kernel(order_ref, pos_ref, q_ref, kn_ref, vn_ref, k_hbm, v_hbm, out_ref, k_buf, v_buf, sid_ref, sems):
    rows, heads, head_dim = q_ref.shape
    seq = k_hbm.shape[1]
    groups = rows // GROUP
    scale = head_dim ** -0.5
    key_id = lax.broadcasted_iota(jnp.int32, sid_ref.shape, 1)
    row_id = lax.broadcasted_iota(jnp.int32, sid_ref.shape, 0)
    sid_ref[...] = jnp.where(lax.rem(key_id, heads) == row_id, lax.div(key_id, heads), seq)
    v_buf[...] = jnp.zeros_like(v_buf)

    def copies(grp, act):
        slot = lax.rem(grp, SLOTS)
        for i in range(GROUP):
            tok = order_ref[grp * GROUP + i]
            need = (pos_ref[tok] + 3) // 4 * 4
            size = seq
            while size >= 4:
                first = need // (2 * size) * (2 * size)

                @pl.when((need // size) % 2 == 1)
                def _(size=size, first=first):
                    src = pl.ds(first, size)
                    for hbm, buf, n in ((k_hbm, k_buf, 0), (v_hbm, v_buf, 1)):
                        copy = pltpu.make_async_copy(hbm.at[tok, src], buf.at[slot, i, src], sems.at[n, slot])
                        if act == 'start':
                            copy.start()
                        else:
                            copy.wait()
                size //= 2

    def compute(grp, steps):
        slot = lax.rem(grp, SLOTS)
        keys = steps * STEP * heads
        toks = [order_ref[grp * GROUP + i] for i in range(GROUP)]
        q_val = [q_ref[t] for t in toks]
        scores = []
        for i in range(GROUP):
            k_val = k_buf[slot, i, pl.ds(0, steps * STEP)].reshape(keys, head_dim)
            raw = lax.dot_general(q_val[i], k_val, (((1,), (1,)), ((), ())), preferred_element_type=jnp.float32)
            scores.append(jnp.where(sid_ref[:, :keys] < pos_ref[toks[i]], raw * scale, -jnp.inf))
        for i in range(GROUP):
            t = toks[i]
            s_new = jnp.sum(q_val[i].astype(jnp.float32) * kn_ref[t].astype(jnp.float32), axis=-1, keepdims=True) * scale
            top = jnp.maximum(jnp.max(scores[i], axis=-1, keepdims=True), s_new)
            e_val = jnp.exp(scores[i] - top)
            e_new = jnp.exp(s_new - top)
            inv = 1.0 / (jnp.sum(e_val, axis=-1, keepdims=True) + e_new)
            p_val = (e_val * inv).astype(jnp.bfloat16)
            p_new = (e_new * inv).astype(jnp.bfloat16).astype(jnp.float32)
            v_val = v_buf[slot, i, pl.ds(0, steps * STEP)].reshape(keys, head_dim)
            res = jnp.dot(p_val, v_val, preferred_element_type=jnp.float32) + p_new * vn_ref[t].astype(jnp.float32)
            out_ref[t] = res.astype(jnp.bfloat16)

    for g in range(SLOTS - 1):
        copies(g, 'start')

    @pl.loop(0, groups)
    def _(grp):
        @pl.when(grp + SLOTS - 1 < groups)
        def _():
            copies(grp + SLOTS - 1, 'start')

        copies(grp, 'wait')
        most = pos_ref[order_ref[grp * GROUP]]
        for i in range(1, GROUP):
            most = jnp.maximum(most, pos_ref[order_ref[grp * GROUP + i]])
        steps = jnp.maximum((most + STEP - 1) // STEP, 1)
        for n in range(1, seq // STEP + 1):
            @pl.when(steps == n)
            def _(n=n):
                compute(grp, n)


def attend_call(order, positions, q_rot, key_new, value_new, k_cache, v_cache):
    rows, seq, heads, head_dim = k_cache.shape
    vmem = pl.BlockSpec(memory_space=pltpu.VMEM)
    smem = pl.BlockSpec(memory_space=pltpu.SMEM)
    hbm = pl.BlockSpec(memory_space=pl.ANY)
    return pl.pallas_call(
        attend_kernel,
        in_specs=[smem, smem, vmem, vmem, vmem, hbm, hbm],
        out_specs=vmem,
        out_shape=jax.ShapeDtypeStruct((rows, heads, head_dim), jnp.bfloat16),
        scratch_shapes=[
            pltpu.VMEM((SLOTS, GROUP, seq, heads, head_dim), jnp.bfloat16),
            pltpu.VMEM((SLOTS, GROUP, seq, heads, head_dim), jnp.bfloat16),
            pltpu.VMEM((heads, seq * heads), jnp.int32),
            pltpu.SemaphoreType.DMA((2, SLOTS)),
        ],
        compiler_params=pltpu.CompilerParams(vmem_limit_bytes=40 * 2 ** 20),
        cost_estimate=pl.CostEstimate(flops=4 * rows * seq * heads * heads * head_dim, bytes_accessed=2 * rows * seq * heads * head_dim, transcendentals=0),
        name='attend',
    )(order, positions, q_rot, key_new, value_new, k_cache, v_cache)


def out_kernel(tile, a_ref, x_ref, vec_ref, wr_ref, pick_ref, w_ref, mid_ref, h_ref, gate_ref, mid_all):
    i = pl.program_id(0)
    cols = pl.ds(pl.multiple_of(i * tile, tile), tile)
    mid = x_ref[:, cols].astype(jnp.float32) + jnp.dot(a_ref[...], w_ref[...], preferred_element_type=jnp.float32) + vec_ref[5:6, cols].astype(jnp.float32)
    mid = mid.astype(jnp.bfloat16)
    mid_ref[...] = mid
    mid_all[:, cols] = mid

    @pl.when(i == pl.num_programs(0) - 1)
    def _():
        h_two = norm_rows(mid_all[...].astype(jnp.float32), vec_ref[6:7], vec_ref[7:8]).astype(jnp.bfloat16)
        lanes = lax.broadcasted_iota(jnp.int32, (h_two.shape[0], 128), 1)
        pick_val = jnp.transpose(pick_ref[...].astype(jnp.float32))
        picks = jnp.where(lanes < 2, pick_val, 0.0)
        h_ref[:, :h_two.shape[1]] = h_two
        h_ref[:, h_two.shape[1]:] = picks.astype(jnp.bfloat16)
        logits = lax.dot_general(h_two, wr_ref[...], (((1,), (1,)), ((), ())), preferred_element_type=jnp.float32)
        ids = lax.broadcasted_iota(jnp.int32, logits.shape, 1).astype(jnp.float32)
        hit_one = ids == pick_val[:, 0:1]
        hit_two = ids == pick_val[:, 1:2]
        keep_one = pick_val[:, 2:2 + logits.shape[1]] == 1.0
        gates = []
        for keep, hit in ((keep_one, hit_one), (keep_one & jnp.logical_not(hit_one), hit_two)):
            masked = jnp.where(keep, logits, -jnp.inf)
            e_val = jnp.exp(masked - jnp.max(masked, axis=-1, keepdims=True))
            top = jnp.sum(jnp.where(hit, e_val, 0.0), axis=-1, keepdims=True)
            gates.append(top / jnp.sum(e_val, axis=-1, keepdims=True))
        lane = lax.broadcasted_iota(jnp.int32, gate_ref.shape, 1)
        gate_ref[...] = jnp.where(lane == 0, gates[0], jnp.where(lane == 1, gates[1], 0.0))


def out_call(attn_flat, tokens, vectors, w_router, picks, w_out):
    rows, d_model = tokens.shape
    tile = 512
    whole = lambda shape: pl.BlockSpec(shape, lambda i: (0,) * len(shape))
    return pl.pallas_call(
        lambda *refs: out_kernel(tile, *refs),
        grid=(d_model // tile,),
        in_specs=[whole(attn_flat.shape), whole(tokens.shape), whole((8, d_model)), whole(w_router.shape), whole(picks.shape), pl.BlockSpec((w_out.shape[0], tile), lambda i: (0, i))],
        out_specs=[pl.BlockSpec((rows, tile), lambda i: (0, i)), whole((rows, d_model + 128)), whole((rows, 128))],
        out_shape=[jax.ShapeDtypeStruct((rows, d_model), jnp.bfloat16), jax.ShapeDtypeStruct((rows, d_model + 128), jnp.bfloat16), jax.ShapeDtypeStruct((rows, 128), jnp.float32)],
        scratch_shapes=[pltpu.VMEM((rows, d_model), jnp.bfloat16)],
        compiler_params=pltpu.CompilerParams(vmem_limit_bytes=40 * 2 ** 20),
        cost_estimate=pl.CostEstimate(flops=2 * rows * d_model * d_model, bytes_accessed=2 * d_model * d_model, transcendentals=0),
        name='project',
    )(attn_flat, tokens, vectors, w_router, picks, w_out)


def attention_order(positions):
    ids = jnp.arange(positions.shape[0], dtype=jnp.int32)
    ahead = (positions[None, :] > positions[:, None]) | ((positions[None, :] == positions[:, None]) & (ids[None, :] < ids[:, None]))
    rank = jnp.sum(ahead.astype(jnp.int32), axis=1)
    return jnp.sum(jnp.where(rank[:, None] == ids[None, :], ids[:, None], 0), axis=0)


def moe_kernel(h_in, x_hbm, gate_ref, wg_hbm, wu_hbm, wd_hbm, out_hbm, hb, wg, wu, wd, xblk, zt_ref, z_ref, acc, stg, d2d, p1a, p1b, p2a, p2b, wsem, xsem, gsend, grecv, dsend, drecv, rsend, rrecv, credit):
    me = lax.axis_index('ep')
    core = lax.rem(me, 2)
    x_pos = lax.rem(lax.div(me, 2), 2)
    y_pos = lax.div(me, 4)
    partner = me + 1 - 2 * core
    xn = me + 2 - 4 * x_pos
    yn = me + 4 - 8 * y_pos
    rows = h_in.shape[0]
    half_rows = rows // 2
    d_model = x_hbm.shape[1]
    half = d_model // 2
    ff = wd.shape[1]
    tile = 512
    zt_ref[...] = jnp.zeros_like(zt_ref)
    mesh_id = pl.DeviceIdType.MESH

    def remote(src, dst, send, recv, dev):
        return pltpu.make_async_remote_copy(src_ref=src, dst_ref=dst, send_sem=send, recv_sem=recv, device_id=(dev,), device_id_type=mesh_id)

    low, high = pl.ds(0, half_rows), pl.ds(half_rows, half_rows)
    gather = [
        remote(h_in, hb.at[1], gsend.at[0], grecv.at[0], partner),
        remote(h_in, hb.at[2], gsend.at[1], grecv.at[1], xn),
        remote(h_in, hb.at[4], gsend.at[2], grecv.at[2], yn),
        remote(hb.at[2], hb.at[3], gsend.at[3], grecv.at[3], partner),
        remote(hb.at[2, low], hb.at[6, low], gsend.at[4], grecv.at[4], yn),
        remote(hb.at[4], hb.at[5], gsend.at[5], grecv.at[5], partner),
        remote(hb.at[4, high], hb.at[6, high], gsend.at[6], grecv.at[6], xn),
        remote(hb.at[6, low], hb.at[7, low], gsend.at[7], grecv.at[7], partner),
        remote(hb.at[6, high], hb.at[7, high], gsend.at[8], grecv.at[8], partner),
    ]
    scatter = [
        remote(acc.at[1, 0], p1a.at[0], rsend.at[0], rrecv.at[0], xn),
        remote(acc.at[2, 1], p1b.at[0], rsend.at[1], rrecv.at[1], yn),
        remote(acc.at[3, 0], p1a.at[1], rsend.at[2], rrecv.at[2], xn),
        remote(acc.at[3, 1], p1b.at[1], rsend.at[3], rrecv.at[3], yn),
        remote(acc.at[1, 1], p2b, rsend.at[4], rrecv.at[4], xn),
        remote(acc.at[2, 0], p2a, rsend.at[5], rrecv.at[5], yn),
    ]

    def weight(e):
        return [pltpu.make_async_copy(hbm.at[e], buf.at[e], wsem.at[n, e]) for n, (hbm, buf) in enumerate(((wg_hbm, wg), (wu_hbm, wu), (wd_hbm, wd)))]

    barrier = pltpu.get_barrier_semaphore()
    for dev in (partner, xn, yn):
        pl.semaphore_signal(barrier, inc=1, device_id=(dev,), device_id_type=mesh_id)
    for e in range(2):
        for copy in weight(e):
            copy.start()
    pl.semaphore_wait(barrier, 3)
    for i in (1, 2, 0):
        gather[i].start()

    def load(first, second):
        copies = [pltpu.make_async_copy(src, xblk.at[pl.ds(n * rows, rows)], xsem.at[n]) for n, src in enumerate((first, second))]
        for copy in copies:
            copy.start()
        for copy in copies:
            copy.wait()

    def merge(dst, src):
        @pl.loop(0, 2 * (rows // 32))
        def _(i):
            slot = lax.div(i, rows // 32)
            at = pl.ds(pl.multiple_of(lax.rem(i, rows // 32) * 32, 32), 32)
            dst[slot, at] = dst[slot, at] + src[slot, at]

    def shared(r, part):
        return remote(stg.at[part], d2d.at[lax.rem(r, 2), part], dsend.at[part], drecv.at[r, part], partner)

    @pl.loop(0, 4)
    def _(r):
        @pl.when(r == 0)
        def _():
            gather[0].wait_recv()
            load(h_in, hb.at[1])

        @pl.when(r == 1)
        def _():
            gather[1].wait_recv()
            gather[3].start()
            gather[4].start()
            gather[2].wait_recv()
            gather[5].start()
            gather[6].start()
            gather[3].wait_recv()
            load(hb.at[2], hb.at[3])

        @pl.when(r == 2)
        def _():
            gather[5].wait_recv()
            load(hb.at[4], hb.at[5])

        @pl.when(r == 3)
        def _():
            gather[7].wait_recv()
            gather[8].wait_recv()
            load(hb.at[6], hb.at[7])

        @pl.loop(0, 2)
        def _(e):
            @pl.when(r == 0)
            def _():
                for copy in weight(e)[:2]:
                    copy.wait()

            x_val = xblk[:, :d_model]
            dims = (((1,), (1,)), ((), ()))
            u_val = lax.dot_general(wg[e], x_val, dims, preferred_element_type=jnp.float32)
            v_val = lax.dot_general(wu[e], x_val, dims, preferred_element_type=jnp.float32)
            zt_ref[:ff] = (jax.nn.silu(u_val) * v_val).astype(jnp.bfloat16)
            z_ref[e] = jnp.transpose(zt_ref[...])

        @pl.when(r == 0)
        def _():
            for e in range(2):
                weight(e)[2].wait()

        @pl.when(r == 2)
        def _():
            gather[4].wait_recv()
            gather[7].start()
            gather[6].wait_recv()
            gather[8].start()

        @pl.loop(0, 2)
        def _(part):
            @pl.when(r > 0)
            def _():
                shared(r - 1, part).wait_send()

            @pl.loop(0, half // tile)
            def _(n):
                wide = pl.ds(pl.multiple_of(part * half + n * tile, tile), tile)
                slim = pl.ds(pl.multiple_of(n * tile, tile), tile)
                first = jnp.dot(z_ref[0, :, :ff], wd[0, :, wide], preferred_element_type=jnp.float32)
                second = jnp.dot(z_ref[1, :, :ff], wd[1, :, wide], preferred_element_type=jnp.float32)
                for slot in range(2):
                    choice = xblk[:, d_model:][:, slot:slot + 1].astype(jnp.float32)
                    lead = (2 * me).astype(jnp.float32)
                    val = jnp.where(choice == lead, first, jnp.where(choice == lead + 1.0, second, 0.0)).astype(jnp.bfloat16)
                    acc[r, part, slot, :, slim] = val[:rows]
                    stg[part, slot, :, slim] = val[rows:]

            @pl.when((r >= 2) & (part == 0))
            def _():
                pl.semaphore_wait(credit, 1)

            shared(r, part).start()

        @pl.loop(0, 2)
        def _(part):
            shared(r, part).wait_recv()
            merge(acc.at[r, part], d2d.at[lax.rem(r, 2), part])

            @pl.when((r == 1) & (part == 0))
            def _():
                scatter[0].start()

            @pl.when((r == 2) & (part == 1))
            def _():
                scatter[1].start()

            @pl.when((r == 3) & (part == 0))
            def _():
                scatter[2].start()

            @pl.when((r == 3) & (part == 1))
            def _():
                scatter[3].start()

        @pl.when(r < 2)
        def _():
            pl.semaphore_signal(credit, inc=1, device_id=(partner,), device_id_type=mesh_id)

    x_copy = pltpu.make_async_copy(x_hbm, xblk.at[pl.ds(0, rows), pl.ds(0, d_model)], xsem.at[0])
    x_copy.start()
    scatter[2].wait_recv()
    merge(acc.at[2, 0], p1a.at[1])
    scatter[5].start()
    scatter[3].wait_recv()
    merge(acc.at[1, 1], p1b.at[1])
    scatter[4].start()
    scatter[0].wait_recv()
    merge(acc.at[0, 0], p1a.at[0])
    scatter[1].wait_recv()
    merge(acc.at[0, 1], p1b.at[0])
    x_copy.wait()
    result = xblk.at[pl.ds(rows, rows), pl.ds(0, d_model)]
    for part, last, buf in ((0, 5, p2a), (1, 4, p2b)):
        scatter[last].wait_recv()

        @pl.loop(0, rows // 16)
        def _(i, part=part, buf=buf):
            at = pl.ds(pl.multiple_of(i * 16, 16), 16)
            wide = pl.ds(part * half, half)
            gates = gate_ref[at]
            y_val = [(acc[0, part, slot, at] + buf[slot, at]).astype(jnp.float32) * gates[:, slot:slot + 1] for slot in range(2)]
            result[at, wide] = (xblk[at, wide].astype(jnp.float32) + (y_val[0] + y_val[1])).astype(jnp.bfloat16)

    out_copy = pltpu.make_async_copy(result, out_hbm, xsem.at[1])
    out_copy.start()
    for copy in gather + scatter:
        copy.wait_send()
    for part in range(2):
        shared(3, part).wait_send()
    out_copy.wait()


def moe_call(h_ext, x_mid, gates, w_gate, w_up, w_down):
    rows, d_model = x_mid.shape
    half = d_model // 2
    ff = w_gate.shape[2]
    ff_pad = pl.cdiv(ff, 128) * 128
    width = h_ext.shape[1]
    vmem = pl.BlockSpec(memory_space=pltpu.VMEM)
    hbm = pl.BlockSpec(memory_space=pl.ANY)
    bf = jnp.bfloat16
    dma = pltpu.SemaphoreType.DMA
    out, _ = pl.pallas_call(
        moe_kernel,
        in_specs=[hbm, hbm, vmem, hbm, hbm, hbm],
        out_specs=[hbm, hbm],
        out_shape=[jax.ShapeDtypeStruct((rows, d_model), bf), jax.ShapeDtypeStruct((8, rows, width), bf)],
        scratch_shapes=[
            pltpu.VMEM((2, ff, d_model), bf),
            pltpu.VMEM((2, ff, d_model), bf),
            pltpu.VMEM((2, ff, d_model), bf),
            pltpu.VMEM((2 * rows, width), bf),
            pltpu.VMEM((ff_pad, 2 * rows), bf),
            pltpu.VMEM((2, 2 * rows, ff_pad), bf),
            pltpu.VMEM((4, 2, 2, rows, half), bf),
            pltpu.VMEM((2, 2, rows, half), bf),
            pltpu.VMEM((2, 2, 2, rows, half), bf),
            pltpu.VMEM((2, 2, rows, half), bf),
            pltpu.VMEM((2, 2, rows, half), bf),
            pltpu.VMEM((2, rows, half), bf),
            pltpu.VMEM((2, rows, half), bf),
            dma((3, 2)),
            dma((2,)),
            dma((9,)),
            dma((9,)),
            dma((2,)),
            dma((4, 2)),
            dma((6,)),
            dma((6,)),
            pltpu.SemaphoreType.REGULAR,
        ],
        compiler_params=pltpu.CompilerParams(vmem_limit_bytes=67043328, collective_id=0, has_side_effects=True),
        name='moe',
    )(h_ext, x_mid, gates, jnp.swapaxes(w_gate, 1, 2), jnp.swapaxes(w_up, 1, 2), w_down)
    return out


def solution(mesh):
    def local_step(tokens, k_cache, v_cache, positions, expert_one, expert_two, eligible, ln1_gain, ln1_bias, w_query, b_query, w_key, b_key, w_value, b_value, w_out, b_out, ln2_gain, ln2_bias, w_router, w_gate, w_up, w_down):
        tok_count, seq_len, heads, head_dim = k_cache.shape
        d_model = tokens.shape[1]
        cos_tab, sin_tab = rope_tables(positions, head_dim)
        sign = jnp.where(jnp.arange(head_dim) < head_dim // 2, -1.0, 1.0)
        vectors = row_stack([ln1_gain, ln1_bias, b_query, b_key, b_value, b_out, ln2_gain, ln2_bias])
        which = lax.broadcasted_iota(jnp.int32, (128, tok_count), 0)
        picks = jnp.where(which == 0, expert_one[None, :], jnp.where(which == 1, expert_two[None, :], jnp.pad(eligible.T, ((2, 110), (0, 0)))))
        q_flat, k_flat, v_flat = qkv_call(tokens, vectors, cos_tab, sin_tab * sign[None, :], w_query, w_key, w_value)
        split = lambda t: t.reshape(tok_count, heads, head_dim)
        key_new, value_new = split(k_flat), split(v_flat)
        attn = attend_call(attention_order(positions), positions, split(q_flat), key_new, value_new, k_cache, v_cache)
        x_mid, h_ext, gates = out_call(attn.reshape(tok_count, heads * head_dim), tokens, vectors, w_router.T, picks, w_out)
        tokens_out = moe_call(h_ext, x_mid, gates, w_gate, w_up, w_down)
        return tokens_out, key_new, value_new

    row_spec = P('ep', None)
    cache_spec = P('ep', None, None, None)
    vec_spec = P('ep')
    rep_one = P(None)
    rep_two = P(None, None)
    expert_spec = P('ep', None, None)
    in_specs = (row_spec, cache_spec, cache_spec, vec_spec, vec_spec, vec_spec, row_spec, rep_one, rep_one, rep_two, rep_one, rep_two, rep_one, rep_two, rep_one, rep_two, rep_one, rep_one, rep_one, rep_two, expert_spec, expert_spec, expert_spec)
    out_specs = (row_spec, expert_spec, expert_spec)
    return jax.shard_map(local_step, mesh=mesh, in_specs=in_specs, out_specs=out_specs, check_vma=False)
```

```python
import jax
import jax.numpy as jnp
from jax import lax
from jax.experimental import pallas as pl
from jax.experimental.pallas import tpu as pltpu
from jax.sharding import PartitionSpec as P

ROPE_BASE = 10000.0
LN_EPS = 1e-5


def rope_tables(positions, head_dim):
    half_dim = head_dim // 2
    inv_freq = ROPE_BASE ** (jnp.arange(half_dim, dtype=jnp.float32) * (-2.0 / head_dim))
    angles = positions.astype(jnp.float32)[:, None] * inv_freq[None, :]
    angles = jnp.concatenate([angles, angles], axis=-1)
    return jnp.cos(angles), jnp.sin(angles)


def norm_rows(x_val, gain, bias):
    mean_val = jnp.mean(x_val, axis=-1, keepdims=True)
    centered = x_val - mean_val
    var_val = jnp.mean(centered * centered, axis=-1, keepdims=True)
    return centered * lax.rsqrt(var_val + LN_EPS) * gain.astype(jnp.float32) + bias.astype(jnp.float32)


def row_stack(vectors):
    which = lax.broadcasted_iota(jnp.int32, (len(vectors), vectors[0].shape[0]), 0)
    out = jnp.zeros((len(vectors), vectors[0].shape[0]), vectors[0].dtype)
    for n, vec in enumerate(vectors):
        out = jnp.where(which == n, vec[None, :], out)
    return out


AHEAD = 4


def qkv_kernel(x_ref, vec_ref, cos_ref, sin_ref, wq_hbm, wk_hbm, wv_hbm, q_ref, k_ref, v_ref, h_ref, w_buf, sems):
    rows, d_model = x_ref.shape
    tile = w_buf.shape[3]
    count = q_ref.shape[1] // tile
    head_dim = cos_ref.shape[1]

    def copies(j, slot):
        cols = pl.ds(pl.multiple_of(j * tile, tile), tile)
        return [pltpu.make_async_copy(hbm.at[:, cols], w_buf.at[slot, n], sems.at[slot, n]) for n, hbm in enumerate((wq_hbm, wk_hbm, wv_hbm))]

    for j in range(AHEAD):
        for copy in copies(j, j):
            copy.start()
    h_ref[...] = norm_rows(x_ref[...].astype(jnp.float32), vec_ref[0:1], vec_ref[1:2]).astype(jnp.bfloat16)

    @pl.loop(0, count)
    def _(j):
        slot = lax.rem(j, AHEAD)
        cols = pl.ds(pl.multiple_of(j * tile, tile), tile)
        now = copies(j, slot)
        for n, o_ref in enumerate((q_ref, k_ref, v_ref)):
            now[n].wait()
            lin = jnp.dot(h_ref[...], w_buf[slot, n], preferred_element_type=jnp.float32) + vec_ref[2 + n:3 + n, cols].astype(jnp.float32)
            if n == 2:
                o_ref[:, cols] = lin.astype(jnp.bfloat16)
            else:
                parts = []
                for c in range(tile // head_dim):
                    part = lin[:, c * head_dim:(c + 1) * head_dim]
                    parts.append(part * cos_ref[...] + pltpu.roll(part, head_dim // 2, 1) * sin_ref[...])
                o_ref[:, cols] = jnp.concatenate(parts, axis=1).astype(jnp.bfloat16)

        @pl.when(j + AHEAD < count)
        def _():
            for copy in copies(j + AHEAD, slot):
                copy.start()


def qkv_call(tokens, vectors, cos_tab, sin_signed, w_query, w_key, w_value):
    rows, d_model = tokens.shape
    cols = w_query.shape[1]
    tile = 256
    vmem = pl.BlockSpec(memory_space=pltpu.VMEM)
    hbm = pl.BlockSpec(memory_space=pl.ANY)
    shape = jax.ShapeDtypeStruct((rows, cols), jnp.bfloat16)
    return pl.pallas_call(
        qkv_kernel,
        in_specs=[vmem, vmem, vmem, vmem, hbm, hbm, hbm],
        out_specs=[vmem, vmem, vmem],
        out_shape=[shape, shape, shape],
        scratch_shapes=[pltpu.VMEM((rows, d_model), jnp.bfloat16), pltpu.VMEM((AHEAD, 3, d_model, tile), jnp.bfloat16), pltpu.SemaphoreType.DMA((AHEAD, 3))],
        compiler_params=pltpu.CompilerParams(vmem_limit_bytes=44 * 2 ** 20),
        cost_estimate=pl.CostEstimate(flops=6 * rows * d_model * cols, bytes_accessed=6 * d_model * cols, transcendentals=0),
        name='qkv',
    )(tokens, vectors, cos_tab, sin_signed, w_query, w_key, w_value)


GROUP = 4
SLOTS = 4
STEP = 16


def attend_kernel(order_ref, pos_ref, q_ref, kn_ref, vn_ref, k_hbm, v_hbm, out_ref, k_buf, v_buf, sid_ref, sems):
    rows, heads, head_dim = q_ref.shape
    seq = k_hbm.shape[1]
    groups = rows // GROUP
    scale = head_dim ** -0.5
    key_id = lax.broadcasted_iota(jnp.int32, sid_ref.shape, 1)
    row_id = lax.broadcasted_iota(jnp.int32, sid_ref.shape, 0)
    sid_ref[...] = jnp.where(lax.rem(key_id, heads) == row_id, lax.div(key_id, heads), seq)

    @pl.loop(0, GROUP * SLOTS)
    def _(i):
        v_buf[i // GROUP, i % GROUP] = jnp.zeros(v_buf.shape[2:], v_buf.dtype)

    def group_at(n):
        return jnp.where(n & 1 == 0, n // 2, groups - 1 - n // 2)

    def each_size(grp, act):
        need = (pos_ref[order_ref[grp * GROUP]] + 3) & -4
        size = seq
        while size >= 4:
            @pl.when((need & size) != 0)
            def _(size=size):
                act(need & (-2 * size), size)

            size //= 2

    def fetch(n):
        grp = group_at(n)
        slot = n & (SLOTS - 1)

        def act(first, size):
            src = pl.ds(first, size)
            for i in range(GROUP):
                tok = order_ref[grp * GROUP + i]
                pltpu.make_async_copy(k_hbm.at[tok, src], k_buf.at[slot, i, src], sems.at[0, slot]).start()
                pltpu.make_async_copy(v_hbm.at[tok, src], v_buf.at[slot, i, src], sems.at[1, slot]).start()

        each_size(grp, act)

    def settle(n):
        slot = n & (SLOTS - 1)

        def act(first, size):
            src = pl.ds(0, size)
            pltpu.make_async_copy(k_hbm.at[pl.ds(0, GROUP), src], k_buf.at[slot, :, src], sems.at[0, slot]).wait()
            pltpu.make_async_copy(v_hbm.at[pl.ds(0, GROUP), src], v_buf.at[slot, :, src], sems.at[1, slot]).wait()

        each_size(group_at(n), act)

    def compute(n, steps):
        grp = group_at(n)
        slot = n & (SLOTS - 1)
        keys = steps * STEP * heads
        toks = [order_ref[grp * GROUP + i] for i in range(GROUP)]
        q_val = [q_ref[t] for t in toks]
        scores = []
        for i in range(GROUP):
            k_val = k_buf[slot, i, pl.ds(0, steps * STEP)].reshape(keys, head_dim)
            raw = lax.dot_general(q_val[i], k_val, (((1,), (1,)), ((), ())), preferred_element_type=jnp.float32)
            scores.append(jnp.where(sid_ref[:, :keys] < pos_ref[toks[i]], raw * scale, -jnp.inf))
        for i in range(GROUP):
            t = toks[i]
            s_new = jnp.sum(q_val[i].astype(jnp.float32) * kn_ref[t].astype(jnp.float32), axis=-1, keepdims=True) * scale
            top = jnp.maximum(jnp.max(scores[i], axis=-1, keepdims=True), s_new)
            e_val = jnp.exp(scores[i] - top)
            e_new = jnp.exp(s_new - top)
            inv = 1.0 / (jnp.sum(e_val, axis=-1, keepdims=True) + e_new)
            p_val = (e_val * inv).astype(jnp.bfloat16)
            p_new = (e_new * inv).astype(jnp.bfloat16).astype(jnp.float32)
            v_val = v_buf[slot, i, pl.ds(0, steps * STEP)].reshape(keys, head_dim)
            res = jnp.dot(p_val, v_val, preferred_element_type=jnp.float32) + p_new * vn_ref[t].astype(jnp.float32)
            out_ref[t] = res.astype(jnp.bfloat16)

    for n in range(SLOTS - 1):
        fetch(n)

    @pl.loop(0, groups)
    def _(n):
        @pl.when(n + SLOTS - 1 < groups)
        def _():
            fetch(n + SLOTS - 1)

        settle(n)
        most = pos_ref[order_ref[group_at(n) * GROUP]]
        steps = jnp.maximum((most + STEP - 1) // STEP, 1)
        for k in range(1, seq // STEP + 1):
            @pl.when(steps == k)
            def _(k=k):
                compute(n, k)


def attend_call(order, positions, q_rot, key_new, value_new, k_cache, v_cache):
    rows, seq, heads, head_dim = k_cache.shape
    vmem = pl.BlockSpec(memory_space=pltpu.VMEM)
    smem = pl.BlockSpec(memory_space=pltpu.SMEM)
    hbm = pl.BlockSpec(memory_space=pl.ANY)
    return pl.pallas_call(
        attend_kernel,
        in_specs=[smem, smem, vmem, vmem, vmem, hbm, hbm],
        out_specs=vmem,
        out_shape=jax.ShapeDtypeStruct((rows, heads, head_dim), jnp.bfloat16),
        scratch_shapes=[
            pltpu.VMEM((SLOTS, GROUP, seq, heads, head_dim), jnp.bfloat16),
            pltpu.VMEM((SLOTS, GROUP, seq, heads, head_dim), jnp.bfloat16),
            pltpu.VMEM((heads, seq * heads), jnp.int32),
            pltpu.SemaphoreType.DMA((2, SLOTS)),
        ],
        compiler_params=pltpu.CompilerParams(vmem_limit_bytes=40 * 2 ** 20),
        cost_estimate=pl.CostEstimate(flops=4 * rows * seq * heads * heads * head_dim, bytes_accessed=2 * rows * seq * heads * head_dim, transcendentals=0),
        name='attend',
    )(order, positions, q_rot, key_new, value_new, k_cache, v_cache)


def out_kernel(a_ref, x_ref, vec_ref, wr_ref, pick_ref, w_hbm, mid_ref, h_ref, gate_ref, w_buf, sems):
    count, _, tile = w_buf.shape

    def weight(j):
        cols = pl.ds(pl.multiple_of(j * tile, tile), tile)
        return pltpu.make_async_copy(w_hbm.at[:, cols], w_buf.at[j], sems.at[j])

    for j in range(count):
        weight(j).start()

    @pl.loop(0, count)
    def _(j):
        weight(j).wait()
        cols = pl.ds(pl.multiple_of(j * tile, tile), tile)
        mid = x_ref[:, cols].astype(jnp.float32) + jnp.dot(a_ref[...], w_buf[j], preferred_element_type=jnp.float32) + vec_ref[5:6, cols].astype(jnp.float32)
        mid_ref[:, cols] = mid.astype(jnp.bfloat16)

    h_two = norm_rows(mid_ref[...].astype(jnp.float32), vec_ref[6:7], vec_ref[7:8]).astype(jnp.bfloat16)
    lanes = lax.broadcasted_iota(jnp.int32, (h_two.shape[0], 128), 1)
    pick_val = jnp.transpose(pick_ref[...].astype(jnp.float32))
    picks = jnp.where(lanes < 2, pick_val, 0.0)
    h_ref[:, :h_two.shape[1]] = h_two
    h_ref[:, h_two.shape[1]:] = picks.astype(jnp.bfloat16)
    logits = lax.dot_general(h_two, wr_ref[...], (((1,), (1,)), ((), ())), preferred_element_type=jnp.float32)
    ids = lax.broadcasted_iota(jnp.int32, logits.shape, 1).astype(jnp.float32)
    hit_one = ids == pick_val[:, 0:1]
    hit_two = ids == pick_val[:, 1:2]
    keep_one = pick_val[:, 2:2 + logits.shape[1]] == 1.0
    gates = []
    for keep, hit in ((keep_one, hit_one), (keep_one & jnp.logical_not(hit_one), hit_two)):
        masked = jnp.where(keep, logits, -jnp.inf)
        e_val = jnp.exp(masked - jnp.max(masked, axis=-1, keepdims=True))
        top = jnp.sum(jnp.where(hit, e_val, 0.0), axis=-1, keepdims=True)
        gates.append(top / jnp.sum(e_val, axis=-1, keepdims=True))
    lane = lax.broadcasted_iota(jnp.int32, gate_ref.shape, 1)
    gate_ref[...] = jnp.where(lane == 0, gates[0], jnp.where(lane == 1, gates[1], 0.0))


def out_call(attn_flat, tokens, vectors, w_router, picks, w_out):
    rows, d_model = tokens.shape
    tile = 256
    vmem = pl.BlockSpec(memory_space=pltpu.VMEM)
    shape = lambda cols, kind: jax.ShapeDtypeStruct((rows, cols), kind)
    return pl.pallas_call(
        out_kernel,
        in_specs=[vmem] * 5 + [pl.BlockSpec(memory_space=pl.ANY)],
        out_specs=[vmem] * 3,
        out_shape=[shape(d_model, jnp.bfloat16), shape(d_model + 128, jnp.bfloat16), shape(128, jnp.float32)],
        scratch_shapes=[pltpu.VMEM((d_model // tile, w_out.shape[0], tile), jnp.bfloat16), pltpu.SemaphoreType.DMA((d_model // tile,))],
        compiler_params=pltpu.CompilerParams(vmem_limit_bytes=48 * 2 ** 20),
        cost_estimate=pl.CostEstimate(flops=2 * rows * d_model * d_model, bytes_accessed=2 * d_model * d_model, transcendentals=0),
        name='project',
    )(attn_flat, tokens, vectors, w_router, picks, w_out)


def attention_order(positions):
    ids = jnp.arange(positions.shape[0], dtype=jnp.int32)
    ahead = (positions[None, :] > positions[:, None]) | ((positions[None, :] == positions[:, None]) & (ids[None, :] < ids[:, None]))
    rank = jnp.sum(ahead.astype(jnp.int32), axis=1)
    return jnp.sum(jnp.where(rank[:, None] == ids[None, :], ids[:, None], 0), axis=0)


def moe_kernel(h_in, x_ref, gate_ref, wg_hbm, wu_hbm, wd_hbm, out_ref, hb, wg, wu, wd, xblk, zt_ref, z_ref, acc, stg, d2d, p1a, p1b, p2a, p2b, wsem, xsem, gsend, grecv, dsend, drecv, rsend, rrecv, credit):
    me = lax.axis_index('ep')
    core = lax.rem(me, 2)
    x_pos = lax.rem(lax.div(me, 2), 2)
    y_pos = lax.div(me, 4)
    partner = me + 1 - 2 * core
    xn = me + 2 - 4 * x_pos
    yn = me + 4 - 8 * y_pos
    rows = h_in.shape[0]
    mid = rows // 2
    d_model = x_ref.shape[1]
    half = d_model // 2
    ff = wd.shape[1]
    tile = 512
    mesh_id = pl.DeviceIdType.MESH
    part_rows = (pl.ds(0, mid), pl.ds(mid, mid))

    def remote(src, dst, send, recv, dev):
        return pltpu.make_async_remote_copy(src_ref=src, dst_ref=dst, send_sem=send, recv_sem=recv, device_id=(dev,), device_id_type=mesh_id)

    gather = []

    def add_gather(src, dst, dev):
        n = len(gather)
        gather.append(remote(src, dst, gsend.at[n], grecv.at[n], dev))
        return gather[-1]

    own = add_gather(h_in, hb.at[1], partner)
    from_x = [add_gather(h_in.at[p], hb.at[2, p], xn) for p in part_rows]
    from_y = [add_gather(h_in.at[p], hb.at[4, p], yn) for p in part_rows]
    share_x = [add_gather(hb.at[2, p], hb.at[3, p], partner) for p in part_rows]
    share_y = [add_gather(hb.at[4, p], hb.at[5, p], partner) for p in part_rows]
    far = [add_gather(hb.at[2, part_rows[0]], hb.at[6, part_rows[0]], yn), add_gather(hb.at[4, part_rows[1]], hb.at[6, part_rows[1]], xn)]
    share_far = [add_gather(hb.at[6, p], hb.at[7, p], partner) for p in part_rows]

    scatter = []

    def add_scatter(src, dst, dev):
        n = len(scatter)
        scatter.append(remote(src, dst, rsend.at[n], rrecv.at[n], dev))
        return scatter[-1]

    x_first = [add_scatter(acc.at[1 + h, 0, :, part_rows[0]], p1a.at[0, h], xn) for h in range(2)]
    y_first = [add_scatter(acc.at[1 + h, 1, :, part_rows[1]], p1b.at[0, h], yn) for h in range(2)]
    x_far = [add_scatter(acc.at[3, 0, :, part_rows[h]], p1a.at[1, h], xn) for h in range(2)]
    y_far = [add_scatter(acc.at[3, 1, :, part_rows[h]], p1b.at[1, h], yn) for h in range(2)]
    y_last = [add_scatter(acc.at[1 + h, 0, :, part_rows[1]], p2a.at[h], yn) for h in range(2)]
    x_last = [add_scatter(acc.at[1 + h, 1, :, part_rows[0]], p2b.at[h], xn) for h in range(2)]

    def weight(e):
        return [pltpu.make_async_copy(hbm.at[e], buf.at[e], wsem.at[n, e]) for n, (hbm, buf) in enumerate(((wg_hbm, wg), (wu_hbm, wu), (wd_hbm, wd)))]

    barrier = pltpu.get_barrier_semaphore()
    for dev in (partner, xn, yn):
        pl.semaphore_signal(barrier, inc=1, device_id=(dev,), device_id_type=mesh_id)
    for e in range(2):
        for copy in weight(e):
            copy.start()
    zt_ref[...] = jnp.zeros_like(zt_ref)
    pl.semaphore_wait(barrier, 3)
    for h in range(2):
        from_x[h].start()
        from_y[h].start()
    own.start()

    def load(sources):
        step = 2 * rows // len(sources)
        copies = [pltpu.make_async_copy(src, xblk.at[pl.ds(n * step, step)], xsem.at[n]) for n, src in enumerate(sources)]
        for copy in copies:
            copy.start()
        for copy in copies:
            copy.wait()

    def merge(dst, src):
        count = dst.shape[1] // 32

        @pl.loop(0, 2 * count)
        def _(i):
            slot = lax.div(i, count)
            at = pl.ds(pl.multiple_of(lax.rem(i, count) * 32, 32), 32)
            dst[slot, at] = dst[slot, at] + src[slot, at]

    def shared(r, part):
        return remote(stg.at[part], d2d.at[lax.rem(r, 2), part], dsend.at[part], drecv.at[r, part], partner)

    def gather_step(h):
        from_x[h].wait_recv()
        share_x[h].start()
        if h == 0:
            far[0].start()
        from_y[h].wait_recv()
        share_y[h].start()
        if h == 1:
            far[1].start()

    def merge_high(r, finish):
        shared(r, 1).wait_recv()
        merge(acc.at[r, 1], d2d.at[lax.rem(r, 2), 1])
        if not finish:
            for h in range(2):
                @pl.when(r == 1 + h)
                def _(h=h):
                    y_first[h].start()

            @pl.when(r < 2)
            def _():
                pl.semaphore_signal(credit, inc=1, device_id=(partner,), device_id_type=mesh_id)

    @pl.loop(0, 4)
    def _(r):
        @pl.when(r == 0)
        def _():
            pltpu.sync_copy(h_in, xblk.at[pl.ds(0, rows)])
            own.wait_recv()
            copy = pltpu.make_async_copy(hb.at[1], xblk.at[pl.ds(rows, rows)], xsem.at[0])
            copy.start()
            copy.wait()

        for h in range(2):
            @pl.when(r == 1 + h)
            def _(h=h):
                share_x[h].wait_recv()
                share_y[h].wait_recv()
                load([hb.at[n, part_rows[h]] for n in (2, 4, 3, 5)])

        @pl.when(r == 3)
        def _():
            share_far[0].wait_recv()
            share_far[1].wait_recv()
            load([hb.at[6], hb.at[7]])

        @pl.loop(0, 2)
        def _(e):
            @pl.when(r == 0)
            def _():
                for copy in weight(e)[:2]:
                    copy.wait()

            x_val = xblk[:, :d_model]
            dims = (((1,), (1,)), ((), ()))
            u_val = lax.dot_general(wg[e], x_val, dims, preferred_element_type=jnp.float32)
            v_val = lax.dot_general(wu[e], x_val, dims, preferred_element_type=jnp.float32)
            zt_ref[:ff] = (jax.nn.silu(u_val) * v_val).astype(jnp.bfloat16)
            z_ref[e] = jnp.transpose(zt_ref[...])

            @pl.when((r > 0) & (e == 0))
            def _():
                merge_high(r - 1, False)

            for h in range(2):
                @pl.when((r == h) & (e == 0))
                def _(h=h):
                    gather_step(h)

        @pl.when(r == 0)
        def _():
            for e in range(2):
                weight(e)[2].wait()

        @pl.when(r == 2)
        def _():
            for h in range(2):
                far[h].wait_recv()
                share_far[h].start()

        @pl.loop(0, 2)
        def _(part):
            @pl.when(r > 0)
            def _():
                shared(r - 1, part).wait_send()

            @pl.loop(0, half // tile)
            def _(n):
                wide = pl.ds(pl.multiple_of(part * half + n * tile, tile), tile)
                slim = pl.ds(pl.multiple_of(n * tile, tile), tile)
                first = jnp.dot(z_ref[0, :, :ff], wd[0, :, wide], preferred_element_type=jnp.float32)
                second = jnp.dot(z_ref[1, :, :ff], wd[1, :, wide], preferred_element_type=jnp.float32)
                for slot in range(2):
                    choice = xblk[:, d_model:][:, slot:slot + 1].astype(jnp.float32)
                    lead = (2 * me).astype(jnp.float32)
                    val = jnp.where(choice == lead, first, jnp.where(choice == lead + 1.0, second, 0.0)).astype(jnp.bfloat16)
                    acc[r, part, slot, :, slim] = val[:rows]
                    stg[part, slot, :, slim] = val[rows:]

            @pl.when((r >= 2) & (part == 0))
            def _():
                pl.semaphore_wait(credit, 1)

            shared(r, part).start()

        shared(r, 0).wait_recv()
        merge(acc.at[r, 0], d2d.at[lax.rem(r, 2), 0])
        for h in range(2):
            @pl.when(r == 1 + h)
            def _(h=h):
                x_first[h].start()

        @pl.when(r == 3)
        def _():
            x_far[0].start()
            x_far[1].start()

    merge_high(3, True)
    y_far[0].start()
    y_far[1].start()
    for h in range(2):
        x_far[h].wait_recv()
        merge(acc.at[1 + h, 0, :, part_rows[1]], p1a.at[1, h])
        y_last[h].start()
        y_far[h].wait_recv()
        merge(acc.at[1 + h, 1, :, part_rows[0]], p1b.at[1, h])
        x_last[h].start()
    for h in range(2):
        x_first[h].wait_recv()
        merge(acc.at[0, 0, :, part_rows[h]], p1a.at[0, h])
        y_first[h].wait_recv()
        merge(acc.at[0, 1, :, part_rows[h]], p1b.at[0, h])
    for h in range(2):
        for part, last, buf in ((0, y_last, p2a), (1, x_last, p2b)):
            last[h].wait_recv()

            @pl.loop(0, mid // 16)
            def _(i, h=h, part=part, buf=buf):
                near = pl.ds(pl.multiple_of(i * 16, 16), 16)
                at = pl.ds(pl.multiple_of(h * mid + i * 16, 16), 16)
                wide = pl.ds(part * half, half)
                gates = gate_ref[at]
                y_val = [(acc[0, part, slot, at] + buf[h, slot, near]).astype(jnp.float32) * gates[:, slot:slot + 1] for slot in range(2)]
                out_ref[at, wide] = (x_ref[at, wide].astype(jnp.float32) + (y_val[0] + y_val[1])).astype(jnp.bfloat16)

    for copy in gather + scatter:
        copy.wait_send()
    for part in range(2):
        shared(3, part).wait_send()


def moe_call(h_ext, x_mid, gates, w_gate, w_up, w_down):
    rows, d_model = x_mid.shape
    half = d_model // 2
    ff = w_gate.shape[2]
    ff_pad = pl.cdiv(ff, 128) * 128
    width = h_ext.shape[1]
    vmem = pl.BlockSpec(memory_space=pltpu.VMEM)
    hbm = pl.BlockSpec(memory_space=pl.ANY)
    bf = jnp.bfloat16
    dma = pltpu.SemaphoreType.DMA
    out, _ = pl.pallas_call(
        moe_kernel,
        in_specs=[vmem, vmem, vmem, hbm, hbm, hbm],
        out_specs=[vmem, hbm],
        out_shape=[jax.ShapeDtypeStruct((rows, d_model), bf), jax.ShapeDtypeStruct((8, rows, width), bf)],
        scratch_shapes=[
            pltpu.VMEM((2, ff, d_model), bf),
            pltpu.VMEM((2, ff, d_model), bf),
            pltpu.VMEM((2, ff, d_model), bf),
            pltpu.VMEM((2 * rows, width), bf),
            pltpu.VMEM((ff_pad, 2 * rows), bf),
            pltpu.VMEM((2, 2 * rows, ff_pad), bf),
            pltpu.VMEM((4, 2, 2, rows, half), bf),
            pltpu.VMEM((2, 2, rows, half), bf),
            pltpu.VMEM((2, 2, 2, rows, half), bf),
            pltpu.VMEM((2, 2, 2, rows // 2, half), bf),
            pltpu.VMEM((2, 2, 2, rows // 2, half), bf),
            pltpu.VMEM((2, 2, rows // 2, half), bf),
            pltpu.VMEM((2, 2, rows // 2, half), bf),
            dma((3, 2)),
            dma((4,)),
            dma((13,)),
            dma((13,)),
            dma((2,)),
            dma((4, 2)),
            dma((12,)),
            dma((12,)),
            pltpu.SemaphoreType.REGULAR,
        ],
        compiler_params=pltpu.CompilerParams(vmem_limit_bytes=67043328, collective_id=0, has_side_effects=True),
        name='moe',
    )(h_ext, x_mid, gates, jnp.swapaxes(w_gate, 1, 2), jnp.swapaxes(w_up, 1, 2), w_down)
    return out


def solution(mesh):
    def local_step(tokens, k_cache, v_cache, positions, expert_one, expert_two, eligible, ln1_gain, ln1_bias, w_query, b_query, w_key, b_key, w_value, b_value, w_out, b_out, ln2_gain, ln2_bias, w_router, w_gate, w_up, w_down):
        tok_count, seq_len, heads, head_dim = k_cache.shape
        d_model = tokens.shape[1]
        cos_tab, sin_tab = rope_tables(positions, head_dim)
        sign = jnp.where(jnp.arange(head_dim) < head_dim // 2, -1.0, 1.0)
        vectors = row_stack([ln1_gain, ln1_bias, b_query, b_key, b_value, b_out, ln2_gain, ln2_bias])
        which = lax.broadcasted_iota(jnp.int32, (128, tok_count), 0)
        picks = jnp.where(which == 0, expert_one[None, :], jnp.where(which == 1, expert_two[None, :], jnp.pad(eligible.T, ((2, 110), (0, 0)))))
        q_flat, k_flat, v_flat = qkv_call(tokens, vectors, cos_tab, sin_tab * sign[None, :], w_query, w_key, w_value)
        split = lambda t: t.reshape(tok_count, heads, head_dim)
        key_new, value_new = split(k_flat), split(v_flat)
        attn = attend_call(attention_order(positions), positions, split(q_flat), key_new, value_new, k_cache, v_cache)
        x_mid, h_ext, gates = out_call(attn.reshape(tok_count, heads * head_dim), tokens, vectors, w_router.T, picks, w_out)
        tokens_out = moe_call(h_ext, x_mid, gates, w_gate, w_up, w_down)
        return tokens_out, key_new, value_new

    row_spec = P('ep', None)
    cache_spec = P('ep', None, None, None)
    vec_spec = P('ep')
    rep_one = P(None)
    rep_two = P(None, None)
    expert_spec = P('ep', None, None)
    in_specs = (row_spec, cache_spec, cache_spec, vec_spec, vec_spec, vec_spec, row_spec, rep_one, rep_one, rep_two, rep_one, rep_two, rep_one, rep_two, rep_one, rep_two, rep_one, rep_one, rep_one, rep_two, expert_spec, expert_spec, expert_spec)
    out_specs = (row_spec, expert_spec, expert_spec)
    return jax.shard_map(local_step, mesh=mesh, in_specs=in_specs, out_specs=out_specs, check_vma=False)
```

```python
import jax
import jax.numpy as jnp
from jax import lax
from jax.experimental import pallas as pl
from jax.experimental.pallas import tpu as pltpu
from jax.sharding import PartitionSpec as P

ROPE_BASE = 10000.0
LN_EPS = 1e-5


def rope_tables(positions, head_dim):
    half_dim = head_dim // 2
    inv_freq = ROPE_BASE ** (jnp.arange(half_dim, dtype=jnp.float32) * (-2.0 / head_dim))
    angles = positions.astype(jnp.float32)[:, None] * inv_freq[None, :]
    angles = jnp.concatenate([angles, angles], axis=-1)
    return jnp.cos(angles), jnp.sin(angles)


def norm_rows(x_val, gain, bias):
    mean_val = jnp.mean(x_val, axis=-1, keepdims=True)
    centered = x_val - mean_val
    var_val = jnp.mean(centered * centered, axis=-1, keepdims=True)
    return centered * lax.rsqrt(var_val + LN_EPS) * gain.astype(jnp.float32) + bias.astype(jnp.float32)


def row_stack(vectors):
    which = lax.broadcasted_iota(jnp.int32, (len(vectors), vectors[0].shape[0]), 0)
    out = jnp.zeros((len(vectors), vectors[0].shape[0]), vectors[0].dtype)
    for n, vec in enumerate(vectors):
        out = jnp.where(which == n, vec[None, :], out)
    return out


AHEAD = 4


def qkv_kernel(x_ref, vec_ref, cos_ref, sin_ref, wq_hbm, wk_hbm, wv_hbm, q_ref, k_ref, v_ref, h_ref, w_buf, sems):
    rows, d_model = x_ref.shape
    tile = w_buf.shape[3]
    count = q_ref.shape[1] // tile
    head_dim = cos_ref.shape[1]

    def copies(j, slot):
        cols = pl.ds(pl.multiple_of(j * tile, tile), tile)
        return [pltpu.make_async_copy(hbm.at[:, cols], w_buf.at[slot, n], sems.at[slot, n]) for n, hbm in enumerate((wq_hbm, wk_hbm, wv_hbm))]

    for j in range(AHEAD):
        for copy in copies(j, j):
            copy.start()
    h_ref[...] = norm_rows(x_ref[...].astype(jnp.float32), vec_ref[0:1], vec_ref[1:2]).astype(jnp.bfloat16)

    @pl.loop(0, count)
    def _(j):
        slot = lax.rem(j, AHEAD)
        cols = pl.ds(pl.multiple_of(j * tile, tile), tile)
        for copy in copies(j, slot):
            copy.wait()
        for n, o_ref in enumerate((q_ref, k_ref, v_ref)):
            lin = jnp.dot(h_ref[...], w_buf[slot, n], preferred_element_type=jnp.float32) + vec_ref[2 + n:3 + n, cols].astype(jnp.float32)
            if n == 2:
                o_ref[:, cols] = lin.astype(jnp.bfloat16)
            else:
                parts = []
                for c in range(tile // head_dim):
                    part = lin[:, c * head_dim:(c + 1) * head_dim]
                    parts.append(part * cos_ref[...] + pltpu.roll(part, head_dim // 2, 1) * sin_ref[...])
                o_ref[:, cols] = jnp.concatenate(parts, axis=1).astype(jnp.bfloat16)

        @pl.when(j + AHEAD < count)
        def _():
            for copy in copies(j + AHEAD, slot):
                copy.start()


def qkv_call(tokens, vectors, cos_tab, sin_signed, w_query, w_key, w_value):
    rows, d_model = tokens.shape
    cols = w_query.shape[1]
    tile = 256
    vmem = pl.BlockSpec(memory_space=pltpu.VMEM)
    hbm = pl.BlockSpec(memory_space=pl.ANY)
    shape = jax.ShapeDtypeStruct((rows, cols), jnp.bfloat16)
    return pl.pallas_call(
        qkv_kernel,
        in_specs=[vmem, vmem, vmem, vmem, hbm, hbm, hbm],
        out_specs=[vmem, vmem, vmem],
        out_shape=[shape, shape, shape],
        scratch_shapes=[pltpu.VMEM((rows, d_model), jnp.bfloat16), pltpu.VMEM((AHEAD, 3, d_model, tile), jnp.bfloat16), pltpu.SemaphoreType.DMA((AHEAD, 3))],
        compiler_params=pltpu.CompilerParams(vmem_limit_bytes=44 * 2 ** 20),
        cost_estimate=pl.CostEstimate(flops=6 * rows * d_model * cols, bytes_accessed=6 * d_model * cols, transcendentals=0),
        name='qkv',
    )(tokens, vectors, cos_tab, sin_signed, w_query, w_key, w_value)


GROUP = 8
SLOTS = 3
STEP = 16
CHUNK = 8


def attend_kernel(order_ref, pos_ref, q_ref, kn_ref, vn_ref, k_hbm, v_hbm, out_ref, k_buf, v_buf, sid_ref, sems):
    rows, heads, head_dim = q_ref.shape
    seq = k_hbm.shape[1]
    groups = rows // GROUP
    scale = head_dim ** -0.5
    key_id = lax.broadcasted_iota(jnp.int32, sid_ref.shape, 1)
    row_id = lax.broadcasted_iota(jnp.int32, sid_ref.shape, 0)
    sid_ref[...] = jnp.where(lax.rem(key_id, heads) == row_id, lax.div(key_id, heads), seq)

    @pl.loop(0, GROUP * SLOTS)
    def _(i):
        v_buf[i // GROUP, i % GROUP] = jnp.zeros(v_buf.shape[2:], v_buf.dtype)

    def group_at(n):
        return jnp.where(n & 1 == 0, n // 2, groups - 1 - n // 2)

    def chunks_at(n):
        return (pos_ref[order_ref[group_at(n) * GROUP]] + CHUNK - 1) // CHUNK

    def fetch(n):
        grp = group_at(n)
        slot = lax.rem(n, SLOTS)
        chunks = chunks_at(n)
        for k in range(1, seq // CHUNK + 1):
            @pl.when(chunks == k)
            def _(k=k):
                src = pl.ds(0, k * CHUNK)
                for i in range(GROUP):
                    tok = order_ref[grp * GROUP + i]
                    pltpu.make_async_copy(k_hbm.at[tok, src], k_buf.at[slot, i, src], sems.at[0, slot]).start()
                    pltpu.make_async_copy(v_hbm.at[tok, src], v_buf.at[slot, i, src], sems.at[1, slot]).start()

    def settle(n):
        slot = lax.rem(n, SLOTS)
        chunks = chunks_at(n)
        size = seq // CHUNK
        while size >= 1:
            @pl.when((chunks & size) != 0)
            def _(size=size):
                src = pl.ds(0, size * CHUNK)
                pltpu.make_async_copy(k_hbm.at[pl.ds(0, GROUP), src], k_buf.at[slot, :, src], sems.at[0, slot]).wait()
                pltpu.make_async_copy(v_hbm.at[pl.ds(0, GROUP), src], v_buf.at[slot, :, src], sems.at[1, slot]).wait()

            size //= 2

    def compute(n, steps):
        grp = group_at(n)
        slot = lax.rem(n, SLOTS)
        keys = steps * STEP * heads
        toks = [order_ref[grp * GROUP + i] for i in range(GROUP)]
        q_val = [q_ref[t] for t in toks]
        scores = []
        for i in range(GROUP):
            k_val = k_buf[slot, i, pl.ds(0, steps * STEP)].reshape(keys, head_dim)
            raw = lax.dot_general(q_val[i], k_val, (((1,), (1,)), ((), ())), preferred_element_type=jnp.float32)
            scores.append(jnp.where(sid_ref[:, :keys] < pos_ref[toks[i]], raw * scale, -jnp.inf))
        for i in range(GROUP):
            t = toks[i]
            s_new = jnp.sum(q_val[i].astype(jnp.float32) * kn_ref[t].astype(jnp.float32), axis=-1, keepdims=True) * scale
            top = jnp.maximum(jnp.max(scores[i], axis=-1, keepdims=True), s_new)
            e_val = jnp.exp(scores[i] - top)
            e_new = jnp.exp(s_new - top)
            inv = 1.0 / (jnp.sum(e_val, axis=-1, keepdims=True) + e_new)
            p_val = (e_val * inv).astype(jnp.bfloat16)
            p_new = (e_new * inv).astype(jnp.bfloat16).astype(jnp.float32)
            v_val = v_buf[slot, i, pl.ds(0, steps * STEP)].reshape(keys, head_dim)
            res = jnp.dot(p_val, v_val, preferred_element_type=jnp.float32) + p_new * vn_ref[t].astype(jnp.float32)
            out_ref[t] = res.astype(jnp.bfloat16)

    for n in range(SLOTS - 1):
        fetch(n)

    @pl.loop(0, groups)
    def _(n):
        @pl.when(n + SLOTS - 1 < groups)
        def _():
            fetch(n + SLOTS - 1)

        settle(n)
        most = pos_ref[order_ref[group_at(n) * GROUP]]
        steps = jnp.maximum((most + STEP - 1) // STEP, 1)
        for k in range(1, seq // STEP + 1):
            @pl.when(steps == k)
            def _(k=k):
                compute(n, k)


def attend_call(order, positions, q_rot, key_new, value_new, k_cache, v_cache):
    rows, seq, heads, head_dim = k_cache.shape
    vmem = pl.BlockSpec(memory_space=pltpu.VMEM)
    smem = pl.BlockSpec(memory_space=pltpu.SMEM)
    hbm = pl.BlockSpec(memory_space=pl.ANY)
    return pl.pallas_call(
        attend_kernel,
        in_specs=[smem, smem, vmem, vmem, vmem, hbm, hbm],
        out_specs=vmem,
        out_shape=jax.ShapeDtypeStruct((rows, heads, head_dim), jnp.bfloat16),
        scratch_shapes=[
            pltpu.VMEM((SLOTS, GROUP, seq, heads, head_dim), jnp.bfloat16),
            pltpu.VMEM((SLOTS, GROUP, seq, heads, head_dim), jnp.bfloat16),
            pltpu.VMEM((heads, seq * heads), jnp.int32),
            pltpu.SemaphoreType.DMA((2, SLOTS)),
        ],
        compiler_params=pltpu.CompilerParams(vmem_limit_bytes=48 * 2 ** 20),
        cost_estimate=pl.CostEstimate(flops=4 * rows * seq * heads * heads * head_dim, bytes_accessed=2 * rows * seq * heads * head_dim, transcendentals=0),
        name='attend',
    )(order, positions, q_rot, key_new, value_new, k_cache, v_cache)


def out_kernel(a_ref, x_hbm, vec_ref, wr_ref, pick_ref, w_hbm, mid_hbm, h_hbm, gate_hbm, x_ref, mid_ref, h_ref, gate_ref, w_buf, sems, io_sems):
    x_copy = pltpu.make_async_copy(x_hbm, x_ref, io_sems.at[0])
    results = [pltpu.make_async_copy(src, dst, io_sems.at[1 + n]) for n, (src, dst) in enumerate(((mid_ref, mid_hbm), (h_ref, h_hbm), (gate_ref, gate_hbm)))]
    x_copy.start()
    count, _, tile = w_buf.shape

    def weight(j):
        cols = pl.ds(pl.multiple_of(j * tile, tile), tile)
        return pltpu.make_async_copy(w_hbm.at[:, cols], w_buf.at[j], sems.at[j])

    for j in range(count):
        weight(j).start()
    x_copy.wait()

    @pl.loop(0, count)
    def _(j):
        weight(j).wait()
        cols = pl.ds(pl.multiple_of(j * tile, tile), tile)
        mid = x_ref[:, cols].astype(jnp.float32) + jnp.dot(a_ref[...], w_buf[j], preferred_element_type=jnp.float32) + vec_ref[5:6, cols].astype(jnp.float32)
        mid_ref[:, cols] = mid.astype(jnp.bfloat16)

    results[0].start()
    h_two = norm_rows(mid_ref[...].astype(jnp.float32), vec_ref[6:7], vec_ref[7:8]).astype(jnp.bfloat16)
    lanes = lax.broadcasted_iota(jnp.int32, (h_two.shape[0], 128), 1)
    pick_val = jnp.transpose(pick_ref[...].astype(jnp.float32))
    picks = jnp.where(lanes < 2, pick_val, 0.0)
    h_ref[:, :h_two.shape[1]] = h_two
    h_ref[:, h_two.shape[1]:] = picks.astype(jnp.bfloat16)
    results[1].start()
    logits = lax.dot_general(h_two, wr_ref[...], (((1,), (1,)), ((), ())), preferred_element_type=jnp.float32)
    ids = lax.broadcasted_iota(jnp.int32, logits.shape, 1).astype(jnp.float32)
    hit_one = ids == pick_val[:, 0:1]
    hit_two = ids == pick_val[:, 1:2]
    keep_one = pick_val[:, 2:2 + logits.shape[1]] == 1.0
    gates = []
    for keep, hit in ((keep_one, hit_one), (keep_one & jnp.logical_not(hit_one), hit_two)):
        masked = jnp.where(keep, logits, -jnp.inf)
        e_val = jnp.exp(masked - jnp.max(masked, axis=-1, keepdims=True))
        top = jnp.sum(jnp.where(hit, e_val, 0.0), axis=-1, keepdims=True)
        gates.append(top / jnp.sum(e_val, axis=-1, keepdims=True))
    lane = lax.broadcasted_iota(jnp.int32, gate_ref.shape, 1)
    gate_ref[...] = jnp.where(lane == 0, gates[0], jnp.where(lane == 1, gates[1], 0.0))
    results[2].start()
    for copy in results:
        copy.wait()


def out_call(attn_flat, tokens, vectors, w_router, picks, w_out):
    rows, d_model = tokens.shape
    tile = 256
    vmem = pl.BlockSpec(memory_space=pltpu.VMEM)
    hbm = pl.BlockSpec(memory_space=pl.ANY)
    shape = lambda cols, kind: jax.ShapeDtypeStruct((rows, cols), kind)
    return pl.pallas_call(
        out_kernel,
        in_specs=[vmem, hbm, vmem, vmem, vmem, hbm],
        out_specs=[pl.BlockSpec(memory_space=pltpu.HBM)] * 3,
        out_shape=[shape(d_model, jnp.bfloat16), shape(d_model + 128, jnp.bfloat16), shape(128, jnp.float32)],
        scratch_shapes=[
            pltpu.VMEM((rows, d_model), jnp.bfloat16),
            pltpu.VMEM((rows, d_model), jnp.bfloat16),
            pltpu.VMEM((rows, d_model + 128), jnp.bfloat16),
            pltpu.VMEM((rows, 128), jnp.float32),
            pltpu.VMEM((d_model // tile, w_out.shape[0], tile), jnp.bfloat16),
            pltpu.SemaphoreType.DMA((d_model // tile,)),
            pltpu.SemaphoreType.DMA((4,)),
        ],
        compiler_params=pltpu.CompilerParams(vmem_limit_bytes=67043328),
        cost_estimate=pl.CostEstimate(flops=2 * rows * d_model * d_model, bytes_accessed=2 * d_model * d_model, transcendentals=0),
        name='project',
    )(attn_flat, tokens, vectors, w_router, picks, w_out)


def attention_order(positions):
    ids = jnp.arange(positions.shape[0], dtype=jnp.int32)
    ahead = (positions[None, :] > positions[:, None]) | ((positions[None, :] == positions[:, None]) & (ids[None, :] < ids[:, None]))
    rank = jnp.sum(ahead.astype(jnp.int32), axis=1)
    return jnp.sum(jnp.where(rank[:, None] == ids[None, :], ids[:, None], 0), axis=0)


def moe_kernel(h_in, x_hbm, gate_hbm, wg_hbm, wu_hbm, wd_hbm, out_hbm, hb, wg, wu, wd, gate_ref, xblk, zt_ref, z_ref, acc, stg, d2d, p1a, p1b, p2a, p2b, wsem, xsem, gsend, grecv, dsend, drecv, rsend, rrecv, credit):
    me = lax.axis_index('ep')
    core = lax.rem(me, 2)
    x_pos = lax.rem(lax.div(me, 2), 2)
    y_pos = lax.div(me, 4)
    partner = me + 1 - 2 * core
    xn = me + 2 - 4 * x_pos
    yn = me + 4 - 8 * y_pos
    rows = h_in.shape[0]
    mid = rows // 2
    d_model = x_hbm.shape[1]
    half = d_model // 2
    ff = wd.shape[1]
    tile = 512
    mesh_id = pl.DeviceIdType.MESH
    part_rows = (pl.ds(0, mid), pl.ds(mid, mid))

    def remote(src, dst, send, recv, dev):
        return pltpu.make_async_remote_copy(src_ref=src, dst_ref=dst, send_sem=send, recv_sem=recv, device_id=(dev,), device_id_type=mesh_id)

    gather = []

    def add_gather(src, dst, dev):
        n = len(gather)
        gather.append(remote(src, dst, gsend.at[n], grecv.at[n], dev))
        return gather[-1]

    own = add_gather(h_in, hb.at[1], partner)
    from_x = [add_gather(h_in.at[p], hb.at[2, p], xn) for p in part_rows]
    from_y = [add_gather(h_in.at[p], hb.at[4, p], yn) for p in part_rows]
    share_x = [add_gather(hb.at[2, p], hb.at[3, p], partner) for p in part_rows]
    share_y = [add_gather(hb.at[4, p], hb.at[5, p], partner) for p in part_rows]
    far = [add_gather(hb.at[2, part_rows[0]], hb.at[6, part_rows[0]], yn), add_gather(hb.at[4, part_rows[1]], hb.at[6, part_rows[1]], xn)]
    share_far = [add_gather(hb.at[6, p], hb.at[7, p], partner) for p in part_rows]

    scatter = []

    def add_scatter(src, dst, dev):
        n = len(scatter)
        scatter.append(remote(src, dst, rsend.at[n], rrecv.at[n], dev))
        return scatter[-1]

    x_first = [add_scatter(acc.at[1 + h, 0, :, part_rows[0]], p1a.at[0, h], xn) for h in range(2)]
    y_first = [add_scatter(acc.at[1 + h, 1, :, part_rows[1]], p1b.at[0, h], yn) for h in range(2)]
    x_far = [add_scatter(acc.at[3, 0, :, part_rows[h]], p1a.at[1, h], xn) for h in range(2)]
    y_far = [add_scatter(acc.at[3, 1, :, part_rows[h]], p1b.at[1, h], yn) for h in range(2)]
    y_last = [add_scatter(acc.at[1 + h, 0, :, part_rows[1]], p2a.at[h], yn) for h in range(2)]
    x_last = [add_scatter(acc.at[1 + h, 1, :, part_rows[0]], p2b.at[h], xn) for h in range(2)]

    def weight(e):
        return [pltpu.make_async_copy(hbm.at[e], buf.at[e], wsem.at[n, e]) for n, (hbm, buf) in enumerate(((wg_hbm, wg), (wu_hbm, wu), (wd_hbm, wd)))]

    barrier = pltpu.get_barrier_semaphore()
    for dev in (partner, xn, yn):
        pl.semaphore_signal(barrier, inc=1, device_id=(dev,), device_id_type=mesh_id)
    for e in range(2):
        for copy in weight(e):
            copy.start()
    zt_ref[...] = jnp.zeros_like(zt_ref)
    pl.semaphore_wait(barrier, 3)
    for h in range(2):
        from_x[h].start()
        from_y[h].start()
    own.start()

    def load(sources):
        step = 2 * rows // len(sources)
        copies = [pltpu.make_async_copy(src, xblk.at[pl.ds(n * step, step)], xsem.at[n]) for n, src in enumerate(sources)]
        for copy in copies:
            copy.start()
        for copy in copies:
            copy.wait()

    def merge(dst, src):
        count = dst.shape[1] // 16

        @pl.loop(0, 2 * count)
        def _(i):
            slot = lax.div(i, count)
            at = pl.ds(pl.multiple_of(lax.rem(i, count) * 16, 16), 16)
            dst[slot, at] = dst[slot, at] + src[slot, at]

    def shared(r, part):
        return remote(stg.at[part], d2d.at[lax.rem(r, 2), part], dsend.at[part], drecv.at[r, part], partner)

    def gather_step(h):
        from_x[h].wait_recv()
        share_x[h].start()
        if h == 0:
            far[0].start()
        from_y[h].wait_recv()
        share_y[h].start()
        if h == 1:
            far[1].start()

    def merge_high(r, finish):
        shared(r, 1).wait_recv()
        merge(acc.at[r, 1], d2d.at[lax.rem(r, 2), 1])
        if not finish:
            for h in range(2):
                @pl.when(r == 1 + h)
                def _(h=h):
                    y_first[h].start()

            @pl.when(r < 2)
            def _():
                pl.semaphore_signal(credit, inc=1, device_id=(partner,), device_id_type=mesh_id)

    @pl.loop(0, 4)
    def _(r):
        @pl.when(r == 0)
        def _():
            own.wait_recv()
            load([h_in, hb.at[1]])

        for h in range(2):
            @pl.when(r == 1 + h)
            def _(h=h):
                share_x[h].wait_recv()
                share_y[h].wait_recv()
                load([hb.at[n, part_rows[h]] for n in (2, 4, 3, 5)])

        @pl.when(r == 3)
        def _():
            share_far[0].wait_recv()
            share_far[1].wait_recv()
            load([hb.at[6], hb.at[7]])

        @pl.loop(0, 2)
        def _(e):
            @pl.when(r == 0)
            def _():
                for copy in weight(e)[:2]:
                    copy.wait()

            x_val = xblk[:, :d_model]
            dims = (((1,), (1,)), ((), ()))
            u_val = lax.dot_general(wg[e], x_val, dims, preferred_element_type=jnp.float32)
            v_val = lax.dot_general(wu[e], x_val, dims, preferred_element_type=jnp.float32)
            zt_ref[:ff] = (jax.nn.silu(u_val) * v_val).astype(jnp.bfloat16)
            z_ref[e] = jnp.transpose(zt_ref[...])

            @pl.when((r > 0) & (e == 0))
            def _():
                merge_high(r - 1, False)

            for h in range(2):
                @pl.when((r == h) & (e == 0))
                def _(h=h):
                    gather_step(h)

        @pl.when(r == 0)
        def _():
            for e in range(2):
                weight(e)[2].wait()

        @pl.when(r == 2)
        def _():
            for h in range(2):
                far[h].wait_recv()
                share_far[h].start()

        @pl.loop(0, 2)
        def _(part):
            @pl.when(r > 0)
            def _():
                shared(r - 1, part).wait_send()

            @pl.loop(0, half // tile)
            def _(n):
                wide = pl.ds(pl.multiple_of(part * half + n * tile, tile), tile)
                slim = pl.ds(pl.multiple_of(n * tile, tile), tile)
                first = jnp.dot(z_ref[0, :, :ff], wd[0, :, wide], preferred_element_type=jnp.float32)
                second = jnp.dot(z_ref[1, :, :ff], wd[1, :, wide], preferred_element_type=jnp.float32)
                for slot in range(2):
                    choice = xblk[:, d_model:][:, slot:slot + 1].astype(jnp.float32)
                    lead = (2 * me).astype(jnp.float32)
                    val = jnp.where(choice == lead, first, jnp.where(choice == lead + 1.0, second, 0.0)).astype(jnp.bfloat16)
                    acc[r, part, slot, :, slim] = val[:rows]
                    stg[part, slot, :, slim] = val[rows:]

            @pl.when((r >= 2) & (part == 0))
            def _():
                pl.semaphore_wait(credit, 1)

            shared(r, part).start()

        shared(r, 0).wait_recv()
        merge(acc.at[r, 0], d2d.at[lax.rem(r, 2), 0])
        for h in range(2):
            @pl.when(r == 1 + h)
            def _(h=h):
                x_first[h].start()

        @pl.when(r == 3)
        def _():
            x_far[0].start()
            x_far[1].start()

    x_ref = xblk.at[pl.ds(0, rows), pl.ds(0, d_model)]
    out_ref = xblk.at[pl.ds(rows, rows), pl.ds(0, d_model)]
    late = [pltpu.make_async_copy(x_hbm, x_ref, xsem.at[0]), pltpu.make_async_copy(gate_hbm, gate_ref, xsem.at[1])]
    for copy in late:
        copy.start()
    merge_high(3, True)
    y_far[0].start()
    y_far[1].start()
    for h in range(2):
        x_far[h].wait_recv()
        merge(acc.at[1 + h, 0, :, part_rows[1]], p1a.at[1, h])
        y_last[h].start()
        y_far[h].wait_recv()
        merge(acc.at[1 + h, 1, :, part_rows[0]], p1b.at[1, h])
        x_last[h].start()
    for h in range(2):
        x_first[h].wait_recv()
        merge(acc.at[0, 0, :, part_rows[h]], p1a.at[0, h])
        y_first[h].wait_recv()
        merge(acc.at[0, 1, :, part_rows[h]], p1b.at[0, h])
    for copy in late:
        copy.wait()
    for h in range(2):
        for part, last, buf in ((0, y_last, p2a), (1, x_last, p2b)):
            last[h].wait_recv()

            @pl.loop(0, mid // 16)
            def _(i, h=h, part=part, buf=buf):
                near = pl.ds(pl.multiple_of(i * 16, 16), 16)
                at = pl.ds(pl.multiple_of(h * mid + i * 16, 16), 16)
                wide = pl.ds(part * half, half)
                gates = gate_ref[at]
                y_val = [(acc[0, part, slot, at] + buf[h, slot, near]).astype(jnp.float32) * gates[:, slot:slot + 1] for slot in range(2)]
                out_ref[at, wide] = (x_ref[at, wide].astype(jnp.float32) + (y_val[0] + y_val[1])).astype(jnp.bfloat16)

    out_copy = pltpu.make_async_copy(out_ref, out_hbm, xsem.at[2])
    out_copy.start()
    for copy in gather + scatter:
        copy.wait_send()
    for part in range(2):
        shared(3, part).wait_send()
    out_copy.wait()


def moe_call(h_ext, x_mid, gates, w_gate, w_up, w_down):
    rows, d_model = x_mid.shape
    half = d_model // 2
    ff = w_gate.shape[2]
    ff_pad = pl.cdiv(ff, 128) * 128
    width = h_ext.shape[1]
    hbm = pl.BlockSpec(memory_space=pl.ANY)
    bf = jnp.bfloat16
    dma = pltpu.SemaphoreType.DMA
    out, _ = pl.pallas_call(
        moe_kernel,
        in_specs=[hbm] * 6,
        out_specs=[hbm, hbm],
        out_shape=[jax.ShapeDtypeStruct((rows, d_model), bf), jax.ShapeDtypeStruct((8, rows, width), bf)],
        scratch_shapes=[
            pltpu.VMEM((2, ff, d_model), bf),
            pltpu.VMEM((2, ff, d_model), bf),
            pltpu.VMEM((2, ff, d_model), bf),
            pltpu.VMEM(gates.shape, gates.dtype),
            pltpu.VMEM((2 * rows, width), bf),
            pltpu.VMEM((ff_pad, 2 * rows), bf),
            pltpu.VMEM((2, 2 * rows, ff_pad), bf),
            pltpu.VMEM((4, 2, 2, rows, half), bf),
            pltpu.VMEM((2, 2, rows, half), bf),
            pltpu.VMEM((2, 2, 2, rows, half), bf),
            pltpu.VMEM((2, 2, 2, rows // 2, half), bf),
            pltpu.VMEM((2, 2, 2, rows // 2, half), bf),
            pltpu.VMEM((2, 2, rows // 2, half), bf),
            pltpu.VMEM((2, 2, rows // 2, half), bf),
            dma((3, 2)),
            dma((4,)),
            dma((13,)),
            dma((13,)),
            dma((2,)),
            dma((4, 2)),
            dma((12,)),
            dma((12,)),
            pltpu.SemaphoreType.REGULAR,
        ],
        compiler_params=pltpu.CompilerParams(vmem_limit_bytes=67043328, collective_id=0, has_side_effects=True),
        name='moe',
    )(h_ext, x_mid, gates, jnp.swapaxes(w_gate, 1, 2), jnp.swapaxes(w_up, 1, 2), w_down)
    return out


def solution(mesh):
    def local_step(tokens, k_cache, v_cache, positions, expert_one, expert_two, eligible, ln1_gain, ln1_bias, w_query, b_query, w_key, b_key, w_value, b_value, w_out, b_out, ln2_gain, ln2_bias, w_router, w_gate, w_up, w_down):
        tok_count, seq_len, heads, head_dim = k_cache.shape
        d_model = tokens.shape[1]
        cos_tab, sin_tab = rope_tables(positions, head_dim)
        sign = jnp.where(jnp.arange(head_dim) < head_dim // 2, -1.0, 1.0)
        vectors = row_stack([ln1_gain, ln1_bias, b_query, b_key, b_value, b_out, ln2_gain, ln2_bias])
        which = lax.broadcasted_iota(jnp.int32, (128, tok_count), 0)
        picks = jnp.where(which == 0, expert_one[None, :], jnp.where(which == 1, expert_two[None, :], jnp.pad(eligible.T, ((2, 110), (0, 0)))))
        q_flat, k_flat, v_flat = qkv_call(tokens, vectors, cos_tab, sin_tab * sign[None, :], w_query, w_key, w_value)
        split = lambda t: t.reshape(tok_count, heads, head_dim)
        key_new, value_new = split(k_flat), split(v_flat)
        attn = attend_call(attention_order(positions), positions, split(q_flat), key_new, value_new, k_cache, v_cache)
        x_mid, h_ext, gates = out_call(attn.reshape(tok_count, heads * head_dim), tokens, vectors, w_router.T, picks, w_out)
        tokens_out = moe_call(h_ext, x_mid, gates, w_gate, w_up, w_down)
        return tokens_out, key_new, value_new

    row_spec = P('ep', None)
    cache_spec = P('ep', None, None, None)
    vec_spec = P('ep')
    rep_one = P(None)
    rep_two = P(None, None)
    expert_spec = P('ep', None, None)
    in_specs = (row_spec, cache_spec, cache_spec, vec_spec, vec_spec, vec_spec, row_spec, rep_one, rep_one, rep_two, rep_one, rep_two, rep_one, rep_two, rep_one, rep_two, rep_one, rep_one, rep_one, rep_two, expert_spec, expert_spec, expert_spec)
    out_specs = (row_spec, expert_spec, expert_spec)
    return jax.shard_map(local_step, mesh=mesh, in_specs=in_specs, out_specs=out_specs, check_vma=False)
```

```python
import jax
import jax.numpy as jnp
from jax import lax
from jax.experimental import pallas as pl
from jax.experimental.pallas import tpu as pltpu
from jax.sharding import PartitionSpec as P

ROPE_BASE = 10000.0
LN_EPS = 1e-5


def rope_tables(positions, head_dim):
    half_dim = head_dim // 2
    inv_freq = ROPE_BASE ** (jnp.arange(half_dim, dtype=jnp.float32) * (-2.0 / head_dim))
    angles = positions.astype(jnp.float32)[:, None] * inv_freq[None, :]
    angles = jnp.concatenate([angles, angles], axis=-1)
    return jnp.cos(angles), jnp.sin(angles)


def norm_rows(x_val, gain, bias):
    mean_val = jnp.mean(x_val, axis=-1, keepdims=True)
    centered = x_val - mean_val
    var_val = jnp.mean(centered * centered, axis=-1, keepdims=True)
    return centered * lax.rsqrt(var_val + LN_EPS) * gain.astype(jnp.float32) + bias.astype(jnp.float32)


def row_stack(vectors):
    which = lax.broadcasted_iota(jnp.int32, (len(vectors), vectors[0].shape[0]), 0)
    out = jnp.zeros((len(vectors), vectors[0].shape[0]), vectors[0].dtype)
    for n, vec in enumerate(vectors):
        out = jnp.where(which == n, vec[None, :], out)
    return out


AHEAD = 4


def qkv_kernel(x_ref, vec_ref, cos_ref, sin_ref, wq_hbm, wk_hbm, wv_hbm, q_ref, k_ref, v_ref, h_ref, w_buf, sems):
    rows, d_model = x_ref.shape
    tile = w_buf.shape[3]
    count = q_ref.shape[1] // tile
    head_dim = cos_ref.shape[1]

    def copies(j, slot):
        cols = pl.ds(pl.multiple_of(j * tile, tile), tile)
        return [pltpu.make_async_copy(hbm.at[:, cols], w_buf.at[slot, n], sems.at[slot, n]) for n, hbm in enumerate((wq_hbm, wk_hbm, wv_hbm))]

    for j in range(AHEAD):
        for copy in copies(j, j):
            copy.start()
    h_ref[...] = norm_rows(x_ref[...].astype(jnp.float32), vec_ref[0:1], vec_ref[1:2]).astype(jnp.bfloat16)

    @pl.loop(0, count)
    def _(j):
        slot = lax.rem(j, AHEAD)
        cols = pl.ds(pl.multiple_of(j * tile, tile), tile)
        for copy in copies(j, slot):
            copy.wait()
        for n, o_ref in enumerate((q_ref, k_ref, v_ref)):
            lin = jnp.dot(h_ref[...], w_buf[slot, n], preferred_element_type=jnp.float32) + vec_ref[2 + n:3 + n, cols].astype(jnp.float32)
            if n == 2:
                o_ref[:, cols] = lin.astype(jnp.bfloat16)
            else:
                parts = []
                for c in range(tile // head_dim):
                    part = lin[:, c * head_dim:(c + 1) * head_dim]
                    parts.append(part * cos_ref[...] + pltpu.roll(part, head_dim // 2, 1) * sin_ref[...])
                o_ref[:, cols] = jnp.concatenate(parts, axis=1).astype(jnp.bfloat16)

        @pl.when(j + AHEAD < count)
        def _():
            for copy in copies(j + AHEAD, slot):
                copy.start()


def qkv_call(tokens, vectors, cos_tab, sin_signed, w_query, w_key, w_value):
    rows, d_model = tokens.shape
    cols = w_query.shape[1]
    tile = 256
    vmem = pl.BlockSpec(memory_space=pltpu.VMEM)
    hbm = pl.BlockSpec(memory_space=pl.ANY)
    shape = jax.ShapeDtypeStruct((rows, cols), jnp.bfloat16)
    return pl.pallas_call(
        qkv_kernel,
        in_specs=[vmem, vmem, vmem, vmem, hbm, hbm, hbm],
        out_specs=[vmem, vmem, vmem],
        out_shape=[shape, shape, shape],
        scratch_shapes=[pltpu.VMEM((rows, d_model), jnp.bfloat16), pltpu.VMEM((AHEAD, 3, d_model, tile), jnp.bfloat16), pltpu.SemaphoreType.DMA((AHEAD, 3))],
        compiler_params=pltpu.CompilerParams(vmem_limit_bytes=44 * 2 ** 20),
        cost_estimate=pl.CostEstimate(flops=6 * rows * d_model * cols, bytes_accessed=6 * d_model * cols, transcendentals=0),
        name='qkv',
    )(tokens, vectors, cos_tab, sin_signed, w_query, w_key, w_value)


GROUP = 8
SLOTS = 3
STEP = 8
CHUNK = 8


def attend_kernel(order_ref, pos_ref, q_ref, kn_ref, vn_ref, k_hbm, v_hbm, out_ref, k_buf, v_buf, sid_ref, sems):
    rows, heads, head_dim = q_ref.shape
    seq = k_hbm.shape[1]
    groups = rows // GROUP
    scale = head_dim ** -0.5
    key_id = lax.broadcasted_iota(jnp.int32, sid_ref.shape, 1)
    row_id = lax.broadcasted_iota(jnp.int32, sid_ref.shape, 0)
    sid_ref[...] = jnp.where(lax.rem(key_id, heads) == row_id, lax.div(key_id, heads), seq)

    @pl.loop(0, GROUP * SLOTS)
    def _(i):
        v_buf[i // GROUP, i % GROUP] = jnp.zeros(v_buf.shape[2:], v_buf.dtype)

    def group_at(n):
        return jnp.where(n & 1 == 0, n // 2, groups - 1 - n // 2)

    def chunks_at(n):
        return (pos_ref[order_ref[group_at(n) * GROUP]] + CHUNK - 1) // CHUNK

    def fetch(n):
        grp = group_at(n)
        slot = lax.rem(n, SLOTS)
        chunks = chunks_at(n)
        for k in range(1, seq // CHUNK + 1):
            @pl.when(chunks == k)
            def _(k=k):
                src = pl.ds(0, k * CHUNK)

                @pl.loop(0, GROUP)
                def _(i):
                    tok = order_ref[grp * GROUP + i]
                    pltpu.make_async_copy(k_hbm.at[tok, src], k_buf.at[slot, i, src], sems.at[0, slot]).start()
                    pltpu.make_async_copy(v_hbm.at[tok, src], v_buf.at[slot, i, src], sems.at[1, slot]).start()

    def settle(n):
        slot = lax.rem(n, SLOTS)
        chunks = chunks_at(n)
        size = seq // CHUNK
        while size >= 1:
            @pl.when((chunks & size) != 0)
            def _(size=size):
                src = pl.ds(0, size * CHUNK)
                pltpu.make_async_copy(k_hbm.at[pl.ds(0, GROUP), src], k_buf.at[slot, :, src], sems.at[0, slot]).wait()
                pltpu.make_async_copy(v_hbm.at[pl.ds(0, GROUP), src], v_buf.at[slot, :, src], sems.at[1, slot]).wait()

            size //= 2

    def compute(n, steps):
        grp = group_at(n)
        slot = lax.rem(n, SLOTS)
        keys = steps * STEP * heads
        toks = [order_ref[grp * GROUP + i] for i in range(GROUP)]
        q_val = [q_ref[t] for t in toks]
        scores = []
        for i in range(GROUP):
            k_val = k_buf[slot, i, pl.ds(0, steps * STEP)].reshape(keys, head_dim)
            raw = lax.dot_general(q_val[i], k_val, (((1,), (1,)), ((), ())), preferred_element_type=jnp.float32)
            scores.append(jnp.where(sid_ref[:, :keys] < pos_ref[toks[i]], raw * scale, -jnp.inf))
        for i in range(GROUP):
            t = toks[i]
            s_new = jnp.sum(q_val[i].astype(jnp.float32) * kn_ref[t].astype(jnp.float32), axis=-1, keepdims=True) * scale
            top = jnp.maximum(jnp.max(scores[i], axis=-1, keepdims=True), s_new)
            e_val = jnp.exp(scores[i] - top)
            e_new = jnp.exp(s_new - top)
            inv = 1.0 / (jnp.sum(e_val, axis=-1, keepdims=True) + e_new)
            p_val = (e_val * inv).astype(jnp.bfloat16)
            p_new = (e_new * inv).astype(jnp.bfloat16).astype(jnp.float32)
            v_val = v_buf[slot, i, pl.ds(0, steps * STEP)].reshape(keys, head_dim)
            res = jnp.dot(p_val, v_val, preferred_element_type=jnp.float32) + p_new * vn_ref[t].astype(jnp.float32)
            out_ref[t] = res.astype(jnp.bfloat16)

    for n in range(SLOTS - 1):
        fetch(n)

    @pl.loop(0, groups)
    def _(n):
        @pl.when(n + SLOTS - 1 < groups)
        def _():
            fetch(n + SLOTS - 1)

        settle(n)
        most = pos_ref[order_ref[group_at(n) * GROUP]]
        steps = jnp.maximum((most + STEP - 1) // STEP, 1)
        for k in range(1, seq // STEP + 1):
            @pl.when(steps == k)
            def _(k=k):
                compute(n, k)


def attend_call(order, positions, q_rot, key_new, value_new, k_cache, v_cache):
    rows, seq, heads, head_dim = k_cache.shape
    vmem = pl.BlockSpec(memory_space=pltpu.VMEM)
    smem = pl.BlockSpec(memory_space=pltpu.SMEM)
    hbm = pl.BlockSpec(memory_space=pl.ANY)
    return pl.pallas_call(
        attend_kernel,
        in_specs=[smem, smem, vmem, vmem, vmem, hbm, hbm],
        out_specs=vmem,
        out_shape=jax.ShapeDtypeStruct((rows, heads, head_dim), jnp.bfloat16),
        scratch_shapes=[
            pltpu.VMEM((SLOTS, GROUP, seq, heads, head_dim), jnp.bfloat16),
            pltpu.VMEM((SLOTS, GROUP, seq, heads, head_dim), jnp.bfloat16),
            pltpu.VMEM((heads, seq * heads), jnp.int32),
            pltpu.SemaphoreType.DMA((2, SLOTS)),
        ],
        compiler_params=pltpu.CompilerParams(vmem_limit_bytes=48 * 2 ** 20),
        cost_estimate=pl.CostEstimate(flops=4 * rows * seq * heads * heads * head_dim, bytes_accessed=2 * rows * seq * heads * head_dim, transcendentals=0),
        name='attend',
    )(order, positions, q_rot, key_new, value_new, k_cache, v_cache)


def out_kernel(a_ref, x_ref, vec_ref, wr_ref, pick_ref, w_hbm, mid_ref, h_ref, gate_ref, w_buf, sems):
    count, _, tile = w_buf.shape

    def weight(j):
        cols = pl.ds(pl.multiple_of(j * tile, tile), tile)
        return pltpu.make_async_copy(w_hbm.at[:, cols], w_buf.at[j], sems.at[j])

    for j in range(count):
        weight(j).start()

    @pl.loop(0, count)
    def _(j):
        weight(j).wait()
        cols = pl.ds(pl.multiple_of(j * tile, tile), tile)
        mid = x_ref[:, cols].astype(jnp.float32) + jnp.dot(a_ref[...], w_buf[j], preferred_element_type=jnp.float32) + vec_ref[5:6, cols].astype(jnp.float32)
        mid_ref[:, cols] = mid.astype(jnp.bfloat16)

    h_two = norm_rows(mid_ref[...].astype(jnp.float32), vec_ref[6:7], vec_ref[7:8]).astype(jnp.bfloat16)
    lanes = lax.broadcasted_iota(jnp.int32, (h_two.shape[0], 128), 1)
    pick_val = jnp.transpose(pick_ref[...].astype(jnp.float32))
    picks = jnp.where(lanes < 2, pick_val, 0.0)
    h_ref[:, :h_two.shape[1]] = h_two
    h_ref[:, h_two.shape[1]:] = picks.astype(jnp.bfloat16)
    logits = lax.dot_general(h_two, wr_ref[...], (((1,), (1,)), ((), ())), preferred_element_type=jnp.float32)
    ids = lax.broadcasted_iota(jnp.int32, logits.shape, 1).astype(jnp.float32)
    hit_one = ids == pick_val[:, 0:1]
    hit_two = ids == pick_val[:, 1:2]
    keep_one = pick_val[:, 2:2 + logits.shape[1]] == 1.0
    gates = []
    for keep, hit in ((keep_one, hit_one), (keep_one & jnp.logical_not(hit_one), hit_two)):
        masked = jnp.where(keep, logits, -jnp.inf)
        e_val = jnp.exp(masked - jnp.max(masked, axis=-1, keepdims=True))
        top = jnp.sum(jnp.where(hit, e_val, 0.0), axis=-1, keepdims=True)
        gates.append(top / jnp.sum(e_val, axis=-1, keepdims=True))
    lane = lax.broadcasted_iota(jnp.int32, gate_ref.shape, 1)
    gate_ref[...] = jnp.where(lane == 0, gates[0], jnp.where(lane == 1, gates[1], 0.0))


def out_call(attn_flat, tokens, vectors, w_router, picks, w_out):
    rows, d_model = tokens.shape
    tile = 256
    vmem = pl.BlockSpec(memory_space=pltpu.VMEM)
    shape = lambda cols, kind: jax.ShapeDtypeStruct((rows, cols), kind)
    return pl.pallas_call(
        out_kernel,
        in_specs=[vmem] * 5 + [pl.BlockSpec(memory_space=pl.ANY)],
        out_specs=[vmem] * 3,
        out_shape=[shape(d_model, jnp.bfloat16), shape(d_model + 128, jnp.bfloat16), shape(128, jnp.float32)],
        scratch_shapes=[pltpu.VMEM((d_model // tile, w_out.shape[0], tile), jnp.bfloat16), pltpu.SemaphoreType.DMA((d_model // tile,))],
        compiler_params=pltpu.CompilerParams(vmem_limit_bytes=48 * 2 ** 20),
        cost_estimate=pl.CostEstimate(flops=2 * rows * d_model * d_model, bytes_accessed=2 * d_model * d_model, transcendentals=0),
        name='project',
    )(attn_flat, tokens, vectors, w_router, picks, w_out)


def attention_order(positions):
    ids = jnp.arange(positions.shape[0], dtype=jnp.int32)
    ahead = (positions[None, :] > positions[:, None]) | ((positions[None, :] == positions[:, None]) & (ids[None, :] < ids[:, None]))
    rank = jnp.sum(ahead.astype(jnp.int32), axis=1)
    return jnp.sum(jnp.where(rank[:, None] == ids[None, :], ids[:, None], 0), axis=0)


def moe_kernel(h_in, x_hbm, gate_hbm, wg_hbm, wu_hbm, wd_hbm, out_hbm, hb, wg, wu, wd, gate_ref, xblk, zt_ref, z_ref, acc, stg, d2d, p1a, p1b, p2a, p2b, wsem, xsem, gsend, grecv, dsend, drecv, rsend, rrecv, credit):
    me = lax.axis_index('ep')
    core = lax.rem(me, 2)
    x_pos = lax.rem(lax.div(me, 2), 2)
    y_pos = lax.div(me, 4)
    partner = me + 1 - 2 * core
    xn = me + 2 - 4 * x_pos
    yn = me + 4 - 8 * y_pos
    rows = h_in.shape[0]
    mid = rows // 2
    d_model = x_hbm.shape[1]
    half = d_model // 2
    ff = wd.shape[1]
    tile = 512
    mesh_id = pl.DeviceIdType.MESH
    part_rows = (pl.ds(0, mid), pl.ds(mid, mid))

    def remote(src, dst, send, recv, dev):
        return pltpu.make_async_remote_copy(src_ref=src, dst_ref=dst, send_sem=send, recv_sem=recv, device_id=(dev,), device_id_type=mesh_id)

    gather = []

    def add_gather(src, dst, dev):
        n = len(gather)
        gather.append(remote(src, dst, gsend.at[n], grecv.at[n], dev))
        return gather[-1]

    own = add_gather(h_in, hb.at[1], partner)
    from_x = [add_gather(h_in.at[p], hb.at[2, p], xn) for p in part_rows]
    from_y = [add_gather(h_in.at[p], hb.at[4, p], yn) for p in part_rows]
    share_x = [add_gather(hb.at[2, p], hb.at[3, p], partner) for p in part_rows]
    share_y = [add_gather(hb.at[4, p], hb.at[5, p], partner) for p in part_rows]
    far = [add_gather(hb.at[2, part_rows[0]], hb.at[6, part_rows[0]], yn), add_gather(hb.at[4, part_rows[1]], hb.at[6, part_rows[1]], xn)]
    share_far = [add_gather(hb.at[6, p], hb.at[7, p], partner) for p in part_rows]

    scatter = []

    def add_scatter(src, dst, dev):
        n = len(scatter)
        scatter.append(remote(src, dst, rsend.at[n], rrecv.at[n], dev))
        return scatter[-1]

    x_first = [add_scatter(acc.at[1 + h, 0, :, part_rows[0]], p1a.at[0, h], xn) for h in range(2)]
    y_first = [add_scatter(acc.at[1 + h, 1, :, part_rows[1]], p1b.at[0, h], yn) for h in range(2)]
    x_far = [add_scatter(acc.at[3, 0, :, part_rows[h]], p1a.at[1, h], xn) for h in range(2)]
    y_far = [add_scatter(acc.at[3, 1, :, part_rows[h]], p1b.at[1, h], yn) for h in range(2)]
    y_last = [add_scatter(acc.at[1 + h, 0, :, part_rows[1]], p2a.at[h], yn) for h in range(2)]
    x_last = [add_scatter(acc.at[1 + h, 1, :, part_rows[0]], p2b.at[h], xn) for h in range(2)]

    def weight(e):
        return [pltpu.make_async_copy(hbm.at[e], buf.at[e], wsem.at[n, e]) for n, (hbm, buf) in enumerate(((wg_hbm, wg), (wu_hbm, wu), (wd_hbm, wd)))]

    barrier = pltpu.get_barrier_semaphore()
    for dev in (partner, xn, yn):
        pl.semaphore_signal(barrier, inc=1, device_id=(dev,), device_id_type=mesh_id)
    for e in range(2):
        for copy in weight(e):
            copy.start()
    zt_ref[...] = jnp.zeros_like(zt_ref)
    pl.semaphore_wait(barrier, 3)
    for h in range(2):
        from_x[h].start()
        from_y[h].start()
    own.start()

    def load(sources):
        step = 2 * rows // len(sources)
        copies = [pltpu.make_async_copy(src, xblk.at[pl.ds(n * step, step)], xsem.at[n]) for n, src in enumerate(sources)]
        for copy in copies:
            copy.start()
        for copy in copies:
            copy.wait()

    def merge(dst, src):
        count = dst.shape[1] // 16

        @pl.loop(0, 2 * count)
        def _(i):
            slot = lax.div(i, count)
            at = pl.ds(pl.multiple_of(lax.rem(i, count) * 16, 16), 16)
            dst[slot, at] = dst[slot, at] + src[slot, at]

    def shared(r, part):
        return remote(stg.at[part], d2d.at[lax.rem(r, 2), part], dsend.at[part], drecv.at[r, part], partner)

    def gather_step(h):
        from_x[h].wait_recv()
        share_x[h].start()
        if h == 0:
            far[0].start()
        from_y[h].wait_recv()
        share_y[h].start()
        if h == 1:
            far[1].start()

    def merge_high(r, finish):
        shared(r, 1).wait_recv()
        merge(acc.at[r, 1], d2d.at[lax.rem(r, 2), 1])
        if not finish:
            for h in range(2):
                @pl.when(r == 1 + h)
                def _(h=h):
                    y_first[h].start()

            @pl.when(r < 2)
            def _():
                pl.semaphore_signal(credit, inc=1, device_id=(partner,), device_id_type=mesh_id)

    @pl.loop(0, 4)
    def _(r):
        @pl.when(r == 0)
        def _():
            own.wait_recv()
            load([h_in, hb.at[1]])

        for h in range(2):
            @pl.when(r == 1 + h)
            def _(h=h):
                share_x[h].wait_recv()
                share_y[h].wait_recv()
                load([hb.at[n, part_rows[h]] for n in (2, 4, 3, 5)])

        @pl.when(r == 3)
        def _():
            share_far[0].wait_recv()
            share_far[1].wait_recv()
            load([hb.at[6], hb.at[7]])

        @pl.loop(0, 2)
        def _(e):
            @pl.when(r == 0)
            def _():
                for copy in weight(e)[:2]:
                    copy.wait()

            x_val = xblk[:, :d_model]
            dims = (((1,), (1,)), ((), ()))
            u_val = lax.dot_general(wg[e], x_val, dims, preferred_element_type=jnp.float32)
            v_val = lax.dot_general(wu[e], x_val, dims, preferred_element_type=jnp.float32)
            zt_ref[:ff] = (jax.nn.silu(u_val) * v_val).astype(jnp.bfloat16)
            z_ref[e] = jnp.transpose(zt_ref[...])

            @pl.when((r > 0) & (e == 0))
            def _():
                merge_high(r - 1, False)

            for h in range(2):
                @pl.when((r == h) & (e == 0))
                def _(h=h):
                    gather_step(h)

        @pl.when(r == 0)
        def _():
            for e in range(2):
                weight(e)[2].wait()

        @pl.when(r == 2)
        def _():
            for h in range(2):
                far[h].wait_recv()
                share_far[h].start()

        @pl.loop(0, 2)
        def _(part):
            @pl.when(r > 0)
            def _():
                shared(r - 1, part).wait_send()

            @pl.loop(0, half // tile)
            def _(n):
                wide = pl.ds(pl.multiple_of(part * half + n * tile, tile), tile)
                slim = pl.ds(pl.multiple_of(n * tile, tile), tile)
                first = jnp.dot(z_ref[0, :, :ff], wd[0, :, wide], preferred_element_type=jnp.float32)
                second = jnp.dot(z_ref[1, :, :ff], wd[1, :, wide], preferred_element_type=jnp.float32)
                for slot in range(2):
                    choice = xblk[:, d_model:][:, slot:slot + 1].astype(jnp.float32)
                    lead = (2 * me).astype(jnp.float32)
                    val = jnp.where(choice == lead, first, jnp.where(choice == lead + 1.0, second, 0.0)).astype(jnp.bfloat16)
                    acc[r, part, slot, :, slim] = val[:rows]
                    stg[part, slot, :, slim] = val[rows:]

            @pl.when((r >= 2) & (part == 0))
            def _():
                pl.semaphore_wait(credit, 1)

            shared(r, part).start()

        shared(r, 0).wait_recv()
        merge(acc.at[r, 0], d2d.at[lax.rem(r, 2), 0])
        for h in range(2):
            @pl.when(r == 1 + h)
            def _(h=h):
                x_first[h].start()

        @pl.when(r == 3)
        def _():
            x_far[0].start()
            x_far[1].start()

    x_ref = xblk.at[pl.ds(0, rows), pl.ds(0, d_model)]
    out_ref = xblk.at[pl.ds(rows, rows), pl.ds(0, d_model)]
    late = [pltpu.make_async_copy(x_hbm, x_ref, xsem.at[0]), pltpu.make_async_copy(gate_hbm, gate_ref, xsem.at[1])]
    for copy in late:
        copy.start()
    merge_high(3, True)
    y_far[0].start()
    y_far[1].start()
    for h in range(2):
        x_far[h].wait_recv()
        merge(acc.at[1 + h, 0, :, part_rows[1]], p1a.at[1, h])
        y_last[h].start()
        y_far[h].wait_recv()
        merge(acc.at[1 + h, 1, :, part_rows[0]], p1b.at[1, h])
        x_last[h].start()
    for h in range(2):
        x_first[h].wait_recv()
        merge(acc.at[0, 0, :, part_rows[h]], p1a.at[0, h])
        y_first[h].wait_recv()
        merge(acc.at[0, 1, :, part_rows[h]], p1b.at[0, h])
    for copy in late:
        copy.wait()
    for h in range(2):
        for part, last, buf in ((0, y_last, p2a), (1, x_last, p2b)):
            last[h].wait_recv()

            @pl.loop(0, mid // 16)
            def _(i, h=h, part=part, buf=buf):
                near = pl.ds(pl.multiple_of(i * 16, 16), 16)
                at = pl.ds(pl.multiple_of(h * mid + i * 16, 16), 16)
                wide = pl.ds(part * half, half)
                gates = gate_ref[at]
                y_val = [(acc[0, part, slot, at] + buf[h, slot, near]).astype(jnp.float32) * gates[:, slot:slot + 1] for slot in range(2)]
                out_ref[at, wide] = (x_ref[at, wide].astype(jnp.float32) + (y_val[0] + y_val[1])).astype(jnp.bfloat16)

    out_copy = pltpu.make_async_copy(out_ref, out_hbm, xsem.at[2])
    out_copy.start()
    for copy in gather + scatter:
        copy.wait_send()
    for part in range(2):
        shared(3, part).wait_send()
    out_copy.wait()


def moe_call(h_ext, x_mid, gates, w_gate, w_up, w_down):
    rows, d_model = x_mid.shape
    half = d_model // 2
    ff = w_gate.shape[2]
    ff_pad = pl.cdiv(ff, 128) * 128
    width = h_ext.shape[1]
    hbm = pl.BlockSpec(memory_space=pl.ANY)
    bf = jnp.bfloat16
    dma = pltpu.SemaphoreType.DMA
    out, _ = pl.pallas_call(
        moe_kernel,
        in_specs=[hbm] * 6,
        out_specs=[hbm, hbm],
        out_shape=[jax.ShapeDtypeStruct((rows, d_model), bf), jax.ShapeDtypeStruct((8, rows, width), bf)],
        scratch_shapes=[
            pltpu.VMEM((2, ff, d_model), bf),
            pltpu.VMEM((2, ff, d_model), bf),
            pltpu.VMEM((2, ff, d_model), bf),
            pltpu.VMEM(gates.shape, gates.dtype),
            pltpu.VMEM((2 * rows, width), bf),
            pltpu.VMEM((ff_pad, 2 * rows), bf),
            pltpu.VMEM((2, 2 * rows, ff_pad), bf),
            pltpu.VMEM((4, 2, 2, rows, half), bf),
            pltpu.VMEM((2, 2, rows, half), bf),
            pltpu.VMEM((2, 2, 2, rows, half), bf),
            pltpu.VMEM((2, 2, 2, rows // 2, half), bf),
            pltpu.VMEM((2, 2, 2, rows // 2, half), bf),
            pltpu.VMEM((2, 2, rows // 2, half), bf),
            pltpu.VMEM((2, 2, rows // 2, half), bf),
            dma((3, 2)),
            dma((4,)),
            dma((13,)),
            dma((13,)),
            dma((2,)),
            dma((4, 2)),
            dma((12,)),
            dma((12,)),
            pltpu.SemaphoreType.REGULAR,
        ],
        compiler_params=pltpu.CompilerParams(vmem_limit_bytes=67043328, collective_id=0, has_side_effects=True),
        name='moe',
    )(h_ext, x_mid, gates, jnp.swapaxes(w_gate, 1, 2), jnp.swapaxes(w_up, 1, 2), w_down)
    return out


def solution(mesh):
    def local_step(tokens, k_cache, v_cache, positions, expert_one, expert_two, eligible, ln1_gain, ln1_bias, w_query, b_query, w_key, b_key, w_value, b_value, w_out, b_out, ln2_gain, ln2_bias, w_router, w_gate, w_up, w_down):
        tok_count, seq_len, heads, head_dim = k_cache.shape
        d_model = tokens.shape[1]
        cos_tab, sin_tab = rope_tables(positions, head_dim)
        sign = jnp.where(jnp.arange(head_dim) < head_dim // 2, -1.0, 1.0)
        vectors = row_stack([ln1_gain, ln1_bias, b_query, b_key, b_value, b_out, ln2_gain, ln2_bias])
        which = lax.broadcasted_iota(jnp.int32, (128, tok_count), 0)
        picks = jnp.where(which == 0, expert_one[None, :], jnp.where(which == 1, expert_two[None, :], jnp.pad(eligible.T, ((2, 110), (0, 0)))))
        q_flat, k_flat, v_flat = qkv_call(tokens, vectors, cos_tab, sin_tab * sign[None, :], w_query, w_key, w_value)
        split = lambda t: t.reshape(tok_count, heads, head_dim)
        key_new, value_new = split(k_flat), split(v_flat)
        attn = attend_call(attention_order(positions), positions, split(q_flat), key_new, value_new, k_cache, v_cache)
        x_mid, h_ext, gates = out_call(attn.reshape(tok_count, heads * head_dim), tokens, vectors, w_router.T, picks, w_out)
        tokens_out = moe_call(h_ext, x_mid, gates, w_gate, w_up, w_down)
        return tokens_out, key_new, value_new

    row_spec = P('ep', None)
    cache_spec = P('ep', None, None, None)
    vec_spec = P('ep')
    rep_one = P(None)
    rep_two = P(None, None)
    expert_spec = P('ep', None, None)
    in_specs = (row_spec, cache_spec, cache_spec, vec_spec, vec_spec, vec_spec, row_spec, rep_one, rep_one, rep_two, rep_one, rep_two, rep_one, rep_two, rep_one, rep_two, rep_one, rep_one, rep_one, rep_two, expert_spec, expert_spec, expert_spec)
    out_specs = (row_spec, expert_spec, expert_spec)
    return jax.shard_map(local_step, mesh=mesh, in_specs=in_specs, out_specs=out_specs, check_vma=False)
```

```python
import jax
import jax.numpy as jnp
from jax import lax
from jax.experimental import pallas as pl
from jax.experimental.pallas import tpu as pltpu
from jax.sharding import PartitionSpec as P

ROPE_BASE = 10000.0
LN_EPS = 1e-5


def rope_tables(positions, head_dim):
    half_dim = head_dim // 2
    inv_freq = ROPE_BASE ** (jnp.arange(half_dim, dtype=jnp.float32) * (-2.0 / head_dim))
    angles = positions.astype(jnp.float32)[:, None] * inv_freq[None, :]
    angles = jnp.concatenate([angles, angles], axis=-1)
    return jnp.cos(angles), jnp.sin(angles)


def norm_rows(x_val, gain, bias):
    mean_val = jnp.mean(x_val, axis=-1, keepdims=True)
    centered = x_val - mean_val
    var_val = jnp.mean(centered * centered, axis=-1, keepdims=True)
    return centered * lax.rsqrt(var_val + LN_EPS) * gain.astype(jnp.float32) + bias.astype(jnp.float32)


def row_stack(vectors):
    which = lax.broadcasted_iota(jnp.int32, (len(vectors), vectors[0].shape[0]), 0)
    out = jnp.zeros((len(vectors), vectors[0].shape[0]), vectors[0].dtype)
    for n, vec in enumerate(vectors):
        out = jnp.where(which == n, vec[None, :], out)
    return out


AHEAD = 4


def qkv_kernel(x_ref, vec_ref, cos_ref, sin_ref, wq_hbm, wk_hbm, wv_hbm, q_ref, k_ref, v_ref, h_ref, w_buf, sems):
    rows, d_model = x_ref.shape
    tile = w_buf.shape[3]
    count = q_ref.shape[1] // tile
    head_dim = cos_ref.shape[1]

    def copies(j, slot):
        cols = pl.ds(pl.multiple_of(j * tile, tile), tile)
        return [pltpu.make_async_copy(hbm.at[:, cols], w_buf.at[slot, n], sems.at[slot, n]) for n, hbm in enumerate((wq_hbm, wk_hbm, wv_hbm))]

    for j in range(AHEAD):
        for copy in copies(j, j):
            copy.start()
    h_ref[...] = norm_rows(x_ref[...].astype(jnp.float32), vec_ref[0:1], vec_ref[1:2]).astype(jnp.bfloat16)

    @pl.loop(0, count)
    def _(j):
        slot = lax.rem(j, AHEAD)
        cols = pl.ds(pl.multiple_of(j * tile, tile), tile)
        for copy in copies(j, slot):
            copy.wait()
        for n, o_ref in enumerate((q_ref, k_ref, v_ref)):
            lin = jnp.dot(h_ref[...], w_buf[slot, n], preferred_element_type=jnp.float32) + vec_ref[2 + n:3 + n, cols].astype(jnp.float32)
            if n == 2:
                o_ref[:, cols] = lin.astype(jnp.bfloat16)
            else:
                parts = []
                for c in range(tile // head_dim):
                    part = lin[:, c * head_dim:(c + 1) * head_dim]
                    parts.append(part * cos_ref[...] + pltpu.roll(part, head_dim // 2, 1) * sin_ref[...])
                o_ref[:, cols] = jnp.concatenate(parts, axis=1).astype(jnp.bfloat16)

        @pl.when(j + AHEAD < count)
        def _():
            for copy in copies(j + AHEAD, slot):
                copy.start()


def qkv_call(tokens, vectors, cos_tab, sin_signed, w_query, w_key, w_value):
    rows, d_model = tokens.shape
    cols = w_query.shape[1]
    tile = 256
    vmem = pl.BlockSpec(memory_space=pltpu.VMEM)
    hbm = pl.BlockSpec(memory_space=pl.ANY)
    shape = jax.ShapeDtypeStruct((rows, cols), jnp.bfloat16)
    return pl.pallas_call(
        qkv_kernel,
        in_specs=[vmem, vmem, vmem, vmem, hbm, hbm, hbm],
        out_specs=[vmem, vmem, vmem],
        out_shape=[shape, shape, shape],
        scratch_shapes=[pltpu.VMEM((rows, d_model), jnp.bfloat16), pltpu.VMEM((AHEAD, 3, d_model, tile), jnp.bfloat16), pltpu.SemaphoreType.DMA((AHEAD, 3))],
        compiler_params=pltpu.CompilerParams(vmem_limit_bytes=44 * 2 ** 20),
        cost_estimate=pl.CostEstimate(flops=6 * rows * d_model * cols, bytes_accessed=6 * d_model * cols, transcendentals=0),
        name='qkv',
    )(tokens, vectors, cos_tab, sin_signed, w_query, w_key, w_value)


GROUP = 8
SLOTS = 3
STEP = 8
CHUNK = 8


def attend_kernel(order_ref, pos_ref, q_ref, kn_ref, vn_ref, k_hbm, v_hbm, out_ref, k_buf, v_buf, sid_ref, sems):
    rows, heads, head_dim = q_ref.shape
    seq = k_hbm.shape[1]
    groups = rows // GROUP
    scale = head_dim ** -0.5
    key_id = lax.broadcasted_iota(jnp.int32, sid_ref.shape, 1)
    row_id = lax.broadcasted_iota(jnp.int32, sid_ref.shape, 0)
    sid_ref[...] = jnp.where(lax.rem(key_id, heads) == row_id, lax.div(key_id, heads), seq)

    @pl.loop(0, GROUP * SLOTS)
    def _(i):
        v_buf[i // GROUP, i % GROUP] = jnp.zeros(v_buf.shape[2:], v_buf.dtype)

    def group_at(n):
        return jnp.where(n & 1 == 0, n // 2, groups - 1 - n // 2)

    def chunks_at(n):
        return (pos_ref[order_ref[group_at(n) * GROUP]] + CHUNK - 1) // CHUNK

    def fetch(n):
        grp = group_at(n)
        slot = lax.rem(n, SLOTS)
        chunks = chunks_at(n)
        for k in range(1, seq // CHUNK + 1):
            @pl.when(chunks == k)
            def _(k=k):
                src = pl.ds(0, k * CHUNK)

                @pl.loop(0, GROUP)
                def _(i):
                    tok = order_ref[grp * GROUP + i]
                    pltpu.make_async_copy(k_hbm.at[tok, src], k_buf.at[slot, i, src], sems.at[0, slot]).start()
                    pltpu.make_async_copy(v_hbm.at[tok, src], v_buf.at[slot, i, src], sems.at[1, slot]).start()

    def settle(n):
        slot = lax.rem(n, SLOTS)
        chunks = chunks_at(n)
        size = seq // CHUNK
        while size >= 1:
            @pl.when((chunks & size) != 0)
            def _(size=size):
                src = pl.ds(0, size * CHUNK)
                pltpu.make_async_copy(k_hbm.at[pl.ds(0, GROUP), src], k_buf.at[slot, :, src], sems.at[0, slot]).wait()
                pltpu.make_async_copy(v_hbm.at[pl.ds(0, GROUP), src], v_buf.at[slot, :, src], sems.at[1, slot]).wait()

            size //= 2

    def compute(n, steps):
        grp = group_at(n)
        slot = lax.rem(n, SLOTS)
        keys = steps * STEP * heads
        toks = [order_ref[grp * GROUP + i] for i in range(GROUP)]
        q_val = [q_ref[t] for t in toks]
        scores = []
        for i in range(GROUP):
            k_val = k_buf[slot, i, pl.ds(0, steps * STEP)].reshape(keys, head_dim)
            raw = lax.dot_general(q_val[i], k_val, (((1,), (1,)), ((), ())), preferred_element_type=jnp.float32)
            scores.append(jnp.where(sid_ref[:, :keys] < pos_ref[toks[i]], raw * scale, -jnp.inf))
        for i in range(GROUP):
            t = toks[i]
            s_new = jnp.sum(q_val[i].astype(jnp.float32) * kn_ref[t].astype(jnp.float32), axis=-1, keepdims=True) * scale
            top = jnp.maximum(jnp.max(scores[i], axis=-1, keepdims=True), s_new)
            e_val = jnp.exp(scores[i] - top)
            e_new = jnp.exp(s_new - top)
            inv = 1.0 / (jnp.sum(e_val, axis=-1, keepdims=True) + e_new)
            p_val = (e_val * inv).astype(jnp.bfloat16)
            p_new = (e_new * inv).astype(jnp.bfloat16).astype(jnp.float32)
            v_val = v_buf[slot, i, pl.ds(0, steps * STEP)].reshape(keys, head_dim)
            res = jnp.dot(p_val, v_val, preferred_element_type=jnp.float32) + p_new * vn_ref[t].astype(jnp.float32)
            out_ref[t] = res.astype(jnp.bfloat16)

    for n in range(SLOTS - 1):
        fetch(n)

    @pl.loop(0, groups)
    def _(n):
        @pl.when(n + SLOTS - 1 < groups)
        def _():
            fetch(n + SLOTS - 1)

        settle(n)
        most = pos_ref[order_ref[group_at(n) * GROUP]]
        steps = jnp.maximum((most + STEP - 1) // STEP, 1)
        for k in range(1, seq // STEP + 1):
            @pl.when(steps == k)
            def _(k=k):
                compute(n, k)


def attend_call(order, positions, q_rot, key_new, value_new, k_cache, v_cache):
    rows, seq, heads, head_dim = k_cache.shape
    vmem = pl.BlockSpec(memory_space=pltpu.VMEM)
    smem = pl.BlockSpec(memory_space=pltpu.SMEM)
    hbm = pl.BlockSpec(memory_space=pl.ANY)
    return pl.pallas_call(
        attend_kernel,
        in_specs=[smem, smem, vmem, vmem, vmem, hbm, hbm],
        out_specs=vmem,
        out_shape=jax.ShapeDtypeStruct((rows, heads, head_dim), jnp.bfloat16),
        scratch_shapes=[
            pltpu.VMEM((SLOTS, GROUP, seq, heads, head_dim), jnp.bfloat16),
            pltpu.VMEM((SLOTS, GROUP, seq, heads, head_dim), jnp.bfloat16),
            pltpu.VMEM((heads, seq * heads), jnp.int32),
            pltpu.SemaphoreType.DMA((2, SLOTS)),
        ],
        compiler_params=pltpu.CompilerParams(vmem_limit_bytes=48 * 2 ** 20),
        cost_estimate=pl.CostEstimate(flops=4 * rows * seq * heads * heads * head_dim, bytes_accessed=2 * rows * seq * heads * head_dim, transcendentals=0),
        name='attend',
    )(order, positions, q_rot, key_new, value_new, k_cache, v_cache)


def router_gates(h_two, wr_val, pick_val):
    logits = lax.dot_general(h_two, wr_val, (((1,), (1,)), ((), ())), preferred_element_type=jnp.float32)
    ids = lax.broadcasted_iota(jnp.int32, logits.shape, 1).astype(jnp.float32)
    hit_one = ids == pick_val[:, 0:1]
    hit_two = ids == pick_val[:, 1:2]
    keep_one = pick_val[:, 2:2 + logits.shape[1]] == 1.0
    gates = []
    for keep, hit in ((keep_one, hit_one), (keep_one & jnp.logical_not(hit_one), hit_two)):
        masked = jnp.where(keep, logits, -jnp.inf)
        e_val = jnp.exp(masked - jnp.max(masked, axis=-1, keepdims=True))
        top = jnp.sum(jnp.where(hit, e_val, 0.0), axis=-1, keepdims=True)
        gates.append(top / jnp.sum(e_val, axis=-1, keepdims=True))
    lane = lax.broadcasted_iota(jnp.int32, pick_val.shape, 1)
    return jnp.where(lane == 0, gates[0], jnp.where(lane == 1, gates[1], 0.0))


def attention_order(positions):
    ids = jnp.arange(positions.shape[0], dtype=jnp.int32)
    ahead = (positions[None, :] > positions[:, None]) | ((positions[None, :] == positions[:, None]) & (ids[None, :] < ids[:, None]))
    rank = jnp.sum(ahead.astype(jnp.int32), axis=1)
    return jnp.sum(jnp.where(rank[:, None] == ids[None, :], ids[:, None], 0), axis=0)


def moe_kernel(a_ref, x_hbm, vec_ref, wr_ref, pick_ref, wo_hbm, wg_hbm, wu_hbm, wd_hbm, out_hbm, hb, wg, wu, wd, sum_ref, mid_ref, h_in, gate_ref, xblk, zt_ref, z_ref, acc, stg, d2d, p1a, p1b, p2a, p2b, wsem, xsem, gsend, grecv, dsend, drecv, rsend, rrecv, osem, credit):
    me = lax.axis_index('ep')
    core = lax.rem(me, 2)
    x_pos = lax.rem(lax.div(me, 2), 2)
    y_pos = lax.div(me, 4)
    partner = me + 1 - 2 * core
    xn = me + 2 - 4 * x_pos
    yn = me + 4 - 8 * y_pos
    rows = x_hbm.shape[0]
    mid = rows // 2
    d_model = x_hbm.shape[1]
    half = d_model // 2
    ff = wd.shape[1]
    tile = 512
    mesh_id = pl.DeviceIdType.MESH
    part_rows = (pl.ds(0, mid), pl.ds(mid, mid))

    def remote(src, dst, send, recv, dev):
        return pltpu.make_async_remote_copy(src_ref=src, dst_ref=dst, send_sem=send, recv_sem=recv, device_id=(dev,), device_id_type=mesh_id)

    gather = []

    def add_gather(src, dst, dev):
        n = len(gather)
        gather.append(remote(src, dst, gsend.at[n], grecv.at[n], dev))
        return gather[-1]

    own = add_gather(h_in, hb.at[1], partner)
    from_x = [add_gather(h_in.at[p], hb.at[2, p], xn) for p in part_rows]
    from_y = [add_gather(h_in.at[p], hb.at[4, p], yn) for p in part_rows]
    share_x = [add_gather(hb.at[2, p], hb.at[3, p], partner) for p in part_rows]
    share_y = [add_gather(hb.at[4, p], hb.at[5, p], partner) for p in part_rows]
    far = [add_gather(hb.at[2, part_rows[0]], hb.at[6, part_rows[0]], yn), add_gather(hb.at[4, part_rows[1]], hb.at[6, part_rows[1]], xn)]
    share_far = [add_gather(hb.at[6, p], hb.at[7, p], partner) for p in part_rows]

    scatter = []

    def add_scatter(src, dst, dev):
        n = len(scatter)
        scatter.append(remote(src, dst, rsend.at[n], rrecv.at[n], dev))
        return scatter[-1]

    x_first = [add_scatter(acc.at[1 + h, 0, :, part_rows[0]], p1a.at[0, h], xn) for h in range(2)]
    y_first = [add_scatter(acc.at[1 + h, 1, :, part_rows[1]], p1b.at[0, h], yn) for h in range(2)]
    x_far = [add_scatter(acc.at[3, 0, :, part_rows[h]], p1a.at[1, h], xn) for h in range(2)]
    y_far = [add_scatter(acc.at[3, 1, :, part_rows[h]], p1b.at[1, h], yn) for h in range(2)]
    y_last = [add_scatter(acc.at[1 + h, 0, :, part_rows[1]], p2a.at[h], yn) for h in range(2)]
    x_last = [add_scatter(acc.at[1 + h, 1, :, part_rows[0]], p2b.at[h], xn) for h in range(2)]

    def weight(e):
        return [pltpu.make_async_copy(hbm.at[e], buf.at[e], wsem.at[n, e]) for n, (hbm, buf) in enumerate(((wg_hbm, wg), (wu_hbm, wu), (wd_hbm, wd)))]

    barrier = pltpu.get_barrier_semaphore()
    for dev in (partner, xn, yn):
        pl.semaphore_signal(barrier, inc=1, device_id=(dev,), device_id_type=mesh_id)
    depth = ff // 128 * 128
    homes = [buf.at[e, pl.ds(0, depth)] for e in range(2) for buf in (wg, wu, wd)]
    refills = [copy for e in range(2) for copy in weight(e)]
    spans = [(n * depth, depth) for n in range(len(homes))]
    rest = d_model - len(homes) * depth
    homes.append(xblk.at[pl.ds(0, rest), pl.ds(0, d_model)])
    spans.append((d_model - rest, rest))
    loads = [pltpu.make_async_copy(wo_hbm.at[pl.ds(*span)], home, osem.at[n]) for n, (span, home) in enumerate(zip(spans, homes))]
    x_loads = [pltpu.make_async_copy(x_hbm.at[:, pl.ds(n * half, half)], stg.at[0, n], xsem.at[n]) for n in range(2)]
    for copy in x_loads + loads:
        copy.start()
    for copy in x_loads:
        copy.wait()
    zt_ref[...] = jnp.zeros_like(zt_ref)
    for n, (span, home) in enumerate(zip(spans, homes)):
        loads[n].wait()

        @pl.loop(0, d_model // tile)
        def _(i, n=n, span=span, home=home):
            cols = pl.ds(pl.multiple_of(i * tile, tile), tile)
            part = jnp.dot(a_ref[:, span[0]:span[0] + span[1]], home[:, cols], preferred_element_type=jnp.float32)
            if n == 0:
                sum_ref[:, cols] = part
            elif n < len(homes) - 1:
                sum_ref[:, cols] += part
            else:
                slim = pl.ds(pl.multiple_of(lax.rem(i, half // tile) * tile, tile), tile)
                val = stg[0, lax.div(i, half // tile), :, slim].astype(jnp.float32) + (sum_ref[:, cols] + part) + vec_ref[5:6, cols].astype(jnp.float32)
                mid_ref[:, cols] = val.astype(jnp.bfloat16)

        if n < len(refills):
            refills[n].start()
    h_two = norm_rows(mid_ref[...].astype(jnp.float32), vec_ref[6:7], vec_ref[7:8]).astype(jnp.bfloat16)
    pick_val = jnp.transpose(pick_ref[...].astype(jnp.float32))
    lanes = lax.broadcasted_iota(jnp.int32, pick_val.shape, 1)
    h_in[:, :d_model] = h_two
    h_in[:, d_model:] = jnp.where(lanes < 2, pick_val, 0.0).astype(jnp.bfloat16)
    gate_ref[...] = router_gates(h_two, wr_ref[...], pick_val)
    pl.semaphore_wait(barrier, 3)
    for h in range(2):
        from_x[h].start()
        from_y[h].start()
    own.start()

    def load(sources):
        step = 2 * rows // len(sources)
        copies = [pltpu.make_async_copy(src, xblk.at[pl.ds(n * step, step)], xsem.at[n]) for n, src in enumerate(sources)]
        for copy in copies:
            copy.start()
        for copy in copies:
            copy.wait()

    def merge(dst, src):
        count = dst.shape[1] // 16

        @pl.loop(0, 2 * count)
        def _(i):
            slot = lax.div(i, count)
            at = pl.ds(pl.multiple_of(lax.rem(i, count) * 16, 16), 16)
            dst[slot, at] = dst[slot, at] + src[slot, at]

    def shared(r, part):
        return remote(stg.at[part], d2d.at[lax.rem(r, 2), part], dsend.at[part], drecv.at[r, part], partner)

    def gather_step(h):
        from_x[h].wait_recv()
        share_x[h].start()
        if h == 0:
            far[0].start()
        from_y[h].wait_recv()
        share_y[h].start()
        if h == 1:
            far[1].start()

    def merge_high(r, finish):
        shared(r, 1).wait_recv()
        merge(acc.at[r, 1], d2d.at[lax.rem(r, 2), 1])
        if not finish:
            for h in range(2):
                @pl.when(r == 1 + h)
                def _(h=h):
                    y_first[h].start()

            @pl.when(r < 2)
            def _():
                pl.semaphore_signal(credit, inc=1, device_id=(partner,), device_id_type=mesh_id)

    @pl.loop(0, 4)
    def _(r):
        @pl.when(r == 0)
        def _():
            own.wait_recv()
            copy = pltpu.make_async_copy(hb.at[1], xblk.at[pl.ds(rows, rows)], xsem.at[0])
            copy.start()
            xblk[:rows] = h_in[...]
            copy.wait()

        for h in range(2):
            @pl.when(r == 1 + h)
            def _(h=h):
                share_x[h].wait_recv()
                share_y[h].wait_recv()
                load([hb.at[n, part_rows[h]] for n in (2, 4, 3, 5)])

        @pl.when(r == 3)
        def _():
            share_far[0].wait_recv()
            share_far[1].wait_recv()
            load([hb.at[6], hb.at[7]])

        @pl.loop(0, 2)
        def _(e):
            @pl.when(r == 0)
            def _():
                for copy in weight(e)[:2]:
                    copy.wait()

            x_val = xblk[:, :d_model]
            dims = (((1,), (1,)), ((), ()))
            u_val = lax.dot_general(wg[e], x_val, dims, preferred_element_type=jnp.float32)
            v_val = lax.dot_general(wu[e], x_val, dims, preferred_element_type=jnp.float32)
            zt_ref[:ff] = (jax.nn.silu(u_val) * v_val).astype(jnp.bfloat16)
            z_ref[e] = jnp.transpose(zt_ref[...])

            @pl.when((r > 0) & (e == 0))
            def _():
                merge_high(r - 1, False)

            @pl.when((r == 1) & (e == 0))
            def _():
                gather_step(1)

        @pl.when(r == 0)
        def _():
            gather_step(0)
            for e in range(2):
                weight(e)[2].wait()

        @pl.when(r == 2)
        def _():
            for h in range(2):
                far[h].wait_recv()
                share_far[h].start()

        @pl.loop(0, 2)
        def _(part):
            @pl.when(r > 0)
            def _():
                shared(r - 1, part).wait_send()

            @pl.loop(0, half // tile)
            def _(n):
                wide = pl.ds(pl.multiple_of(part * half + n * tile, tile), tile)
                slim = pl.ds(pl.multiple_of(n * tile, tile), tile)
                first = jnp.dot(z_ref[0, :, :ff], wd[0, :, wide], preferred_element_type=jnp.float32)
                second = jnp.dot(z_ref[1, :, :ff], wd[1, :, wide], preferred_element_type=jnp.float32)
                for slot in range(2):
                    choice = xblk[:, d_model:][:, slot:slot + 1].astype(jnp.float32)
                    lead = (2 * me).astype(jnp.float32)
                    val = jnp.where(choice == lead, first, jnp.where(choice == lead + 1.0, second, 0.0)).astype(jnp.bfloat16)
                    acc[r, part, slot, :, slim] = val[:rows]
                    stg[part, slot, :, slim] = val[rows:]

            @pl.when((r >= 2) & (part == 0))
            def _():
                pl.semaphore_wait(credit, 1)

            shared(r, part).start()

        shared(r, 0).wait_recv()
        merge(acc.at[r, 0], d2d.at[lax.rem(r, 2), 0])
        for h in range(2):
            @pl.when(r == 1 + h)
            def _(h=h):
                x_first[h].start()

        @pl.when(r == 3)
        def _():
            x_far[0].start()
            x_far[1].start()

    out_ref = xblk.at[pl.ds(rows, rows), pl.ds(0, d_model)]
    merge_high(3, True)
    y_far[0].start()
    y_far[1].start()
    for h in range(2):
        x_far[h].wait_recv()
        merge(acc.at[1 + h, 0, :, part_rows[1]], p1a.at[1, h])
        y_last[h].start()
        y_far[h].wait_recv()
        merge(acc.at[1 + h, 1, :, part_rows[0]], p1b.at[1, h])
        x_last[h].start()
    for h in range(2):
        x_first[h].wait_recv()
        merge(acc.at[0, 0, :, part_rows[h]], p1a.at[0, h])
        y_first[h].wait_recv()
        merge(acc.at[0, 1, :, part_rows[h]], p1b.at[0, h])
    for h in range(2):
        for part, last, buf in ((0, y_last, p2a), (1, x_last, p2b)):
            last[h].wait_recv()

            @pl.loop(0, mid // 16)
            def _(i, h=h, part=part, buf=buf):
                near = pl.ds(pl.multiple_of(i * 16, 16), 16)
                at = pl.ds(pl.multiple_of(h * mid + i * 16, 16), 16)
                wide = pl.ds(part * half, half)
                gates = gate_ref[at]
                y_val = [(acc[0, part, slot, at] + buf[h, slot, near]).astype(jnp.float32) * gates[:, slot:slot + 1] for slot in range(2)]
                out_ref[at, wide] = (mid_ref[at, wide].astype(jnp.float32) + (y_val[0] + y_val[1])).astype(jnp.bfloat16)

    out_copy = pltpu.make_async_copy(out_ref, out_hbm, xsem.at[2])
    out_copy.start()
    for copy in gather + scatter:
        copy.wait_send()
    for part in range(2):
        shared(3, part).wait_send()
    out_copy.wait()


def moe_call(attn_flat, tokens, vectors, w_router, picks, w_out, w_gate, w_up, w_down):
    rows, d_model = tokens.shape
    half = d_model // 2
    ff = w_gate.shape[2]
    ff_pad = pl.cdiv(ff, 128) * 128
    width = d_model + 128
    vmem = pl.BlockSpec(memory_space=pltpu.VMEM)
    hbm = pl.BlockSpec(memory_space=pl.ANY)
    bf = jnp.bfloat16
    dma = pltpu.SemaphoreType.DMA
    out, _ = pl.pallas_call(
        moe_kernel,
        in_specs=[vmem, hbm, vmem, vmem, vmem] + [hbm] * 4,
        out_specs=[hbm, hbm],
        out_shape=[jax.ShapeDtypeStruct((rows, d_model), bf), jax.ShapeDtypeStruct((8, rows, width), bf)],
        scratch_shapes=[
            pltpu.VMEM((2, ff, d_model), bf),
            pltpu.VMEM((2, ff, d_model), bf),
            pltpu.VMEM((2, ff, d_model), bf),
            pltpu.VMEM((rows, d_model), jnp.float32),
            pltpu.VMEM((rows, d_model), bf),
            pltpu.VMEM((rows, width), bf),
            pltpu.VMEM((rows, 128), jnp.float32),
            pltpu.VMEM((2 * rows, width), bf),
            pltpu.VMEM((ff_pad, 2 * rows), bf),
            pltpu.VMEM((2, 2 * rows, ff_pad), bf),
            pltpu.VMEM((4, 2, 2, rows, half), bf),
            pltpu.VMEM((2, 2, rows, half), bf),
            pltpu.VMEM((2, 2, 2, rows, half), bf),
            pltpu.VMEM((2, 2, 2, rows // 2, half), bf),
            pltpu.VMEM((2, 2, 2, rows // 2, half), bf),
            pltpu.VMEM((2, 2, rows // 2, half), bf),
            pltpu.VMEM((2, 2, rows // 2, half), bf),
            dma((3, 2)),
            dma((4,)),
            dma((13,)),
            dma((13,)),
            dma((2,)),
            dma((4, 2)),
            dma((12,)),
            dma((12,)),
            dma((7,)),
            pltpu.SemaphoreType.REGULAR,
        ],
        compiler_params=pltpu.CompilerParams(vmem_limit_bytes=67043328, collective_id=0, has_side_effects=True),
        name='moe',
    )(attn_flat, tokens, vectors, w_router, picks, w_out, jnp.swapaxes(w_gate, 1, 2), jnp.swapaxes(w_up, 1, 2), w_down)
    return out


def solution(mesh):
    def local_step(tokens, k_cache, v_cache, positions, expert_one, expert_two, eligible, ln1_gain, ln1_bias, w_query, b_query, w_key, b_key, w_value, b_value, w_out, b_out, ln2_gain, ln2_bias, w_router, w_gate, w_up, w_down):
        tok_count, seq_len, heads, head_dim = k_cache.shape
        d_model = tokens.shape[1]
        cos_tab, sin_tab = rope_tables(positions, head_dim)
        sign = jnp.where(jnp.arange(head_dim) < head_dim // 2, -1.0, 1.0)
        vectors = row_stack([ln1_gain, ln1_bias, b_query, b_key, b_value, b_out, ln2_gain, ln2_bias])
        which = lax.broadcasted_iota(jnp.int32, (128, tok_count), 0)
        picks = jnp.where(which == 0, expert_one[None, :], jnp.where(which == 1, expert_two[None, :], jnp.pad(eligible.T, ((2, 110), (0, 0)))))
        q_flat, k_flat, v_flat = qkv_call(tokens, vectors, cos_tab, sin_tab * sign[None, :], w_query, w_key, w_value)
        split = lambda t: t.reshape(tok_count, heads, head_dim)
        key_new, value_new = split(k_flat), split(v_flat)
        attn = attend_call(attention_order(positions), positions, split(q_flat), key_new, value_new, k_cache, v_cache)
        tokens_out = moe_call(attn.reshape(tok_count, heads * head_dim), tokens, vectors, w_router.T, picks, w_out, w_gate, w_up, w_down)
        return tokens_out, key_new, value_new

    row_spec = P('ep', None)
    cache_spec = P('ep', None, None, None)
    vec_spec = P('ep')
    rep_one = P(None)
    rep_two = P(None, None)
    expert_spec = P('ep', None, None)
    in_specs = (row_spec, cache_spec, cache_spec, vec_spec, vec_spec, vec_spec, row_spec, rep_one, rep_one, rep_two, rep_one, rep_two, rep_one, rep_two, rep_one, rep_two, rep_one, rep_one, rep_one, rep_two, expert_spec, expert_spec, expert_spec)
    out_specs = (row_spec, expert_spec, expert_spec)
    return jax.shard_map(local_step, mesh=mesh, in_specs=in_specs, out_specs=out_specs, check_vma=False)
```

```python
import jax
import jax.numpy as jnp
from jax import lax
from jax.experimental import pallas as pl
from jax.experimental.pallas import tpu as pltpu
from jax.sharding import PartitionSpec as P

ROPE_BASE = 10000.0
LN_EPS = 1e-5


def rope_tables(positions, head_dim):
    half_dim = head_dim // 2
    inv_freq = ROPE_BASE ** (jnp.arange(half_dim, dtype=jnp.float32) * (-2.0 / head_dim))
    angles = positions.astype(jnp.float32)[:, None] * inv_freq[None, :]
    angles = jnp.concatenate([angles, angles], axis=-1)
    return jnp.cos(angles), jnp.sin(angles)


def norm_rows(x_val, gain, bias):
    mean_val = jnp.mean(x_val, axis=-1, keepdims=True)
    centered = x_val - mean_val
    var_val = jnp.mean(centered * centered, axis=-1, keepdims=True)
    return centered * lax.rsqrt(var_val + LN_EPS) * gain.astype(jnp.float32) + bias.astype(jnp.float32)


def row_stack(vectors):
    which = lax.broadcasted_iota(jnp.int32, (len(vectors), vectors[0].shape[0]), 0)
    out = jnp.zeros((len(vectors), vectors[0].shape[0]), vectors[0].dtype)
    for n, vec in enumerate(vectors):
        out = jnp.where(which == n, vec[None, :], out)
    return out


AHEAD = 4


def qkv_kernel(x_ref, vec_ref, cos_ref, sin_ref, wq_hbm, wk_hbm, wv_hbm, q_ref, k_ref, v_ref, h_ref, w_buf, sems):
    rows, d_model = x_ref.shape
    tile = w_buf.shape[3]
    count = q_ref.shape[1] // tile
    head_dim = cos_ref.shape[1]

    def copies(j, slot):
        cols = pl.ds(pl.multiple_of(j * tile, tile), tile)
        return [pltpu.make_async_copy(hbm.at[:, cols], w_buf.at[slot, n], sems.at[slot, n]) for n, hbm in enumerate((wq_hbm, wk_hbm, wv_hbm))]

    for j in range(AHEAD):
        for copy in copies(j, j):
            copy.start()
    h_ref[...] = norm_rows(x_ref[...].astype(jnp.float32), vec_ref[0:1], vec_ref[1:2]).astype(jnp.bfloat16)

    @pl.loop(0, count)
    def _(j):
        slot = lax.rem(j, AHEAD)
        cols = pl.ds(pl.multiple_of(j * tile, tile), tile)
        for copy in copies(j, slot):
            copy.wait()
        for n, o_ref in enumerate((q_ref, k_ref, v_ref)):
            lin = jnp.dot(h_ref[...], w_buf[slot, n], preferred_element_type=jnp.float32) + vec_ref[2 + n:3 + n, cols].astype(jnp.float32)
            if n == 2:
                o_ref[:, cols] = lin.astype(jnp.bfloat16)
            else:
                parts = []
                for c in range(tile // head_dim):
                    part = lin[:, c * head_dim:(c + 1) * head_dim]
                    parts.append(part * cos_ref[...] + pltpu.roll(part, head_dim // 2, 1) * sin_ref[...])
                o_ref[:, cols] = jnp.concatenate(parts, axis=1).astype(jnp.bfloat16)

        @pl.when(j + AHEAD < count)
        def _():
            for copy in copies(j + AHEAD, slot):
                copy.start()


def qkv_call(tokens, vectors, cos_tab, sin_signed, w_query, w_key, w_value):
    rows, d_model = tokens.shape
    cols = w_query.shape[1]
    tile = 256
    vmem = pl.BlockSpec(memory_space=pltpu.VMEM)
    hbm = pl.BlockSpec(memory_space=pl.ANY)
    shape = jax.ShapeDtypeStruct((rows, cols), jnp.bfloat16)
    return pl.pallas_call(
        qkv_kernel,
        in_specs=[vmem, vmem, vmem, vmem, hbm, hbm, hbm],
        out_specs=[vmem, vmem, vmem],
        out_shape=[shape, shape, shape],
        scratch_shapes=[pltpu.VMEM((rows, d_model), jnp.bfloat16), pltpu.VMEM((AHEAD, 3, d_model, tile), jnp.bfloat16), pltpu.SemaphoreType.DMA((AHEAD, 3))],
        compiler_params=pltpu.CompilerParams(vmem_limit_bytes=44 * 2 ** 20),
        cost_estimate=pl.CostEstimate(flops=6 * rows * d_model * cols, bytes_accessed=6 * d_model * cols, transcendentals=0),
        name='qkv',
    )(tokens, vectors, cos_tab, sin_signed, w_query, w_key, w_value)


GROUP = 8
SLOTS = 3
STEP = 8
CHUNK = 8


def attend_kernel(order_ref, pos_ref, q_ref, kn_ref, vn_ref, k_hbm, v_hbm, out_ref, k_buf, v_buf, sid_ref, sems):
    rows, heads, head_dim = q_ref.shape
    seq = k_hbm.shape[1]
    groups = rows // GROUP
    scale = head_dim ** -0.5
    key_id = lax.broadcasted_iota(jnp.int32, sid_ref.shape, 1)
    row_id = lax.broadcasted_iota(jnp.int32, sid_ref.shape, 0)
    sid_ref[...] = jnp.where(lax.rem(key_id, heads) == row_id, lax.div(key_id, heads), seq)

    @pl.loop(0, GROUP * SLOTS)
    def _(i):
        v_buf[i // GROUP, i % GROUP] = jnp.zeros(v_buf.shape[2:], v_buf.dtype)

    def group_at(n):
        return jnp.where(n & 1 == 0, n // 2, groups - 1 - n // 2)

    def chunks_at(n):
        return (pos_ref[order_ref[group_at(n) * GROUP]] + CHUNK - 1) // CHUNK

    def fetch(n):
        grp = group_at(n)
        slot = lax.rem(n, SLOTS)
        chunks = chunks_at(n)
        for k in range(1, seq // CHUNK + 1):
            @pl.when(chunks == k)
            def _(k=k):
                src = pl.ds(0, k * CHUNK)

                @pl.loop(0, GROUP)
                def _(i):
                    tok = order_ref[grp * GROUP + i]
                    pltpu.make_async_copy(k_hbm.at[tok, src], k_buf.at[slot, i, src], sems.at[0, slot]).start()
                    pltpu.make_async_copy(v_hbm.at[tok, src], v_buf.at[slot, i, src], sems.at[1, slot]).start()

    def settle(n):
        slot = lax.rem(n, SLOTS)
        chunks = chunks_at(n)
        size = seq // CHUNK
        while size >= 1:
            @pl.when((chunks & size) != 0)
            def _(size=size):
                src = pl.ds(0, size * CHUNK)
                pltpu.make_async_copy(k_hbm.at[pl.ds(0, GROUP), src], k_buf.at[slot, :, src], sems.at[0, slot]).wait()
                pltpu.make_async_copy(v_hbm.at[pl.ds(0, GROUP), src], v_buf.at[slot, :, src], sems.at[1, slot]).wait()

            size //= 2

    def compute(n, steps):
        grp = group_at(n)
        slot = lax.rem(n, SLOTS)
        keys = steps * STEP * heads
        toks = [order_ref[grp * GROUP + i] for i in range(GROUP)]
        q_val = [q_ref[t] for t in toks]
        scores = []
        for i in range(GROUP):
            k_val = k_buf[slot, i, pl.ds(0, steps * STEP)].reshape(keys, head_dim)
            raw = lax.dot_general(q_val[i], k_val, (((1,), (1,)), ((), ())), preferred_element_type=jnp.float32)
            scores.append(jnp.where(sid_ref[:, :keys] < pos_ref[toks[i]], raw * scale, -jnp.inf))
        for i in range(GROUP):
            t = toks[i]
            s_new = jnp.sum(q_val[i].astype(jnp.float32) * kn_ref[t].astype(jnp.float32), axis=-1, keepdims=True) * scale
            top = jnp.maximum(jnp.max(scores[i], axis=-1, keepdims=True), s_new)
            e_val = jnp.exp(scores[i] - top)
            e_new = jnp.exp(s_new - top)
            inv = 1.0 / (jnp.sum(e_val, axis=-1, keepdims=True) + e_new)
            p_val = (e_val * inv).astype(jnp.bfloat16)
            p_new = (e_new * inv).astype(jnp.bfloat16).astype(jnp.float32)
            v_val = v_buf[slot, i, pl.ds(0, steps * STEP)].reshape(keys, head_dim)
            res = jnp.dot(p_val, v_val, preferred_element_type=jnp.float32) + p_new * vn_ref[t].astype(jnp.float32)
            out_ref[t] = res.astype(jnp.bfloat16)

    for n in range(SLOTS - 1):
        fetch(n)

    @pl.loop(0, groups)
    def _(n):
        @pl.when(n + SLOTS - 1 < groups)
        def _():
            fetch(n + SLOTS - 1)

        settle(n)
        most = pos_ref[order_ref[group_at(n) * GROUP]]
        steps = jnp.maximum((most + STEP - 1) // STEP, 1)
        for k in range(1, seq // STEP + 1):
            @pl.when(steps == k)
            def _(k=k):
                compute(n, k)


def attend_call(order, positions, q_rot, key_new, value_new, k_cache, v_cache):
    rows, seq, heads, head_dim = k_cache.shape
    vmem = pl.BlockSpec(memory_space=pltpu.VMEM)
    smem = pl.BlockSpec(memory_space=pltpu.SMEM)
    hbm = pl.BlockSpec(memory_space=pl.ANY)
    return pl.pallas_call(
        attend_kernel,
        in_specs=[smem, smem, vmem, vmem, vmem, hbm, hbm],
        out_specs=vmem,
        out_shape=jax.ShapeDtypeStruct((rows, heads, head_dim), jnp.bfloat16),
        scratch_shapes=[
            pltpu.VMEM((SLOTS, GROUP, seq, heads, head_dim), jnp.bfloat16),
            pltpu.VMEM((SLOTS, GROUP, seq, heads, head_dim), jnp.bfloat16),
            pltpu.VMEM((heads, seq * heads), jnp.int32),
            pltpu.SemaphoreType.DMA((2, SLOTS)),
        ],
        compiler_params=pltpu.CompilerParams(vmem_limit_bytes=48 * 2 ** 20),
        cost_estimate=pl.CostEstimate(flops=4 * rows * seq * heads * heads * head_dim, bytes_accessed=2 * rows * seq * heads * head_dim, transcendentals=0),
        name='attend',
    )(order, positions, q_rot, key_new, value_new, k_cache, v_cache)


def out_kernel(a_ref, x_ref, vec_ref, wr_ref, pick_ref, w_hbm, mid_ref, h_ref, gate_ref, w_buf, sems):
    count, _, tile = w_buf.shape

    def weight(j):
        cols = pl.ds(pl.multiple_of(j * tile, tile), tile)
        return pltpu.make_async_copy(w_hbm.at[:, cols], w_buf.at[j], sems.at[j])

    for j in range(count):
        weight(j).start()

    @pl.loop(0, count)
    def _(j):
        weight(j).wait()
        cols = pl.ds(pl.multiple_of(j * tile, tile), tile)
        mid = x_ref[:, cols].astype(jnp.float32) + jnp.dot(a_ref[...], w_buf[j], preferred_element_type=jnp.float32) + vec_ref[5:6, cols].astype(jnp.float32)
        mid_ref[:, cols] = mid.astype(jnp.bfloat16)

    h_two = norm_rows(mid_ref[...].astype(jnp.float32), vec_ref[6:7], vec_ref[7:8]).astype(jnp.bfloat16)
    lanes = lax.broadcasted_iota(jnp.int32, (h_two.shape[0], 128), 1)
    pick_val = jnp.transpose(pick_ref[...].astype(jnp.float32))
    picks = jnp.where(lanes < 2, pick_val, 0.0)
    h_ref[:, :h_two.shape[1]] = h_two
    h_ref[:, h_two.shape[1]:] = picks.astype(jnp.bfloat16)
    logits = lax.dot_general(h_two, wr_ref[...], (((1,), (1,)), ((), ())), preferred_element_type=jnp.float32)
    ids = lax.broadcasted_iota(jnp.int32, logits.shape, 1).astype(jnp.float32)
    hit_one = ids == pick_val[:, 0:1]
    hit_two = ids == pick_val[:, 1:2]
    keep_one = pick_val[:, 2:2 + logits.shape[1]] == 1.0
    gates = []
    for keep, hit in ((keep_one, hit_one), (keep_one & jnp.logical_not(hit_one), hit_two)):
        masked = jnp.where(keep, logits, -jnp.inf)
        e_val = jnp.exp(masked - jnp.max(masked, axis=-1, keepdims=True))
        top = jnp.sum(jnp.where(hit, e_val, 0.0), axis=-1, keepdims=True)
        gates.append(top / jnp.sum(e_val, axis=-1, keepdims=True))
    lane = lax.broadcasted_iota(jnp.int32, gate_ref.shape, 1)
    gate_ref[...] = jnp.where(lane == 0, gates[0], jnp.where(lane == 1, gates[1], 0.0))


def out_call(attn_flat, tokens, vectors, w_router, picks, w_out):
    rows, d_model = tokens.shape
    tile = 256
    vmem = pl.BlockSpec(memory_space=pltpu.VMEM)
    shape = lambda cols, kind: jax.ShapeDtypeStruct((rows, cols), kind)
    return pl.pallas_call(
        out_kernel,
        in_specs=[vmem] * 5 + [pl.BlockSpec(memory_space=pl.ANY)],
        out_specs=[vmem] * 3,
        out_shape=[shape(d_model, jnp.bfloat16), shape(d_model + 128, jnp.bfloat16), shape(128, jnp.float32)],
        scratch_shapes=[pltpu.VMEM((d_model // tile, w_out.shape[0], tile), jnp.bfloat16), pltpu.SemaphoreType.DMA((d_model // tile,))],
        compiler_params=pltpu.CompilerParams(vmem_limit_bytes=48 * 2 ** 20),
        cost_estimate=pl.CostEstimate(flops=2 * rows * d_model * d_model, bytes_accessed=2 * d_model * d_model, transcendentals=0),
        name='project',
    )(attn_flat, tokens, vectors, w_router, picks, w_out)


def attention_order(positions):
    ids = jnp.arange(positions.shape[0], dtype=jnp.int32)
    ahead = (positions[None, :] > positions[:, None]) | ((positions[None, :] == positions[:, None]) & (ids[None, :] < ids[:, None]))
    rank = jnp.sum(ahead.astype(jnp.int32), axis=1)
    return jnp.sum(jnp.where(rank[:, None] == ids[None, :], ids[:, None], 0), axis=0)


def moe_kernel(h_in, x_hbm, gate_hbm, wg_hbm, wu_hbm, wd_hbm, out_hbm, hb, wg, wu, wd, gate_ref, xblk, zt_ref, z_ref, acc, stg, d2d, p1a, p1b, p2a, p2b, wsem, xsem, gsend, grecv, dsend, drecv, rsend, rrecv, credit):
    me = lax.axis_index('ep')
    core = lax.rem(me, 2)
    x_pos = lax.rem(lax.div(me, 2), 2)
    y_pos = lax.div(me, 4)
    partner = me + 1 - 2 * core
    xn = me + 2 - 4 * x_pos
    yn = me + 4 - 8 * y_pos
    rows = h_in.shape[0]
    mid = rows // 2
    d_model = x_hbm.shape[1]
    half = d_model // 2
    ff = wd.shape[1]
    tile = 512
    mesh_id = pl.DeviceIdType.MESH
    part_rows = (pl.ds(0, mid), pl.ds(mid, mid))

    def remote(src, dst, send, recv, dev):
        return pltpu.make_async_remote_copy(src_ref=src, dst_ref=dst, send_sem=send, recv_sem=recv, device_id=(dev,), device_id_type=mesh_id)

    gather = []

    def add_gather(src, dst, dev):
        n = len(gather)
        gather.append(remote(src, dst, gsend.at[n], grecv.at[n], dev))
        return gather[-1]

    own = add_gather(h_in, hb.at[1], partner)
    from_x = [add_gather(h_in.at[p], hb.at[2, p], xn) for p in part_rows]
    from_y = [add_gather(h_in.at[p], hb.at[4, p], yn) for p in part_rows]
    share_x = [add_gather(hb.at[2, p], hb.at[3, p], partner) for p in part_rows]
    share_y = [add_gather(hb.at[4, p], hb.at[5, p], partner) for p in part_rows]
    far = [add_gather(hb.at[2, part_rows[0]], hb.at[6, part_rows[0]], yn), add_gather(hb.at[4, part_rows[1]], hb.at[6, part_rows[1]], xn)]
    share_far = [add_gather(hb.at[6, p], hb.at[7, p], partner) for p in part_rows]

    scatter = []

    def add_scatter(src, dst, dev):
        n = len(scatter)
        scatter.append(remote(src, dst, rsend.at[n], rrecv.at[n], dev))
        return scatter[-1]

    x_first = [add_scatter(acc.at[1 + h, 0, :, part_rows[0]], p1a.at[0, h], xn) for h in range(2)]
    y_first = [add_scatter(acc.at[1 + h, 1, :, part_rows[1]], p1b.at[0, h], yn) for h in range(2)]
    x_far = [add_scatter(acc.at[3, 0, :, part_rows[h]], p1a.at[1, h], xn) for h in range(2)]
    y_far = [add_scatter(acc.at[3, 1, :, part_rows[h]], p1b.at[1, h], yn) for h in range(2)]
    y_last = [add_scatter(acc.at[1 + h, 0, :, part_rows[1]], p2a.at[h], yn) for h in range(2)]
    x_last = [add_scatter(acc.at[1 + h, 1, :, part_rows[0]], p2b.at[h], xn) for h in range(2)]

    def weight(e):
        return [pltpu.make_async_copy(hbm.at[e], buf.at[e], wsem.at[n, e]) for n, (hbm, buf) in enumerate(((wg_hbm, wg), (wu_hbm, wu), (wd_hbm, wd)))]

    barrier = pltpu.get_barrier_semaphore()
    for dev in (partner, xn, yn):
        pl.semaphore_signal(barrier, inc=1, device_id=(dev,), device_id_type=mesh_id)
    for copy in weight(0)[:2]:
        copy.start()
    zt_ref[...] = jnp.zeros_like(zt_ref)
    pl.semaphore_wait(barrier, 3)
    for h in range(2):
        from_x[h].start()
        from_y[h].start()
    own.start()

    def load(sources):
        step = 2 * rows // len(sources)
        copies = [pltpu.make_async_copy(src, xblk.at[pl.ds(n * step, step)], xsem.at[n]) for n, src in enumerate(sources)]
        for copy in copies:
            copy.start()
        for copy in copies:
            copy.wait()

    def merge(dst, src):
        count = dst.shape[1] // 16

        @pl.loop(0, 2 * count)
        def _(i):
            slot = lax.div(i, count)
            at = pl.ds(pl.multiple_of(lax.rem(i, count) * 16, 16), 16)
            dst[slot, at] = dst[slot, at] + src[slot, at]

    def shared(r, part):
        return remote(stg.at[part], d2d.at[lax.rem(r, 2), part], dsend.at[part], drecv.at[r, part], partner)

    def gather_step(h):
        from_x[h].wait_recv()
        share_x[h].start()
        if h == 0:
            far[0].start()
        from_y[h].wait_recv()
        share_y[h].start()
        if h == 1:
            far[1].start()

    def merge_high(r, finish):
        shared(r, 1).wait_recv()
        merge(acc.at[r, 1], d2d.at[lax.rem(r, 2), 1])
        if not finish:
            for h in range(2):
                @pl.when(r == 1 + h)
                def _(h=h):
                    y_first[h].start()

            @pl.when(r < 2)
            def _():
                pl.semaphore_signal(credit, inc=1, device_id=(partner,), device_id_type=mesh_id)

    @pl.loop(0, 4)
    def _(r):
        @pl.when(r == 0)
        def _():
            own.wait_recv()
            load([h_in, hb.at[1]])

        for h in range(2):
            @pl.when(r == 1 + h)
            def _(h=h):
                share_x[h].wait_recv()
                share_y[h].wait_recv()
                load([hb.at[n, part_rows[h]] for n in (2, 4, 3, 5)])

        @pl.when(r == 3)
        def _():
            share_far[0].wait_recv()
            share_far[1].wait_recv()
            load([hb.at[6], hb.at[7]])

        @pl.loop(0, 2)
        def _(e):
            @pl.when(r == 0)
            def _():
                for copy in weight(e)[:2]:
                    copy.wait()

                @pl.when(e == 0)
                def _():
                    for copy in weight(1)[:2] + [weight(0)[2], weight(1)[2]]:
                        copy.start()

            x_val = xblk[:, :d_model]
            dims = (((1,), (1,)), ((), ()))
            u_val = lax.dot_general(wg[e], x_val, dims, preferred_element_type=jnp.float32)
            v_val = lax.dot_general(wu[e], x_val, dims, preferred_element_type=jnp.float32)
            zt_ref[:ff] = (jax.nn.silu(u_val) * v_val).astype(jnp.bfloat16)
            z_ref[e] = jnp.transpose(zt_ref[...])

            @pl.when((r > 0) & (e == 0))
            def _():
                merge_high(r - 1, False)

        @pl.when(r == 1)
        def _():
            gather_step(1)

        @pl.when(r == 0)
        def _():
            for e in range(2):
                weight(e)[2].wait()

        @pl.when(r == 2)
        def _():
            for h in range(2):
                far[h].wait_recv()
                share_far[h].start()

        @pl.loop(0, 2)
        def _(part):
            @pl.when(r > 0)
            def _():
                shared(r - 1, part).wait_send()

            @pl.loop(0, half // tile)
            def _(n):
                wide = pl.ds(pl.multiple_of(part * half + n * tile, tile), tile)
                slim = pl.ds(pl.multiple_of(n * tile, tile), tile)
                first = jnp.dot(z_ref[0, :, :ff], wd[0, :, wide], preferred_element_type=jnp.float32)
                second = jnp.dot(z_ref[1, :, :ff], wd[1, :, wide], preferred_element_type=jnp.float32)
                for slot in range(2):
                    choice = xblk[:, d_model:][:, slot:slot + 1].astype(jnp.float32)
                    lead = (2 * me).astype(jnp.float32)
                    val = jnp.where(choice == lead, first, jnp.where(choice == lead + 1.0, second, 0.0)).astype(jnp.bfloat16)
                    acc[r, part, slot, :, slim] = val[:rows]
                    stg[part, slot, :, slim] = val[rows:]

            @pl.when((r >= 2) & (part == 0))
            def _():
                pl.semaphore_wait(credit, 1)

            shared(r, part).start()

        @pl.when(r == 0)
        def _():
            gather_step(0)

        shared(r, 0).wait_recv()
        merge(acc.at[r, 0], d2d.at[lax.rem(r, 2), 0])
        for h in range(2):
            @pl.when(r == 1 + h)
            def _(h=h):
                x_first[h].start()

        @pl.when(r == 3)
        def _():
            x_far[0].start()
            x_far[1].start()

    x_ref = xblk.at[pl.ds(0, rows), pl.ds(0, d_model)]
    out_ref = xblk.at[pl.ds(rows, rows), pl.ds(0, d_model)]
    late = [pltpu.make_async_copy(x_hbm, x_ref, xsem.at[0]), pltpu.make_async_copy(gate_hbm, gate_ref, xsem.at[1])]
    for copy in late:
        copy.start()
    merge_high(3, True)
    y_far[0].start()
    y_far[1].start()
    for h in range(2):
        x_far[h].wait_recv()
        merge(acc.at[1 + h, 0, :, part_rows[1]], p1a.at[1, h])
        y_last[h].start()
        y_far[h].wait_recv()
        merge(acc.at[1 + h, 1, :, part_rows[0]], p1b.at[1, h])
        x_last[h].start()
    for h in range(2):
        x_first[h].wait_recv()
        merge(acc.at[0, 0, :, part_rows[h]], p1a.at[0, h])
        y_first[h].wait_recv()
        merge(acc.at[0, 1, :, part_rows[h]], p1b.at[0, h])
    for copy in late:
        copy.wait()
    for h in range(2):
        for part, last, buf in ((0, y_last, p2a), (1, x_last, p2b)):
            last[h].wait_recv()

            @pl.loop(0, mid // 16)
            def _(i, h=h, part=part, buf=buf):
                near = pl.ds(pl.multiple_of(i * 16, 16), 16)
                at = pl.ds(pl.multiple_of(h * mid + i * 16, 16), 16)
                wide = pl.ds(part * half, half)
                gates = gate_ref[at]
                y_val = [(acc[0, part, slot, at] + buf[h, slot, near]).astype(jnp.float32) * gates[:, slot:slot + 1] for slot in range(2)]
                out_ref[at, wide] = (x_ref[at, wide].astype(jnp.float32) + (y_val[0] + y_val[1])).astype(jnp.bfloat16)

    out_copy = pltpu.make_async_copy(out_ref, out_hbm, xsem.at[2])
    out_copy.start()
    for copy in gather + scatter:
        copy.wait_send()
    for part in range(2):
        shared(3, part).wait_send()
    out_copy.wait()


def moe_call(h_ext, x_mid, gates, w_gate, w_up, w_down):
    rows, d_model = x_mid.shape
    half = d_model // 2
    ff = w_gate.shape[2]
    ff_pad = pl.cdiv(ff, 128) * 128
    width = h_ext.shape[1]
    hbm = pl.BlockSpec(memory_space=pl.ANY)
    bf = jnp.bfloat16
    dma = pltpu.SemaphoreType.DMA
    out, _ = pl.pallas_call(
        moe_kernel,
        in_specs=[hbm] * 6,
        out_specs=[hbm, hbm],
        out_shape=[jax.ShapeDtypeStruct((rows, d_model), bf), jax.ShapeDtypeStruct((8, rows, width), bf)],
        scratch_shapes=[
            pltpu.VMEM((2, ff, d_model), bf),
            pltpu.VMEM((2, ff, d_model), bf),
            pltpu.VMEM((2, ff, d_model), bf),
            pltpu.VMEM(gates.shape, gates.dtype),
            pltpu.VMEM((2 * rows, width), bf),
            pltpu.VMEM((ff_pad, 2 * rows), bf),
            pltpu.VMEM((2, 2 * rows, ff_pad), bf),
            pltpu.VMEM((4, 2, 2, rows, half), bf),
            pltpu.VMEM((2, 2, rows, half), bf),
            pltpu.VMEM((2, 2, 2, rows, half), bf),
            pltpu.VMEM((2, 2, 2, rows // 2, half), bf),
            pltpu.VMEM((2, 2, 2, rows // 2, half), bf),
            pltpu.VMEM((2, 2, rows // 2, half), bf),
            pltpu.VMEM((2, 2, rows // 2, half), bf),
            dma((3, 2)),
            dma((4,)),
            dma((13,)),
            dma((13,)),
            dma((2,)),
            dma((4, 2)),
            dma((12,)),
            dma((12,)),
            pltpu.SemaphoreType.REGULAR,
        ],
        compiler_params=pltpu.CompilerParams(vmem_limit_bytes=67043328, collective_id=0, has_side_effects=True),
        name='moe',
    )(h_ext, x_mid, gates, jnp.swapaxes(w_gate, 1, 2), jnp.swapaxes(w_up, 1, 2), w_down)
    return out


def solution(mesh):
    def local_step(tokens, k_cache, v_cache, positions, expert_one, expert_two, eligible, ln1_gain, ln1_bias, w_query, b_query, w_key, b_key, w_value, b_value, w_out, b_out, ln2_gain, ln2_bias, w_router, w_gate, w_up, w_down):
        tok_count, seq_len, heads, head_dim = k_cache.shape
        d_model = tokens.shape[1]
        cos_tab, sin_tab = rope_tables(positions, head_dim)
        sign = jnp.where(jnp.arange(head_dim) < head_dim // 2, -1.0, 1.0)
        vectors = row_stack([ln1_gain, ln1_bias, b_query, b_key, b_value, b_out, ln2_gain, ln2_bias])
        which = lax.broadcasted_iota(jnp.int32, (128, tok_count), 0)
        picks = jnp.where(which == 0, expert_one[None, :], jnp.where(which == 1, expert_two[None, :], jnp.pad(eligible.T, ((2, 110), (0, 0)))))
        q_flat, k_flat, v_flat = qkv_call(tokens, vectors, cos_tab, sin_tab * sign[None, :], w_query, w_key, w_value)
        split = lambda t: t.reshape(tok_count, heads, head_dim)
        key_new, value_new = split(k_flat), split(v_flat)
        attn = attend_call(attention_order(positions), positions, split(q_flat), key_new, value_new, k_cache, v_cache)
        x_mid, h_ext, gates = out_call(attn.reshape(tok_count, heads * head_dim), tokens, vectors, w_router.T, picks, w_out)
        tokens_out = moe_call(h_ext, x_mid, gates, w_gate, w_up, w_down)
        return tokens_out, key_new, value_new

    row_spec = P('ep', None)
    cache_spec = P('ep', None, None, None)
    vec_spec = P('ep')
    rep_one = P(None)
    rep_two = P(None, None)
    expert_spec = P('ep', None, None)
    in_specs = (row_spec, cache_spec, cache_spec, vec_spec, vec_spec, vec_spec, row_spec, rep_one, rep_one, rep_two, rep_one, rep_two, rep_one, rep_two, rep_one, rep_two, rep_one, rep_one, rep_one, rep_two, expert_spec, expert_spec, expert_spec)
    out_specs = (row_spec, expert_spec, expert_spec)
    return jax.shard_map(local_step, mesh=mesh, in_specs=in_specs, out_specs=out_specs, check_vma=False)
```

```python
import jax
import jax.numpy as jnp
from jax import lax
from jax.experimental import pallas as pl
from jax.experimental.pallas import tpu as pltpu
from jax.sharding import PartitionSpec as P

ROPE_BASE = 10000.0
LN_EPS = 1e-5


def rope_tables(positions, head_dim):
    half_dim = head_dim // 2
    inv_freq = ROPE_BASE ** (jnp.arange(half_dim, dtype=jnp.float32) * (-2.0 / head_dim))
    angles = positions.astype(jnp.float32)[:, None] * inv_freq[None, :]
    angles = jnp.concatenate([angles, angles], axis=-1)
    return jnp.cos(angles), jnp.sin(angles)


def norm_rows(x_val, gain, bias):
    mean_val = jnp.mean(x_val, axis=-1, keepdims=True)
    centered = x_val - mean_val
    var_val = jnp.mean(centered * centered, axis=-1, keepdims=True)
    return centered * lax.rsqrt(var_val + LN_EPS) * gain.astype(jnp.float32) + bias.astype(jnp.float32)


def row_stack(vectors):
    which = lax.broadcasted_iota(jnp.int32, (len(vectors), vectors[0].shape[0]), 0)
    out = jnp.zeros((len(vectors), vectors[0].shape[0]), vectors[0].dtype)
    for n, vec in enumerate(vectors):
        out = jnp.where(which == n, vec[None, :], out)
    return out


AHEAD = 4


def qkv_kernel(x_ref, vec_ref, cos_ref, sin_ref, wq_hbm, wk_hbm, wv_hbm, q_ref, k_ref, v_ref, h_ref, w_buf, sems):
    rows, d_model = x_ref.shape
    tile = w_buf.shape[3]
    count = q_ref.shape[1] // tile
    head_dim = cos_ref.shape[1]

    def copies(j, slot):
        cols = pl.ds(pl.multiple_of(j * tile, tile), tile)
        return [pltpu.make_async_copy(hbm.at[:, cols], w_buf.at[slot, n], sems.at[slot, n]) for n, hbm in enumerate((wq_hbm, wk_hbm, wv_hbm))]

    for j in range(AHEAD):
        for copy in copies(j, j):
            copy.start()
    h_ref[...] = norm_rows(x_ref[...].astype(jnp.float32), vec_ref[0:1], vec_ref[1:2]).astype(jnp.bfloat16)

    @pl.loop(0, count)
    def _(j):
        slot = lax.rem(j, AHEAD)
        cols = pl.ds(pl.multiple_of(j * tile, tile), tile)
        for copy in copies(j, slot):
            copy.wait()
        for n, o_ref in enumerate((q_ref, k_ref, v_ref)):
            lin = jnp.dot(h_ref[...], w_buf[slot, n], preferred_element_type=jnp.float32) + vec_ref[2 + n:3 + n, cols].astype(jnp.float32)
            if n == 2:
                o_ref[:, cols] = lin.astype(jnp.bfloat16)
            else:
                parts = []
                for c in range(tile // head_dim):
                    part = lin[:, c * head_dim:(c + 1) * head_dim]
                    parts.append(part * cos_ref[...] + pltpu.roll(part, head_dim // 2, 1) * sin_ref[...])
                o_ref[:, cols] = jnp.concatenate(parts, axis=1).astype(jnp.bfloat16)

        @pl.when(j + AHEAD < count)
        def _():
            for copy in copies(j + AHEAD, slot):
                copy.start()


def qkv_call(tokens, vectors, cos_tab, sin_signed, w_query, w_key, w_value):
    rows, d_model = tokens.shape
    cols = w_query.shape[1]
    tile = 256
    vmem = pl.BlockSpec(memory_space=pltpu.VMEM)
    hbm = pl.BlockSpec(memory_space=pl.ANY)
    shape = jax.ShapeDtypeStruct((rows, cols), jnp.bfloat16)
    return pl.pallas_call(
        qkv_kernel,
        in_specs=[vmem, vmem, vmem, vmem, hbm, hbm, hbm],
        out_specs=[vmem, vmem, vmem],
        out_shape=[shape, shape, shape],
        scratch_shapes=[pltpu.VMEM((rows, d_model), jnp.bfloat16), pltpu.VMEM((AHEAD, 3, d_model, tile), jnp.bfloat16), pltpu.SemaphoreType.DMA((AHEAD, 3))],
        compiler_params=pltpu.CompilerParams(vmem_limit_bytes=44 * 2 ** 20),
        cost_estimate=pl.CostEstimate(flops=6 * rows * d_model * cols, bytes_accessed=6 * d_model * cols, transcendentals=0),
        name='qkv',
    )(tokens, vectors, cos_tab, sin_signed, w_query, w_key, w_value)


GROUP = 8
SLOTS = 4
CHUNK = 8


def attend_kernel(order_ref, pos_ref, q_ref, kn_ref, vn_ref, k_hbm, v_hbm, out_ref, k_buf, v_buf, sid_ref, sems):
    rows, heads, head_dim = q_ref.shape
    seq = k_hbm.shape[1]
    groups = rows // GROUP
    scale = head_dim ** -0.5
    key_id = lax.broadcasted_iota(jnp.int32, sid_ref.shape, 1)
    row_id = lax.broadcasted_iota(jnp.int32, sid_ref.shape, 0)
    sid_ref[...] = jnp.where(lax.rem(key_id, heads) == row_id, lax.div(key_id, heads), seq)

    def group_at(n):
        return jnp.where(n & 1 == 0, n // 2, groups - 1 - n // 2)

    def chunks_at(n):
        return jnp.maximum((pos_ref[order_ref[group_at(n) * GROUP]] + CHUNK - 1) // CHUNK, 1)

    def fetch(n):
        grp = group_at(n)
        slot = lax.rem(n, SLOTS)
        chunks = chunks_at(n)
        for k in range(1, seq // CHUNK + 1):
            @pl.when(chunks == k)
            def _(k=k):
                src = pl.ds(0, k * CHUNK)

                @pl.loop(0, GROUP)
                def _(i):
                    tok = order_ref[grp * GROUP + i]
                    pltpu.make_async_copy(k_hbm.at[tok, src], k_buf.at[slot, i, src], sems.at[0, slot]).start()
                    pltpu.make_async_copy(v_hbm.at[tok, src], v_buf.at[slot, i, src], sems.at[1, slot]).start()

    def settle(n):
        slot = lax.rem(n, SLOTS)
        chunks = chunks_at(n)
        size = seq // CHUNK
        while size >= 1:
            @pl.when((chunks & size) != 0)
            def _(size=size):
                src = pl.ds(0, size * CHUNK)
                pltpu.make_async_copy(k_hbm.at[pl.ds(0, GROUP), src], k_buf.at[slot, :, src], sems.at[0, slot]).wait()
                pltpu.make_async_copy(v_hbm.at[pl.ds(0, GROUP), src], v_buf.at[slot, :, src], sems.at[1, slot]).wait()

            size //= 2

    def compute(n, steps):
        grp = group_at(n)
        slot = lax.rem(n, SLOTS)
        keys = steps * CHUNK * heads
        toks = [order_ref[grp * GROUP + i] for i in range(GROUP)]
        q_val = [q_ref[t] for t in toks]
        scores = []
        for i in range(GROUP):
            k_val = k_buf[slot, i, pl.ds(0, steps * CHUNK)].reshape(keys, head_dim)
            raw = lax.dot_general(q_val[i], k_val, (((1,), (1,)), ((), ())), preferred_element_type=jnp.float32)
            scores.append(jnp.where(sid_ref[:, :keys] < pos_ref[toks[i]], raw * scale, -jnp.inf))
        for i in range(GROUP):
            t = toks[i]
            s_new = jnp.sum(q_val[i].astype(jnp.float32) * kn_ref[t].astype(jnp.float32), axis=-1, keepdims=True) * scale
            top = jnp.maximum(jnp.max(scores[i], axis=-1, keepdims=True), s_new)
            e_val = jnp.exp(scores[i] - top)
            e_new = jnp.exp(s_new - top)
            inv = 1.0 / (jnp.sum(e_val, axis=-1, keepdims=True) + e_new)
            p_val = (e_val * inv).astype(jnp.bfloat16)
            p_new = (e_new * inv).astype(jnp.bfloat16).astype(jnp.float32)
            v_val = v_buf[slot, i, pl.ds(0, steps * CHUNK)].reshape(keys, head_dim)
            res = jnp.dot(p_val, v_val, preferred_element_type=jnp.float32) + p_new * vn_ref[t].astype(jnp.float32)
            out_ref[t] = res.astype(jnp.bfloat16)

    for n in range(SLOTS - 1):
        fetch(n)

    @pl.loop(0, groups)
    def _(n):
        @pl.when(n + SLOTS - 1 < groups)
        def _():
            fetch(n + SLOTS - 1)

        settle(n)
        steps = chunks_at(n)
        for k in range(1, seq // CHUNK + 1):
            @pl.when(steps == k)
            def _(k=k):
                compute(n, k)


def attend_call(order, positions, q_rot, key_new, value_new, k_cache, v_cache):
    rows, seq, heads, head_dim = k_cache.shape
    vmem = pl.BlockSpec(memory_space=pltpu.VMEM)
    smem = pl.BlockSpec(memory_space=pltpu.SMEM)
    hbm = pl.BlockSpec(memory_space=pl.ANY)
    return pl.pallas_call(
        attend_kernel,
        in_specs=[smem, smem, vmem, vmem, vmem, hbm, hbm],
        out_specs=vmem,
        out_shape=jax.ShapeDtypeStruct((rows, heads, head_dim), jnp.bfloat16),
        scratch_shapes=[
            pltpu.VMEM((SLOTS, GROUP, seq, heads, head_dim), jnp.bfloat16),
            pltpu.VMEM((SLOTS, GROUP, seq, heads, head_dim), jnp.bfloat16),
            pltpu.VMEM((heads, seq * heads), jnp.int32),
            pltpu.SemaphoreType.DMA((2, SLOTS)),
        ],
        compiler_params=pltpu.CompilerParams(vmem_limit_bytes=48 * 2 ** 20),
        cost_estimate=pl.CostEstimate(flops=4 * rows * seq * heads * heads * head_dim, bytes_accessed=2 * rows * seq * heads * head_dim, transcendentals=0),
        name='attend',
    )(order, positions, q_rot, key_new, value_new, k_cache, v_cache)


def out_kernel(a_ref, x_ref, vec_ref, wr_ref, pick_ref, w_hbm, mid_ref, h_ref, gate_ref, w_buf, sems):
    count, _, tile = w_buf.shape

    def weight(j):
        cols = pl.ds(pl.multiple_of(j * tile, tile), tile)
        return pltpu.make_async_copy(w_hbm.at[:, cols], w_buf.at[j], sems.at[j])

    for j in range(count):
        weight(j).start()

    @pl.loop(0, count)
    def _(j):
        weight(j).wait()
        cols = pl.ds(pl.multiple_of(j * tile, tile), tile)
        mid = x_ref[:, cols].astype(jnp.float32) + jnp.dot(a_ref[...], w_buf[j], preferred_element_type=jnp.float32) + vec_ref[5:6, cols].astype(jnp.float32)
        mid_ref[:, cols] = mid.astype(jnp.bfloat16)

    h_two = norm_rows(mid_ref[...].astype(jnp.float32), vec_ref[6:7], vec_ref[7:8]).astype(jnp.bfloat16)
    lanes = lax.broadcasted_iota(jnp.int32, (h_two.shape[0], 128), 1)
    pick_val = jnp.transpose(pick_ref[...].astype(jnp.float32))
    picks = jnp.where(lanes < 2, pick_val, 0.0)
    h_ref[:, :h_two.shape[1]] = h_two
    h_ref[:, h_two.shape[1]:] = picks.astype(jnp.bfloat16)
    logits = lax.dot_general(h_two, wr_ref[...], (((1,), (1,)), ((), ())), preferred_element_type=jnp.float32)
    ids = lax.broadcasted_iota(jnp.int32, logits.shape, 1).astype(jnp.float32)
    hit_one = ids == pick_val[:, 0:1]
    hit_two = ids == pick_val[:, 1:2]
    keep_one = pick_val[:, 2:2 + logits.shape[1]] == 1.0
    gates = []
    for keep, hit in ((keep_one, hit_one), (keep_one & jnp.logical_not(hit_one), hit_two)):
        masked = jnp.where(keep, logits, -jnp.inf)
        e_val = jnp.exp(masked - jnp.max(masked, axis=-1, keepdims=True))
        top = jnp.sum(jnp.where(hit, e_val, 0.0), axis=-1, keepdims=True)
        gates.append(top / jnp.sum(e_val, axis=-1, keepdims=True))
    lane = lax.broadcasted_iota(jnp.int32, gate_ref.shape, 1)
    gate_ref[...] = jnp.where(lane == 0, gates[0], jnp.where(lane == 1, gates[1], 0.0))


def out_call(attn_flat, tokens, vectors, w_router, picks, w_out):
    rows, d_model = tokens.shape
    tile = 256
    vmem = pl.BlockSpec(memory_space=pltpu.VMEM)
    shape = lambda cols, kind: jax.ShapeDtypeStruct((rows, cols), kind)
    return pl.pallas_call(
        out_kernel,
        in_specs=[vmem] * 5 + [pl.BlockSpec(memory_space=pl.ANY)],
        out_specs=[vmem] * 3,
        out_shape=[shape(d_model, jnp.bfloat16), shape(d_model + 128, jnp.bfloat16), shape(128, jnp.float32)],
        scratch_shapes=[pltpu.VMEM((d_model // tile, w_out.shape[0], tile), jnp.bfloat16), pltpu.SemaphoreType.DMA((d_model // tile,))],
        compiler_params=pltpu.CompilerParams(vmem_limit_bytes=48 * 2 ** 20),
        cost_estimate=pl.CostEstimate(flops=2 * rows * d_model * d_model, bytes_accessed=2 * d_model * d_model, transcendentals=0),
        name='project',
    )(attn_flat, tokens, vectors, w_router, picks, w_out)


def attention_order(positions):
    ids = jnp.arange(positions.shape[0], dtype=jnp.int32)
    ahead = (positions[None, :] > positions[:, None]) | ((positions[None, :] == positions[:, None]) & (ids[None, :] < ids[:, None]))
    rank = jnp.sum(ahead.astype(jnp.int32), axis=1)
    return jnp.sum(jnp.where(rank[:, None] == ids[None, :], ids[:, None], 0), axis=0)


def moe_kernel(h_in, x_hbm, gate_hbm, wg_hbm, wu_hbm, wd_hbm, out_hbm, hb, wg, wu, wd, gate_ref, xblk, zt_ref, z_ref, acc, stg, d2d, p1a, p1b, p2a, p2b, wsem, xsem, gsend, grecv, dsend, drecv, rsend, rrecv, credit):
    me = lax.axis_index('ep')
    core = lax.rem(me, 2)
    x_pos = lax.rem(lax.div(me, 2), 2)
    y_pos = lax.div(me, 4)
    partner = me + 1 - 2 * core
    xn = me + 2 - 4 * x_pos
    yn = me + 4 - 8 * y_pos
    rows = h_in.shape[0]
    mid = rows // 2
    d_model = x_hbm.shape[1]
    half = d_model // 2
    ff = wd.shape[1]
    tile = 512
    mesh_id = pl.DeviceIdType.MESH
    part_rows = (pl.ds(0, mid), pl.ds(mid, mid))

    def remote(src, dst, send, recv, dev):
        return pltpu.make_async_remote_copy(src_ref=src, dst_ref=dst, send_sem=send, recv_sem=recv, device_id=(dev,), device_id_type=mesh_id)

    gather = []

    def add_gather(src, dst, dev):
        n = len(gather)
        gather.append(remote(src, dst, gsend.at[n], grecv.at[n], dev))
        return gather[-1]

    own = add_gather(h_in, hb.at[1], partner)
    from_x = [add_gather(h_in.at[p], hb.at[2, p], xn) for p in part_rows]
    from_y = [add_gather(h_in.at[p], hb.at[4, p], yn) for p in part_rows]
    share_x = [add_gather(hb.at[2, p], hb.at[3, p], partner) for p in part_rows]
    share_y = [add_gather(hb.at[4, p], hb.at[5, p], partner) for p in part_rows]
    far = [add_gather(hb.at[2, part_rows[0]], hb.at[6, part_rows[0]], yn), add_gather(hb.at[4, part_rows[1]], hb.at[6, part_rows[1]], xn)]
    share_far = [add_gather(hb.at[6, p], hb.at[7, p], partner) for p in part_rows]

    scatter = []

    def add_scatter(src, dst, dev):
        n = len(scatter)
        scatter.append(remote(src, dst, rsend.at[n], rrecv.at[n], dev))
        return scatter[-1]

    x_first = [add_scatter(acc.at[1 + h, 0, :, part_rows[0]], p1a.at[0, h], xn) for h in range(2)]
    y_first = [add_scatter(acc.at[1 + h, 1, :, part_rows[1]], p1b.at[0, h], yn) for h in range(2)]
    x_far = [add_scatter(acc.at[3, 0, :, part_rows[h]], p1a.at[1, h], xn) for h in range(2)]
    y_far = [add_scatter(acc.at[3, 1, :, part_rows[h]], p1b.at[1, h], yn) for h in range(2)]
    y_last = [add_scatter(acc.at[1 + h, 0, :, part_rows[1]], p2a.at[h], yn) for h in range(2)]
    x_last = [add_scatter(acc.at[1 + h, 1, :, part_rows[0]], p2b.at[h], xn) for h in range(2)]

    def weight(e):
        return [pltpu.make_async_copy(hbm.at[e], buf.at[e], wsem.at[n, e]) for n, (hbm, buf) in enumerate(((wg_hbm, wg), (wu_hbm, wu), (wd_hbm, wd)))]

    barrier = pltpu.get_barrier_semaphore()
    for dev in (partner, xn, yn):
        pl.semaphore_signal(barrier, inc=1, device_id=(dev,), device_id_type=mesh_id)
    for copy in weight(0)[:2]:
        copy.start()
    zt_ref[...] = jnp.zeros_like(zt_ref)
    pl.semaphore_wait(barrier, 3)
    for h in range(2):
        from_x[h].start()
        from_y[h].start()
    own.start()

    def load(sources):
        step = 2 * rows // len(sources)
        copies = [pltpu.make_async_copy(src, xblk.at[pl.ds(n * step, step)], xsem.at[n]) for n, src in enumerate(sources)]
        for copy in copies:
            copy.start()
        for copy in copies:
            copy.wait()

    def merge(dst, src):
        count = dst.shape[1] // 16

        @pl.loop(0, 2 * count)
        def _(i):
            slot = lax.div(i, count)
            at = pl.ds(pl.multiple_of(lax.rem(i, count) * 16, 16), 16)
            dst[slot, at] = dst[slot, at] + src[slot, at]

    def shared(r, part):
        return remote(stg.at[part], d2d.at[lax.rem(r, 2), part], dsend.at[part], drecv.at[r, part], partner)

    def gather_step(h):
        from_x[h].wait_recv()
        share_x[h].start()
        if h == 0:
            far[0].start()
        from_y[h].wait_recv()
        share_y[h].start()
        if h == 1:
            far[1].start()

    def merge_high(r, finish):
        shared(r, 1).wait_recv()
        merge(acc.at[r, 1], d2d.at[lax.rem(r, 2), 1])
        if not finish:
            for h in range(2):
                @pl.when(r == 1 + h)
                def _(h=h):
                    y_first[h].start()

            @pl.when(r < 2)
            def _():
                pl.semaphore_signal(credit, inc=1, device_id=(partner,), device_id_type=mesh_id)

    @pl.loop(0, 4)
    def _(r):
        @pl.when(r == 0)
        def _():
            own.wait_recv()
            load([h_in, hb.at[1]])

        for h in range(2):
            @pl.when(r == 1 + h)
            def _(h=h):
                share_x[h].wait_recv()
                share_y[h].wait_recv()
                load([hb.at[n, part_rows[h]] for n in (2, 4, 3, 5)])

        @pl.when(r == 3)
        def _():
            share_far[0].wait_recv()
            share_far[1].wait_recv()
            load([hb.at[6], hb.at[7]])

        @pl.loop(0, 2)
        def _(e):
            @pl.when(r == 0)
            def _():
                for copy in weight(e)[:2]:
                    copy.wait()

                @pl.when(e == 0)
                def _():
                    for copy in weight(1)[:2] + [weight(0)[2], weight(1)[2]]:
                        copy.start()

            x_val = xblk[:, :d_model]
            dims = (((1,), (1,)), ((), ()))
            u_val = lax.dot_general(wg[e], x_val, dims, preferred_element_type=jnp.float32)
            v_val = lax.dot_general(wu[e], x_val, dims, preferred_element_type=jnp.float32)
            zt_ref[:ff] = (jax.nn.silu(u_val) * v_val).astype(jnp.bfloat16)
            z_ref[e] = jnp.transpose(zt_ref[...])

            @pl.when((r > 0) & (e == 0))
            def _():
                merge_high(r - 1, False)

        @pl.when(r == 1)
        def _():
            gather_step(1)

        @pl.when(r == 0)
        def _():
            for e in range(2):
                weight(e)[2].wait()

        @pl.when(r == 2)
        def _():
            for h in range(2):
                far[h].wait_recv()
                share_far[h].start()

        @pl.loop(0, 2)
        def _(part):
            @pl.when(r > 0)
            def _():
                shared(r - 1, part).wait_send()

            @pl.loop(0, half // tile)
            def _(n):
                wide = pl.ds(pl.multiple_of(part * half + n * tile, tile), tile)
                slim = pl.ds(pl.multiple_of(n * tile, tile), tile)
                first = jnp.dot(z_ref[0, :, :ff], wd[0, :, wide], preferred_element_type=jnp.float32)
                second = jnp.dot(z_ref[1, :, :ff], wd[1, :, wide], preferred_element_type=jnp.float32)
                for slot in range(2):
                    choice = xblk[:, d_model:][:, slot:slot + 1].astype(jnp.float32)
                    lead = (2 * me).astype(jnp.float32)
                    val = jnp.where(choice == lead, first, jnp.where(choice == lead + 1.0, second, 0.0)).astype(jnp.bfloat16)
                    acc[r, part, slot, :, slim] = val[:rows]
                    stg[part, slot, :, slim] = val[rows:]

            @pl.when((r >= 2) & (part == 0))
            def _():
                pl.semaphore_wait(credit, 1)

            shared(r, part).start()

        @pl.when(r == 0)
        def _():
            gather_step(0)

        shared(r, 0).wait_recv()
        merge(acc.at[r, 0], d2d.at[lax.rem(r, 2), 0])
        for h in range(2):
            @pl.when(r == 1 + h)
            def _(h=h):
                x_first[h].start()

        @pl.when(r == 3)
        def _():
            x_far[0].start()
            x_far[1].start()

    x_ref = xblk.at[pl.ds(0, rows), pl.ds(0, d_model)]
    out_ref = xblk.at[pl.ds(rows, rows), pl.ds(0, d_model)]
    late = [pltpu.make_async_copy(x_hbm, x_ref, xsem.at[0]), pltpu.make_async_copy(gate_hbm, gate_ref, xsem.at[1])]
    for copy in late:
        copy.start()
    merge_high(3, True)
    y_far[0].start()
    y_far[1].start()
    for h in range(2):
        x_far[h].wait_recv()
        merge(acc.at[1 + h, 0, :, part_rows[1]], p1a.at[1, h])
        y_last[h].start()
        y_far[h].wait_recv()
        merge(acc.at[1 + h, 1, :, part_rows[0]], p1b.at[1, h])
        x_last[h].start()
    for h in range(2):
        x_first[h].wait_recv()
        merge(acc.at[0, 0, :, part_rows[h]], p1a.at[0, h])
        y_first[h].wait_recv()
        merge(acc.at[0, 1, :, part_rows[h]], p1b.at[0, h])
    for copy in late:
        copy.wait()
    for h in range(2):
        for part, last, buf in ((0, y_last, p2a), (1, x_last, p2b)):
            last[h].wait_recv()

            @pl.loop(0, mid // 16)
            def _(i, h=h, part=part, buf=buf):
                near = pl.ds(pl.multiple_of(i * 16, 16), 16)
                at = pl.ds(pl.multiple_of(h * mid + i * 16, 16), 16)
                wide = pl.ds(part * half, half)
                gates = gate_ref[at]
                y_val = [(acc[0, part, slot, at] + buf[h, slot, near]).astype(jnp.float32) * gates[:, slot:slot + 1] for slot in range(2)]
                out_ref[at, wide] = (x_ref[at, wide].astype(jnp.float32) + (y_val[0] + y_val[1])).astype(jnp.bfloat16)

    out_copy = pltpu.make_async_copy(out_ref, out_hbm, xsem.at[2])
    out_copy.start()
    for copy in gather + scatter:
        copy.wait_send()
    for part in range(2):
        shared(3, part).wait_send()
    out_copy.wait()


def moe_call(h_ext, x_mid, gates, w_gate, w_up, w_down):
    rows, d_model = x_mid.shape
    half = d_model // 2
    ff = w_gate.shape[2]
    ff_pad = pl.cdiv(ff, 128) * 128
    width = h_ext.shape[1]
    hbm = pl.BlockSpec(memory_space=pl.ANY)
    bf = jnp.bfloat16
    dma = pltpu.SemaphoreType.DMA
    out, _ = pl.pallas_call(
        moe_kernel,
        in_specs=[hbm] * 6,
        out_specs=[hbm, hbm],
        out_shape=[jax.ShapeDtypeStruct((rows, d_model), bf), jax.ShapeDtypeStruct((8, rows, width), bf)],
        scratch_shapes=[
            pltpu.VMEM((2, ff, d_model), bf),
            pltpu.VMEM((2, ff, d_model), bf),
            pltpu.VMEM((2, ff, d_model), bf),
            pltpu.VMEM(gates.shape, gates.dtype),
            pltpu.VMEM((2 * rows, width), bf),
            pltpu.VMEM((ff_pad, 2 * rows), bf),
            pltpu.VMEM((2, 2 * rows, ff_pad), bf),
            pltpu.VMEM((4, 2, 2, rows, half), bf),
            pltpu.VMEM((2, 2, rows, half), bf),
            pltpu.VMEM((2, 2, 2, rows, half), bf),
            pltpu.VMEM((2, 2, 2, rows // 2, half), bf),
            pltpu.VMEM((2, 2, 2, rows // 2, half), bf),
            pltpu.VMEM((2, 2, rows // 2, half), bf),
            pltpu.VMEM((2, 2, rows // 2, half), bf),
            dma((3, 2)),
            dma((4,)),
            dma((13,)),
            dma((13,)),
            dma((2,)),
            dma((4, 2)),
            dma((12,)),
            dma((12,)),
            pltpu.SemaphoreType.REGULAR,
        ],
        compiler_params=pltpu.CompilerParams(vmem_limit_bytes=67043328, collective_id=0, has_side_effects=True),
        name='moe',
    )(h_ext, x_mid, gates, jnp.swapaxes(w_gate, 1, 2), jnp.swapaxes(w_up, 1, 2), w_down)
    return out


def solution(mesh):
    def local_step(tokens, k_cache, v_cache, positions, expert_one, expert_two, eligible, ln1_gain, ln1_bias, w_query, b_query, w_key, b_key, w_value, b_value, w_out, b_out, ln2_gain, ln2_bias, w_router, w_gate, w_up, w_down):
        tok_count, seq_len, heads, head_dim = k_cache.shape
        d_model = tokens.shape[1]
        cos_tab, sin_tab = rope_tables(positions, head_dim)
        sign = jnp.where(jnp.arange(head_dim) < head_dim // 2, -1.0, 1.0)
        vectors = row_stack([ln1_gain, ln1_bias, b_query, b_key, b_value, b_out, ln2_gain, ln2_bias])
        which = lax.broadcasted_iota(jnp.int32, (128, tok_count), 0)
        picks = jnp.where(which == 0, expert_one[None, :], jnp.where(which == 1, expert_two[None, :], jnp.pad(eligible.T, ((2, 110), (0, 0)))))
        q_flat, k_flat, v_flat = qkv_call(tokens, vectors, cos_tab, sin_tab * sign[None, :], w_query, w_key, w_value)
        split = lambda t: t.reshape(tok_count, heads, head_dim)
        key_new, value_new = split(k_flat), split(v_flat)
        attn = attend_call(attention_order(positions), positions, split(q_flat), key_new, value_new, k_cache, v_cache)
        x_mid, h_ext, gates = out_call(attn.reshape(tok_count, heads * head_dim), tokens, vectors, w_router.T, picks, w_out)
        tokens_out = moe_call(h_ext, x_mid, gates, w_gate, w_up, w_down)
        return tokens_out, key_new, value_new

    row_spec = P('ep', None)
    cache_spec = P('ep', None, None, None)
    vec_spec = P('ep')
    rep_one = P(None)
    rep_two = P(None, None)
    expert_spec = P('ep', None, None)
    in_specs = (row_spec, cache_spec, cache_spec, vec_spec, vec_spec, vec_spec, row_spec, rep_one, rep_one, rep_two, rep_one, rep_two, rep_one, rep_two, rep_one, rep_two, rep_one, rep_one, rep_one, rep_two, expert_spec, expert_spec, expert_spec)
    out_specs = (row_spec, expert_spec, expert_spec)
    return jax.shard_map(local_step, mesh=mesh, in_specs=in_specs, out_specs=out_specs, check_vma=False)
```
